32 devices in a mesh: gx: 2 (over x), gy: 4 (over z), gz: 4 (over y, core).
Axes of the slice: x: 2, y: 2, z: 4, core: 2. Of those that a mesh axis runs over, the one named last changes fastest.
Arguments:
- conductivity: float32 [16, 32, 1024], P('gx', 'gy', 'gz'), may hold values from 0.1 to 10
- source: float32 [16, 32, 1024], P('gx', 'gy', 'gz'), may hold values from -5 to 5
Outputs:
- solution: float32 [16, 32, 1024], P('gx', 'gy', 'gz')
- residual: float32 [16, 32, 1024], P('gx', 'gy', 'gz')
The draws below stay inside these ranges and needn't reach their ends.
All inputs are finite; a program needn't handle non-finite values.
Results may differ from the reference program's by a relative error of at most 0.0003.
Values sent between devices are 32-bit elements; how exact they have to be, the bound alone decides.
A program may use at most 64 MiB of HBM per device.

```python
import math
import jax
import jax.numpy as jnp

LEVELS = 3
DEGREE = 4
COARSE_DEGREE = 8
NX = 16
NY = 32
NZ = 1024


def draw_source(key, part):
    rough = jnp.clip(jax.random.normal(key, (NX, NY, NZ), jnp.float32), -5.0, 5.0)
    return rough


def levels(stream_key, dims, cuts, smallest, largest):
    def one(position, parts):
        steps = jax.random.uniform(jax.random.fold_in(jax.random.fold_in(stream_key, 6), position), (parts,), jnp.float32, smallest / len(cuts), largest / len(cuts))
        return jnp.repeat(jnp.exp(steps), dims[position] // parts).reshape((-1,) + (1,) * (len(dims) - position - 1))

    factor_of = one(*cuts[0])
    for cut in cuts[1:]:
        factor_of = factor_of * one(*cut)
    return factor_of


def setup_inputs(seed: int = 0) -> dict:
    seeds = jax.random.split(jax.random.key(seed), 3)
    return {
        "conductivity": jnp.clip(jnp.exp(math.log(10.0) - 4.6051702 * jax.random.uniform(seeds[0], (NX, NY, NZ), jnp.float32) ** levels(seeds[0], (NX, NY, NZ), ((0, 2), (1, 4), (2, 4)), -0.2, 0.2)), 0.1, 10.0),
        "source": draw_source(jax.random.fold_in(seeds[2], 71), 0),
    }


weight_table = {1: 14.0 / 30.0, 2: 3.0 / 30.0, 3: 1.0 / 30.0}
neighbour_offsets = [(along_one, along_two, along_three) for along_one in (-1, 0, 1) for along_two in (-1, 0, 1) for along_three in (-1, 0, 1) if (along_one, along_two, along_three) != (0, 0, 0)]
smooth_low = 0.5
coarse_low = 0.03
upper_bound = 2.0


def shifted(padded, offset):
    return padded[1 + offset[0]:padded.shape[0] - 1 + offset[0], 1 + offset[1]:padded.shape[1] - 1 + offset[1], 1 + offset[2]:padded.shape[2] - 1 + offset[2]]


def stencil(field_pad, coeff_pad, spacing):
    centre_field = shifted(field_pad, (0, 0, 0))
    centre_coeff = shifted(coeff_pad, (0, 0, 0))
    total = jnp.zeros(centre_field.shape, jnp.float32)
    for offset in neighbour_offsets:
        weight = weight_table[abs(offset[0]) + abs(offset[1]) + abs(offset[2])]
        total = total + weight * (centre_coeff + shifted(coeff_pad, offset)) * (centre_field - shifted(field_pad, offset))
    return total * (0.5 / spacing)


def diagonal_of(coeff_pad, spacing):
    centre_coeff = shifted(coeff_pad, (0, 0, 0))
    total = jnp.zeros(centre_coeff.shape, jnp.float32)
    for offset in neighbour_offsets:
        weight = weight_table[abs(offset[0]) + abs(offset[1]) + abs(offset[2])]
        total = total + weight * (centre_coeff + shifted(coeff_pad, offset))
    return total * (0.5 / spacing)


def coarsen(values):
    extent = values.shape
    return values.reshape(extent[0] // 2, 2, extent[1] // 2, 2, extent[2] // 2, 2).mean(axis=(1, 3, 5))


def refine(values):
    return jnp.repeat(jnp.repeat(jnp.repeat(values, 2, axis=0), 2, axis=1), 2, axis=2)


def chebyshev_coefs(degree, lower):
    centre = (upper_bound + lower) / 2.0
    half_width = (upper_bound - lower) / 2.0
    ratio_term = centre / half_width
    rho_prev = 1.0 / ratio_term
    weights = []
    for number in range(1, degree):
        rho_next = 1.0 / (2.0 * ratio_term - rho_prev)
        weights.append((rho_next * rho_prev, 2.0 * rho_next / half_width))
        rho_prev = rho_next
    return centre, weights


def smooth(operate, diagonal, right_side, start, degree, lower, final):
    centre, weights = chebyshev_coefs(degree, lower)
    if start is None:
        residual = right_side
    else:
        residual = right_side - operate(start)
    update = residual / (centre * diagonal)
    solution = update if start is None else start + update
    for pair in weights:
        residual = residual - operate(update)
        update = pair[0] * update + pair[1] * residual / diagonal
        solution = solution + update
    if final:
        residual = residual - operate(update)
    return solution, residual


def reference(conductivity, source):
    coeffs = [conductivity]
    for number in range(1, LEVELS):
        coeffs.append(coarsen(coeffs[-1]))

    def cycle(grid_level, right_side):
        spacing = float(4 ** grid_level)
        coeff_pad = jnp.pad(coeffs[grid_level], 1)
        diagonal = diagonal_of(coeff_pad, spacing)

        def operate(field):
            return stencil(jnp.pad(field, 1), coeff_pad, spacing)

        if grid_level == LEVELS - 1:
            return smooth(operate, diagonal, right_side, None, COARSE_DEGREE, coarse_low, False)
        solution, residual = smooth(operate, diagonal, right_side, None, DEGREE, smooth_low, True)
        correction, ignored = cycle(grid_level + 1, coarsen(residual))
        solution = solution + refine(correction)
        return smooth(operate, diagonal, right_side, solution, DEGREE, smooth_low, grid_level == 0)

    return cycle(0, source)
```

```python
import functools

import jax
import jax.numpy as jnp
from jax import lax
from jax.experimental import pallas as pl
from jax.experimental.pallas import tpu as pltpu
from jax.sharding import PartitionSpec as P

LEVELS = 3
DEGREE = 4
COARSE_DEGREE = 8
MESH = pl.DeviceIdType.MESH


weight_table = {1: 14.0 / 30.0, 2: 3.0 / 30.0, 3: 1.0 / 30.0}
neighbour_offsets = [
    (along_one, along_two, along_three)
    for along_one in (-1, 0, 1)
    for along_two in (-1, 0, 1)
    for along_three in (-1, 0, 1)
    if (along_one, along_two, along_three) != (0, 0, 0)
]
smooth_low = 0.5
coarse_low = 0.03
upper_bound = 2.0


def padded_2(block, sides, width):
    for axis, dim in sides:
        count = lax.axis_size(axis)
        forward = [(i, i + 1) for i in range(count - 1)]
        backward = [(target, source) for source, target in forward]
        low = lax.ppermute(
            lax.slice_in_dim(block, block.shape[dim] - width, None, axis=dim), axis, forward
        )
        high = lax.ppermute(lax.slice_in_dim(block, 0, width, axis=dim), axis, backward)
        block = jnp.concatenate([low, block, high], axis=dim)
    return block


def shifted(padded, offset):
    return padded[
        1 + offset[0] : padded.shape[0] - 1 + offset[0],
        1 + offset[1] : padded.shape[1] - 1 + offset[1],
        1 + offset[2] : padded.shape[2] - 1 + offset[2],
    ]


def inner(values, margin):
    return values[
        margin : values.shape[0] - margin,
        margin : values.shape[1] - margin,
        margin : values.shape[2] - margin,
    ]


def stencil(field_pad, coeff_pad, spacing):
    centre_field = shifted(field_pad, (0, 0, 0))
    centre_coeff = shifted(coeff_pad, (0, 0, 0))
    total = jnp.zeros(centre_field.shape, jnp.float32)
    for offset in neighbour_offsets:
        weight = weight_table[abs(offset[0]) + abs(offset[1]) + abs(offset[2])]
        total = total + weight * (centre_coeff + shifted(coeff_pad, offset)) * (
            centre_field - shifted(field_pad, offset)
        )
    return total * (0.5 / spacing)


def diagonal_of(coeff_pad, spacing):
    centre_coeff = shifted(coeff_pad, (0, 0, 0))
    total = jnp.zeros(centre_coeff.shape, jnp.float32)
    for offset in neighbour_offsets:
        weight = weight_table[abs(offset[0]) + abs(offset[1]) + abs(offset[2])]
        total = total + weight * (centre_coeff + shifted(coeff_pad, offset))
    return total * (0.5 / spacing)


def coarsen(values):
    extent = values.shape
    return values.reshape(extent[0] // 2, 2, extent[1] // 2, 2, extent[2] // 2, 2).mean(
        axis=(1, 3, 5)
    )


def refine(values):
    return jnp.repeat(jnp.repeat(jnp.repeat(values, 2, axis=0), 2, axis=1), 2, axis=2)


def chebyshev_coefs(degree, lower):
    centre = (upper_bound + lower) / 2.0
    half_width = (upper_bound - lower) / 2.0
    ratio_term = centre / half_width
    rho_prev = 1.0 / ratio_term
    weights = []
    for number in range(1, degree):
        rho_next = 1.0 / (2.0 * ratio_term - rho_prev)
        weights.append((rho_next * rho_prev, 2.0 * rho_next / half_width))
        rho_prev = rho_next
    return (centre, weights)


def inside_mask(extent, margin):
    first_pos = (
        lax.axis_index("gx") * extent[0]
        + jnp.arange(extent[0] + 2 * margin, dtype=jnp.int32)
        - margin
    )
    second_pos = (
        lax.axis_index("gy") * extent[1]
        + jnp.arange(extent[1] + 2 * margin, dtype=jnp.int32)
        - margin
    )
    third_pos = (
        lax.axis_index("gz") * extent[2]
        + jnp.arange(extent[2] + 2 * margin, dtype=jnp.int32)
        - margin
    )
    first_ok = (first_pos >= 0) & (first_pos < extent[0] * lax.axis_size("gx"))
    second_ok = (second_pos >= 0) & (second_pos < extent[1] * lax.axis_size("gy"))
    third_ok = (third_pos >= 0) & (third_pos < extent[2] * lax.axis_size("gz"))
    return first_ok[:, None, None] & second_ok[None, :, None] & third_ok[None, None, :]


def operate_near(context, field):
    spacing, coeff_ext, diagonal_ext, inside = context
    padded = padded_2(field, (("gx", 0), ("gy", 1), ("gz", 2)), 1)
    return stencil(padded, inner(coeff_ext, 1), spacing)


def two_steps(context, solution, residual, update, first_pair, second_pair):
    spacing, coeff_ext, diagonal_ext, inside = context
    diagonal = inner(diagonal_ext, 1)
    stacked = jnp.stack([update, residual])
    padded = padded_2(stacked, (("gx", 1), ("gy", 2), ("gz", 3)), 2)
    update_wide = padded[0]
    residual_wide = padded[1]
    residual_near = inner(residual_wide, 1) - stencil(update_wide, coeff_ext, spacing)
    update_near = (
        first_pair[0] * inner(update_wide, 1) + first_pair[1] * residual_near / diagonal_ext
    )
    update_near = jnp.where(inside, update_near, 0.0)
    solution = solution + inner(update_near, 1)
    residual = inner(residual_near, 1) - stencil(update_near, inner(coeff_ext, 1), spacing)
    if second_pair is None:
        update = inner(update_near, 1)
    else:
        update = second_pair[0] * inner(update_near, 1) + second_pair[1] * residual / diagonal
        solution = solution + update
    return (solution, residual, update)


def relax(context, right_side, start, degree, lower, final):
    diagonal = inner(context[2], 1)
    centre, weights = chebyshev_coefs(degree, lower)
    if start is None:
        residual = right_side
    else:
        residual = right_side - operate_near(context, start)
    update = residual / (centre * diagonal)
    solution = update if start is None else start + update
    plan_list = list(weights) + ([None] if final else [])
    position = 0
    while position + 1 < len(plan_list):
        solution, residual, update = two_steps(
            context, solution, residual, update, plan_list[position], plan_list[position + 1]
        )
        position = position + 2
    leftover = plan_list[position:]
    for pair in leftover:
        residual = residual - operate_near(context, update)
        update = pair[0] * update + pair[1] * residual / diagonal
        solution = solution + update
    return (solution, residual)


def body(conductivity, source):
    coeff_now = conductivity
    contexts = []
    for grid_level in range(LEVELS):
        if grid_level > 0:
            coeff_now = coarsen(coeff_now)
        spacing = float(4**grid_level)
        coeff_ext = padded_2(coeff_now, (("gx", 0), ("gy", 1), ("gz", 2)), 2)
        inside = inside_mask(coeff_now.shape, 1)
        diagonal_ext = jnp.where(inside, diagonal_of(coeff_ext, spacing), 1.0)
        contexts.append((spacing, coeff_ext, diagonal_ext, inside))

    def cycle(grid_level, right_side):
        context = contexts[grid_level]
        if grid_level == LEVELS - 1:
            return relax(context, right_side, None, COARSE_DEGREE, coarse_low, False)
        solution, residual = relax(context, right_side, None, DEGREE, smooth_low, True)
        correction, ignored = cycle(grid_level + 1, coarsen(residual))
        solution = solution + refine(correction)
        return relax(context, right_side, solution, DEGREE, smooth_low, grid_level == 0)

    return cycle(0, source)


def cells(shape, dim):
    return lax.broadcasted_iota(jnp.int32, shape, dim)


def ones_where(condition):
    return jnp.where(condition, 1.0, 0.0).astype(jnp.bfloat16)


def pick(dense, chosen):
    total = None
    for _ in range(3):
        part = dense.astype(jnp.bfloat16)
        dense = dense - part.astype(jnp.float32)
        term = jnp.dot(part, chosen, preferred_element_type=jnp.float32)
        total = term if total is None else total + term
    return total


def turn(values, shift):
    dim = len(values.shape) - 1
    return pltpu.roll(values, shift % values.shape[dim], dim)


def beside(values):
    low, high = turn(values, 1), turn(values, -1)
    tiles = values.shape[0]
    if tiles > 1:
        lane = cells(values.shape, 2)
        low = jnp.where(lane == 0, jnp.concatenate([low[tiles - 1 :], low[: tiles - 1]]), low)
        high = jnp.where(lane == 127, jnp.concatenate([high[1:], high[:1]]), high)
    return low + high


FACE = 14.0 / 3.0


def around_of(before, here, after, tiles):
    faces = before[0] + after[0] + here[1]
    edges = before[1] + after[1]
    inward = FACE * here[0] + faces + (1.0 / 3.0) * edges
    return (FACE * faces + edges)[:tiles] + beside(inward)[:tiles]


class Level:
    def __init__(self, refs, scale):
        self.ks, self.r, self.dg, self.di = refs[:4]
        self.now, self.new = refs[4:6], refs[6:8]
        self.scale = scale

    def grab(self, ref, p, row):
        return (
            ref[p, :, row : row + 8, :],
            ref[p, :, row - 1 : row + 7, :] + ref[p, :, row + 1 : row + 9, :],
        )

    def diagonal(self, raw, span, rows):
        base, count = span
        for row in rows:
            at = slice(row, row + 8)
            before, here = self.grab(raw, base - 1, row), self.grab(raw, base, row)
            for p in (base + j for j in range(count)):
                after = self.grab(raw, p + 1, row)
                near = around_of(before, here, after, raw.shape[1])
                total = self.scale * (128.0 * here[0] + 3.0 * near)
                self.dg[p, :, at, :] = total
                self.di[p, :, at, :] = jnp.where(here[0] > 0.0, 1.0 / total, 0.0)
                self.ks[p, :, at, :] = (3.0 * self.scale) * here[0]
                before, here = here, after

    def first_update(self, span, rows, centre):
        base, count = span
        for row in rows:
            at = slice(row, row + 8)
            for p in (base + j for j in range(count)):
                fresh = self.r[p, :, at, :] * self.di[p, :, at, :] * (1.0 / centre)
                self.now[0][p, :, at, :] = fresh
                self.now[1][p, :, at, :] = fresh * self.ks[p, :, at, :]

    def apply(self, span, rows, pair, tiles=None):
        base, count = span
        tiles = tiles or self.r.shape[1]
        some = slice(0, tiles)
        for row in rows:
            at = slice(row, row + 8)
            before = [self.grab(ref, base - 1, row) for ref in self.now]
            here = [self.grab(ref, base, row) for ref in self.now]
            for p in (base + j for j in range(count)):
                after = [self.grab(ref, p + 1, row) for ref in self.now]
                plain, heavy = (around_of(*parts, tiles) for parts in zip(before, here, after))
                coeff = self.ks[p, some, at, :]
                field = here[0][0][:tiles]
                left = self.dg[p, some, at, :] * field - (coeff * plain + heavy)
                left = self.r[p, some, at, :] - left
                self.r[p, some, at, :] = left
                if pair is not None:
                    fresh = pair[1] * (left * self.di[p, some, at, :])
                    if pair[0] != 0.0:
                        fresh = pair[0] * field + fresh
                    self.new[0][p, some, at, :] = fresh
                    self.new[1][p, some, at, :] = coeff * fresh
                before, here = here, after
        self.now, self.new = self.new, self.now


def kernel(sizes, block, *refs):
    (nx, ny, nz) = sizes
    (bx, by, bz) = block
    deep = 5
    cx, cy = bx // 2, by // 2
    (k_in, b_in, x_out, r_out) = refs[:4]
    (k_raw, k_mid, k_low) = refs[4:7]
    fine = Level(refs[7:15], 0.5 / 30.0)
    mid = Level(refs[15:23], 0.5 / 4.0 / 30.0)
    low = Level(refs[23:31], 0.5 / 16.0 / 30.0)
    (r_near, x_fine, x_mid, x_low, half_sum) = refs[31:36]
    (k_send, b_send, k_edge, b_edge, k_side, b_side) = refs[36:42]
    (z_send, z_got, zr_send, zr_got) = refs[42:46]
    (load_sem, send_sem, k_sem, b_sem, r_sem, z_sem, zr_sem) = refs[46:53]
    (far_send, far_k, far_b) = refs[53:56]
    ix, iy, iz = lax.axis_index("gx"), lax.axis_index("gy"), lax.axis_index("gz")
    own = 1 + deep * ix
    other = (1 - ix, iy, iz)
    mine = (pl.ds(own, bx), pl.ds(0, 2), pl.ds(by, by), slice(None))

    def span(width):
        return (own - ix * width, bx + width)

    both, middle = (by // 2, by + by // 2), (by,)

    for ref, target, which in ((k_in, k_raw, 0), (b_in, fine.r, 1)):
        for t in range(2):
            pltpu.make_async_copy(
                ref.at[:, :, pl.ds(128 * t, 128)],
                target.at[pl.ds(own, bx), t, pl.ds(by, by), :],
                load_sem.at[which],
            ).start()

    barrier = pltpu.get_barrier_semaphore()
    z_there = {1: iz + 1 < nz, -1: iz > 0}
    y_there = {1: iy + 1 < ny, -1: iy > 0, 0: None}

    def when(*conditions):
        kept = [c for c in conditions if c is not None]
        if not kept:
            return lambda f: f()
        total = kept[0]
        for c in kept[1:]:
            total = total & c
        return pl.when(total)

    def column(skip):
        for jx in range(nx):
            for jy in range(ny):
                if jx or jy or not skip:
                    yield ((ix + jx) % nx, (iy + jy) % ny)

    def greet(target):
        pl.semaphore_signal(barrier, inc=1, device_id=target, device_id_type=MESH)

    for jx, jy in column(True):
        greet((jx, jy, iz))
    for dz in (1, -1):
        @when(z_there[dz])
        def _():
            for jx, jy in column(False):
                greet((jx, jy, iz + dz))

    def clear(ref, *at):
        for p in range(ref.shape[0]):
            ref[(p, *at)] = jnp.zeros(ref[(p, *at)].shape, jnp.float32)

    for p in (0, bx + deep + 1):
        k_raw[p] = jnp.zeros(k_raw.shape[1:], jnp.float32)
    for ref in (k_raw, fine.r, r_near):
        @pl.when(iy == 0)
        def _():
            clear(ref, slice(0, 2), slice(0, by))

        @pl.when(iy == ny - 1)
        def _():
            clear(ref, slice(0, 2), slice(2 * by, 3 * by))

    def blank(ref, dims):
        ref[dims] = jnp.zeros(ref[dims].shape, jnp.float32)

    for ref in (z_got, zr_got):
        for side, gone in ((0, iz == 0), (1, iz == nz - 1)):
            @pl.when(gone)
            def _():
                blank(ref, (side,))

        for j, gone in ((2, iy == 0), (0, iy == ny - 1)):
            @pl.when(gone)
            def _():
                for side in (0, 1):
                    blank(ref, (side, j))
    for ref in (k_side, b_side):
        for side, gone in ((0, iz == 0), (1, iz == nz - 1)):
            @pl.when(gone)
            def _():
                blank(ref, (side,))
    for ref in (*fine.now, *fine.new, *mid.now, *mid.new, *low.now, *low.new, k_low, x_mid):
        clear(ref)
    top = nx * cx + 1
    for p in (0, top):
        k_mid[p] = jnp.zeros(k_mid.shape[1:], jnp.float32)
    for row in (0, ny * cy + 1):
        clear(k_mid, slice(None), slice(row, row + 1))
    half_sum[...] = jnp.zeros(half_sum.shape, jnp.float32)

    lane = cells((8, 128), 1)
    shrink = ones_where(cells((256, 128), 0) >> 1 == cells((256, 128), 1))

    def wide(values):
        return jnp.concatenate([values[0], values[1]], axis=1)

    def coarse_block(ref, send, edge):
        for q in range(cx):
            p = own + 2 * q
            half_sum[q, :, 0:by, :] = (
                ref[p, 0:2, by : 2 * by, :] + ref[p + 1, 0:2, by : 2 * by, :]
            )
        rows = [
            wide(
                half_sum[q, :, pl.ds(0, by, stride=2), :]
                + half_sum[q, :, pl.ds(1, by, stride=2), :]
            )
            for q in range(cx)
        ]
        parts = (pick(jnp.concatenate(rows, axis=0), shrink) * 0.125).reshape(cx, by, 128)
        send[...] = parts
        low_part = parts[0]
        top_part = turn(parts[0], 32)
        for q in range(1, cx):
            here = (lane >> 5) == q
            low_part = jnp.where(here, turn(parts[q], 32 * q), low_part)
            top_part = jnp.where(here, turn(parts[q], 32 * q - 96), top_part)
        edge[0] = top_part
        edge[1] = low_part

    def pack_z(ref, kind, into):
        slot = lane >> 4
        front = (lane & 15) < 8
        packs = [jnp.zeros((8, 128), jnp.float32)] * 2 if into is None else into
        top, bottom = packs
        for q in range(bx):
            here = slot == q
            low_tile = ref[own + q, 0, by : 2 * by, :]
            top_tile = ref[own + q, 1, by : 2 * by, :]
            if kind == 0:
                top = jnp.where(here & front, turn(top_tile, 16 * q - 120), top)
                bottom = jnp.where(
                    here & jnp.logical_not(front), turn(low_tile, 16 * q + 8), bottom
                )
            else:
                after = slot == (q + 1) % 8
                top = jnp.where(
                    here & jnp.logical_not(front), turn(top_tile, 16 * q + 8 - 120), top
                )
                bottom = jnp.where(after & front, turn(low_tile, 16 * q + 16), bottom)
        return (top, bottom)

    def save_z(packs, send):
        for side in (0, 1):
            send[side, 0] = packs[side]
            moved = turn(packs[side], -16 * (bx - deep))
            send[side, 1] = jnp.where(ix == 0, moved, packs[side])

    def remote(source, target, out_sem, in_sem, device):
        return pltpu.make_async_remote_copy(
            src_ref=source,
            dst_ref=target,
            send_sem=out_sem,
            recv_sem=in_sem,
            device_id=device,
            device_id_type=MESH,
        )

    def near_views(ref, depth, dy, start_x, start_own, source):
        if dy == 0:
            rows = pl.ds(by, by)
        elif source:
            rows = pl.ds(2 * by - depth, depth) if dy == 1 else pl.ds(by, depth)
        else:
            rows = pl.ds(by - depth, depth) if dy == 1 else pl.ds(2 * by, depth)
        return [ref.at[pl.ds(start, planes), pl.ds(0, 2), rows, :]
                for start, planes in ((start_x, depth), (start_own, bx))]

    def near_start(source, target, depth, sems):
        start_from = jnp.where(ix == 0, bx + 1 - depth, deep + 1)
        start_to = jnp.where(ix == 0, deep + 1 - depth, bx + 1)
        for dy in (0, 1, -1):
            @when(y_there[dy])
            def _():
                froms = near_views(source, depth, dy, start_from, own, True)
                tos = near_views(target, depth, dy, start_to, own, False)
                args = (send_sem.at[0, dy + 1], sems.at[dy + 1])
                remote(froms[0], tos[0], *args, (1 - ix, iy + dy, iz)).start()
                if dy != 0:
                    remote(froms[1], tos[1], *args, (ix, iy + dy, iz)).start()

    def near_bytes(ref, depth, dy):
        if dy == 0:
            return ref.at[pl.ds(1, depth), pl.ds(0, 2), pl.ds(by, by), :]
        return ref.at[pl.ds(1, depth + bx), pl.ds(0, 2), pl.ds(by, depth), :]

    def near_wait(target, depth, sems):
        for dy in (0, 1, -1):
            @when(y_there[-dy])
            def _():
                view = near_bytes(target, depth, dy)
                remote(view, view, send_sem.at[0, dy + 1], sems.at[dy + 1], other).wait_recv()

    def near_sent(target, depths):
        for dy in (0, 1, -1):
            @when(y_there[dy])
            def _():
                for depth in depths:
                    view = near_bytes(target, depth, dy)
                    remote(view, view, send_sem.at[0, dy + 1], k_sem.at[dy + 1], other).wait_send()

    def z_start(send, got, sems):
        for side, dz in ((0, 1), (1, -1)):
            for dy in (0, 1, -1):
                @when(z_there[dz], y_there[dy])
                def _():
                    for xi in (0, 1):
                        remote(
                            send.at[side, xi],
                            got.at[side, dy + 1, xi],
                            send_sem.at[1 + side, dy + 1],
                            sems.at[side, dy + 1],
                            (ix if xi == 0 else 1 - ix, iy + dy, iz + dz),
                        ).start()

    def z_wait(got, sems, sent):
        for side, dz in ((0, 1), (1, -1)):
            for dy in (0, 1, -1):
                view = got.at[side, dy + 1]
                there = (z_there[dz], y_there[dy]) if sent else (z_there[-dz], y_there[-dy])

                @when(*there)
                def _():
                    args = (send_sem.at[1 + side, dy + 1], sems.at[side, dy + 1])
                    move = remote(view, view, *args, other)
                    if sent:
                        move.wait_send()
                    else:
                        move.wait_recv()

    def unpack_z(got, kind, target, count):
        front = (lane & 15) < 8
        kept = (lane < 8) | (lane >= 120)
        start_x = jnp.where(ix == 0, bx + 1, deep + 1 - count)
        skip = 0 if kind == 0 else 8
        for group in range(3):
            for xi, start, planes in ((0, own, bx), (1, None, deep)):
                lower, upper = got[0, 2 - group, xi], got[1, 2 - group, xi]
                pair = (lower, upper) if kind == 0 else (upper, lower)
                merged = jnp.where(front, *pair)
                first = own if xi == 0 else jnp.where(ix == 0, bx + 1, 1)
                for q in range(planes):
                    target[first + q, 2, by * group : by * group + by, :] = jnp.where(
                        kept, turn(merged, -(16 * q + 8 + skip)), 0.0
                    )

    def far_start(send, edge, target, side_target, sems):
        for jx, jy in column(True):
            remote(
                send.at[:, pl.ds(0, cy), :],
                target.at[pl.ds(1 + cx * ix, cx), 0, pl.ds(1 + cy * iy, cy), :],
                far_send.at[0],
                sems.at[0],
                (jx, jy, iz),
            ).start()
        for side, dz in ((0, 1), (1, -1)):
            @when(z_there[dz])
            def _():
                for jx, jy in column(False):
                    remote(
                        edge.at[side, pl.ds(0, cy), :],
                        side_target.at[side, ix, pl.ds(cy * iy, cy), :],
                        far_send.at[1 + side],
                        sems.at[1 + side],
                        (jx, jy, iz + dz),
                    ).start()

    def far_moves(target, side_target, sems, sent):
        view = target.at[pl.ds(1, nx * ny - 1), 0, pl.ds(1, cx * cy), :]
        move = remote(view, view, far_send.at[0], sems.at[0], other)
        yield None, move
        for side, dz in ((0, 1), (1, -1)):
            view = side_target.at[side]
            move = remote(view, view, far_send.at[1 + side], sems.at[1 + side], other)
            yield z_there[dz if sent else -dz], move

    def far_wait(target, side_target, sems):
        for there, move in far_moves(target, side_target, sems, False):
            when(there)(move.wait_recv)

    def far_sent(target, side_target, sems):
        for there, move in far_moves(target, side_target, sems, True):
            when(there)(move.wait_send)

    def keep_own(send, target):
        for jy in range(ny):
            @pl.when(iy == jy)
            def _():
                for q in range(cx):
                    rows = slice(1 + cy * jy, 1 + cy * jy + cy)
                    target[1 + cx * ix + q, 0, rows, :] = send[q, 0:cy, :]

    def unpack_far(side_target, target):
        shape = side_target.shape[2:]
        column_of = cells(shape, 1)
        for jx in range(nx):
            below, above = side_target[0, jx], side_target[1, jx]
            for q in range(cx):
                upper = jnp.where(column_of < 32, turn(above, -32 * q), 0.0)
                target[1 + cx * jx + q, 1, 1 : 1 + shape[0], :] = jnp.where(
                    column_of >= 96, turn(below, 96 - 32 * q), upper
                )

    for which, ref in ((0, k_raw), (1, fine.r)):
        view = ref.at[mine]
        pltpu.make_async_copy(view, view, load_sem.at[which]).wait()
    save_z(pack_z(fine.r, 1, pack_z(k_raw, 0, None)), z_send)
    coarse_block(k_raw, k_send, k_edge)

    peers = nx * ny - 1
    for dz in (1, -1):
        peers = peers + jnp.where(z_there[dz], nx * ny, 0)
    pl.semaphore_wait(barrier, peers)

    near_start(k_raw, k_raw, deep, k_sem)
    z_start(z_send, z_got, z_sem)
    near_start(fine.r, fine.r, deep - 1, b_sem)
    far_start(k_send, k_edge, k_mid, k_side, far_k)
    keep_own(k_send, k_mid)

    near_wait(k_raw, deep, k_sem)
    z_wait(z_got, z_sem, False)
    unpack_z(z_got, 0, k_raw, deep)
    fine.diagonal(k_raw, span(4), both)
    unpack_z(z_got, 1, fine.r, deep)
    near_wait(fine.r, deep - 1, b_sem)
    near_sent(fine.r, (deep, deep - 1))
    z_wait(z_got, z_sem, True)

    own_fine = [(q, own + q) for q in range(bx)]
    own_rows = slice(by, 2 * by)

    def add_fine(ref, fresh=False):
        for q, p in own_fine:
            value = ref[p, 0:2, own_rows, :]
            x_fine[q] = value if fresh else x_fine[q] + value

    def smooth_fine():
        for number in range(DEGREE):
            pair = weights[number] if number < DEGREE - 1 else None
            width = DEGREE - 1 - number
            fine.apply(span(width), both if width else middle, pair, None if width else 2)
            if pair is not None:
                add_fine(fine.now[0])

    centre, weights = chebyshev_coefs(DEGREE, smooth_low)
    fine.first_update(span(4), both, centre)
    add_fine(fine.now[0], True)
    smooth_fine()

    coarse_block(fine.r, b_send, b_edge)
    far_sent(k_mid, k_side, far_k)
    far_start(b_send, b_edge, mid.r, b_side, far_b)
    keep_own(b_send, mid.r)
    save_z(pack_z(fine.r, 0, None), zr_send)
    near_start(fine.r, r_near, deep - 1, r_sem)
    z_start(zr_send, zr_got, zr_sem)
    for q, p in own_fine:
        r_near[p, 0:2, own_rows, :] = fine.r[p, 0:2, own_rows, :]

    mid_span, mid_rows = (1, nx * cx), tuple(range(1, ny * cy, 8))
    low_span, low_rows = (1, nx * cx // 2), tuple(range(1, ny * cy // 2, 8))
    lows = nx * cx // 2
    low_row = ny * cy // 2

    def to_low(ref, target):
        rows = []
        for q in range(lows):
            total = None
            for p in (1 + 2 * q, 2 + 2 * q):
                for row in (1, 2):
                    part = ref[p, :, pl.ds(row, low_row, stride=2), :]
                    total = part if total is None else total + part
            rows.append(wide(total))
        parts = pick(jnp.concatenate(rows, axis=0), shrink) * 0.125
        target[1 : 1 + lows, 0, 1 : 1 + low_row, :] = parts.reshape(lows, low_row, 128)

    far_wait(k_mid, k_side, far_k)
    unpack_far(k_side, k_mid)
    mid.diagonal(k_mid, mid_span, mid_rows)
    to_low(k_mid, k_low)
    low.diagonal(k_low, low_span, low_rows)

    far_wait(mid.r, b_side, far_b)
    unpack_far(b_side, mid.r)
    start = 8
    inside = (slice(1, 1 + nx * cx), slice(None), slice(1, 1 + ny * cy))

    def add_mid(ref, fresh=False):
        for q in range(nx * cx):
            value = ref[1 + q, :, 1 : 1 + ny * cy, :]
            at = (q, slice(None), slice(start, start + ny * cy))
            x_mid[at] = value if fresh else x_mid[at] + value

    mid.first_update(mid_span, mid_rows, centre)
    add_mid(mid.now[0], True)
    for number in range(DEGREE):
        pair = weights[number] if number < DEGREE - 1 else None
        mid.apply(mid_span, mid_rows, pair)
        if pair is not None:
            add_mid(mid.now[0])

    to_low(mid.r, low.r)
    low_centre, low_weights = chebyshev_coefs(COARSE_DEGREE, coarse_low)
    low.first_update(low_span, low_rows, low_centre)

    def low_now():
        return low.now[0][1 : 1 + lows, 0, 1 : 1 + low_row, :]

    x_low[...] = low_now()
    for pair in low_weights:
        low.apply(low_span, low_rows, pair)
        x_low[...] += low_now()

    spread = ones_where(cells((128, 256), 0) == cells((128, 256), 1) >> 1)
    fixed = pick(x_low[...].reshape(lows * low_row, 128), spread).reshape(lows, low_row, 256)
    for q in range(lows):
        for t in range(2):
            value = fixed[q, :, 128 * t : 128 * t + 128]
            for p in (1 + 2 * q, 2 + 2 * q):
                for row in (1, 2):
                    mid.now[0][p, t, pl.ds(row, low_row, stride=2), :] = value
    for p in range(1, 1 + nx * cx):
        at = (p, slice(None), slice(1, 1 + ny * cy))
        mid.now[1][at] = mid.ks[at] * mid.now[0][at]
    add_mid(mid.now[0])
    mid.apply(mid_span, mid_rows, (0.0, 1.0 / centre))
    add_mid(mid.now[0])
    for pair in weights:
        mid.apply(mid_span, mid_rows, pair)
        add_mid(mid.now[0])

    near_wait(r_near, deep - 1, r_sem)
    z_wait(zr_got, zr_sem, False)
    unpack_z(zr_got, 0, r_near, deep)
    shape = (256, 384)
    from_lane, to_lane = cells(shape, 0), cells(shape, 1)
    to_lane = jnp.where(
        to_lane < 256, to_lane >> 1, (to_lane >> 1) + jnp.where(to_lane < 320, 0, 64)
    )
    widen = ones_where(from_lane == to_lane)
    planes = (bx + deep + 1) // 2
    rows = []
    x_rows = 16
    for j in range(planes):
        from_row = start - 3 + cy * iy
        rows.append(wide(x_mid[ix + j, :, pl.ds(from_row, x_rows), :]))
    fixed = pick(jnp.concatenate(rows, axis=0), widen).reshape(planes, x_rows, 384)
    for j in range(planes):
        for t in range(3):
            value = fixed[j, :, 128 * t : 128 * t + 128]
            for p in (0, 1):
                for row in (0, 1):
                    at = 1 - ix + 2 * j + p
                    fine.now[0][at, t, pl.ds(2 + row, 8, stride=2), :] = value[0:8]
                    fine.now[0][at, t, pl.ds(18 + row, 2, stride=2), :] = value[8:10]
    for p in range(1, 1 + bx + deep):
        fine.now[1][p] = (3.0 * fine.scale) * k_raw[p] * fine.now[0][p]
    add_fine(fine.now[0])
    fine.r = r_near
    fine.apply(span(4), both, (0.0, 1.0 / centre))
    add_fine(fine.now[0])
    smooth_fine()
    for q, p in own_fine:
        for t in range(2):
            x_out[q, :, 128 * t : 128 * t + 128] = x_fine[q, t]
            r_out[q, :, 128 * t : 128 * t + 128] = fine.r[p, t, own_rows, :]
    near_sent(r_near, (deep - 1,))
    z_wait(zr_got, zr_sem, True)
    far_sent(mid.r, b_side, far_b)


def gathered(sizes, conductivity, source):
    (nx, ny, nz) = sizes
    (bx, by, bz) = conductivity.shape
    kept = lambda *shape: pltpu.VMEM(shape, jnp.float32)
    fine = kept(bx + 7, 3, 3 * by, 128)
    mid = kept(nx * bx // 2 + 2, 2, ny * by // 2 + 8, 128)
    low = kept(nx * bx // 4 + 2, 1, ny * by // 4 + 8, 128)
    cx, cy = bx // 2, by // 2
    scratch = [fine, mid, low] + [fine] * 8 + [mid] * 8 + [low] * 8
    scratch += [fine, kept(bx, 2, by, 128), kept(nx * cx, 2, ny * cy + 24, 128)]
    scratch += [kept(nx * cx // 2, ny * cy // 2, 128), kept(cx, 2, 2 * by, 128)]
    scratch += [kept(cx, by, 128)] * 2 + [kept(2, by, 128)] * 2
    scratch += [kept(2, nx, ny * cy, 128)] * 2
    scratch += [kept(2, 2, by, 128), kept(2, 3, 2, by, 128)] * 2
    dma = pltpu.SemaphoreType.DMA
    scratch += [dma((2,)), dma((3, 3)), dma((3,)), dma((3,)), dma((3,)), dma((2, 3)), dma((2, 3))]
    scratch += [dma((3,)), dma((3,)), dma((3,))]
    shape = jax.ShapeDtypeStruct((bx, by, bz), jnp.float32)
    vmem = pl.BlockSpec(memory_space=pltpu.VMEM)
    anywhere = pl.BlockSpec(memory_space=pl.ANY)
    return pl.pallas_call(
        functools.partial(kernel, sizes, (bx, by, bz)),
        out_shape=(shape, shape),
        in_specs=[anywhere, anywhere],
        out_specs=(vmem, vmem),
        scratch_shapes=scratch,
        compiler_params=pltpu.CompilerParams(
            collective_id=0, has_side_effects=True, vmem_limit_bytes=48 * 1024 * 1024
        ),
    )(conductivity, source)


def plan(conductivity, source):
    sizes = tuple(lax.axis_size(axis) for axis in ("gx", "gy", "gz"))
    (bx, by, bz) = conductivity.shape
    fits = (bx, by, bz) == (8, 8, 256) and sizes[0] == 2 and sizes[1] == 4
    if fits:
        return gathered(sizes, conductivity, source)
    return body(conductivity, source)


def solution(mesh):
    in_specs = (P("gx", "gy", "gz"), P("gx", "gy", "gz"))
    out_specs = (P("gx", "gy", "gz"), P("gx", "gy", "gz"))
    return jax.shard_map(plan, mesh=mesh, in_specs=in_specs, out_specs=out_specs, check_vma=False)
```

```python
import functools

import jax
import jax.numpy as jnp
from jax import lax
from jax.experimental import pallas as pl
from jax.experimental.pallas import tpu as pltpu
from jax.sharding import PartitionSpec as P

LEVELS = 3
DEGREE = 4
COARSE_DEGREE = 8
MESH = pl.DeviceIdType.MESH


weight_table = {1: 14.0 / 30.0, 2: 3.0 / 30.0, 3: 1.0 / 30.0}
neighbour_offsets = [
    (along_one, along_two, along_three)
    for along_one in (-1, 0, 1)
    for along_two in (-1, 0, 1)
    for along_three in (-1, 0, 1)
    if (along_one, along_two, along_three) != (0, 0, 0)
]
smooth_low = 0.5
coarse_low = 0.03
upper_bound = 2.0


def padded_2(block, sides, width):
    for axis, dim in sides:
        count = lax.axis_size(axis)
        forward = [(i, i + 1) for i in range(count - 1)]
        backward = [(target, source) for source, target in forward]
        low = lax.ppermute(
            lax.slice_in_dim(block, block.shape[dim] - width, None, axis=dim), axis, forward
        )
        high = lax.ppermute(lax.slice_in_dim(block, 0, width, axis=dim), axis, backward)
        block = jnp.concatenate([low, block, high], axis=dim)
    return block


def shifted(padded, offset):
    return padded[
        1 + offset[0] : padded.shape[0] - 1 + offset[0],
        1 + offset[1] : padded.shape[1] - 1 + offset[1],
        1 + offset[2] : padded.shape[2] - 1 + offset[2],
    ]


def inner(values, margin):
    return values[
        margin : values.shape[0] - margin,
        margin : values.shape[1] - margin,
        margin : values.shape[2] - margin,
    ]


def stencil(field_pad, coeff_pad, spacing):
    centre_field = shifted(field_pad, (0, 0, 0))
    centre_coeff = shifted(coeff_pad, (0, 0, 0))
    total = jnp.zeros(centre_field.shape, jnp.float32)
    for offset in neighbour_offsets:
        weight = weight_table[abs(offset[0]) + abs(offset[1]) + abs(offset[2])]
        total = total + weight * (centre_coeff + shifted(coeff_pad, offset)) * (
            centre_field - shifted(field_pad, offset)
        )
    return total * (0.5 / spacing)


def diagonal_of(coeff_pad, spacing):
    centre_coeff = shifted(coeff_pad, (0, 0, 0))
    total = jnp.zeros(centre_coeff.shape, jnp.float32)
    for offset in neighbour_offsets:
        weight = weight_table[abs(offset[0]) + abs(offset[1]) + abs(offset[2])]
        total = total + weight * (centre_coeff + shifted(coeff_pad, offset))
    return total * (0.5 / spacing)


def coarsen(values):
    extent = values.shape
    return values.reshape(extent[0] // 2, 2, extent[1] // 2, 2, extent[2] // 2, 2).mean(
        axis=(1, 3, 5)
    )


def refine(values):
    return jnp.repeat(jnp.repeat(jnp.repeat(values, 2, axis=0), 2, axis=1), 2, axis=2)


def chebyshev_coefs(degree, lower):
    centre = (upper_bound + lower) / 2.0
    half_width = (upper_bound - lower) / 2.0
    ratio_term = centre / half_width
    rho_prev = 1.0 / ratio_term
    weights = []
    for number in range(1, degree):
        rho_next = 1.0 / (2.0 * ratio_term - rho_prev)
        weights.append((rho_next * rho_prev, 2.0 * rho_next / half_width))
        rho_prev = rho_next
    return (centre, weights)


def inside_mask(extent, margin):
    first_pos = (
        lax.axis_index("gx") * extent[0]
        + jnp.arange(extent[0] + 2 * margin, dtype=jnp.int32)
        - margin
    )
    second_pos = (
        lax.axis_index("gy") * extent[1]
        + jnp.arange(extent[1] + 2 * margin, dtype=jnp.int32)
        - margin
    )
    third_pos = (
        lax.axis_index("gz") * extent[2]
        + jnp.arange(extent[2] + 2 * margin, dtype=jnp.int32)
        - margin
    )
    first_ok = (first_pos >= 0) & (first_pos < extent[0] * lax.axis_size("gx"))
    second_ok = (second_pos >= 0) & (second_pos < extent[1] * lax.axis_size("gy"))
    third_ok = (third_pos >= 0) & (third_pos < extent[2] * lax.axis_size("gz"))
    return first_ok[:, None, None] & second_ok[None, :, None] & third_ok[None, None, :]


def operate_near(context, field):
    spacing, coeff_ext, diagonal_ext, inside = context
    padded = padded_2(field, (("gx", 0), ("gy", 1), ("gz", 2)), 1)
    return stencil(padded, inner(coeff_ext, 1), spacing)


def two_steps(context, solution, residual, update, first_pair, second_pair):
    spacing, coeff_ext, diagonal_ext, inside = context
    diagonal = inner(diagonal_ext, 1)
    stacked = jnp.stack([update, residual])
    padded = padded_2(stacked, (("gx", 1), ("gy", 2), ("gz", 3)), 2)
    update_wide = padded[0]
    residual_wide = padded[1]
    residual_near = inner(residual_wide, 1) - stencil(update_wide, coeff_ext, spacing)
    update_near = (
        first_pair[0] * inner(update_wide, 1) + first_pair[1] * residual_near / diagonal_ext
    )
    update_near = jnp.where(inside, update_near, 0.0)
    solution = solution + inner(update_near, 1)
    residual = inner(residual_near, 1) - stencil(update_near, inner(coeff_ext, 1), spacing)
    if second_pair is None:
        update = inner(update_near, 1)
    else:
        update = second_pair[0] * inner(update_near, 1) + second_pair[1] * residual / diagonal
        solution = solution + update
    return (solution, residual, update)


def relax(context, right_side, start, degree, lower, final):
    diagonal = inner(context[2], 1)
    centre, weights = chebyshev_coefs(degree, lower)
    if start is None:
        residual = right_side
    else:
        residual = right_side - operate_near(context, start)
    update = residual / (centre * diagonal)
    solution = update if start is None else start + update
    plan_list = list(weights) + ([None] if final else [])
    position = 0
    while position + 1 < len(plan_list):
        solution, residual, update = two_steps(
            context, solution, residual, update, plan_list[position], plan_list[position + 1]
        )
        position = position + 2
    leftover = plan_list[position:]
    for pair in leftover:
        residual = residual - operate_near(context, update)
        update = pair[0] * update + pair[1] * residual / diagonal
        solution = solution + update
    return (solution, residual)


def body(conductivity, source):
    coeff_now = conductivity
    contexts = []
    for grid_level in range(LEVELS):
        if grid_level > 0:
            coeff_now = coarsen(coeff_now)
        spacing = float(4**grid_level)
        coeff_ext = padded_2(coeff_now, (("gx", 0), ("gy", 1), ("gz", 2)), 2)
        inside = inside_mask(coeff_now.shape, 1)
        diagonal_ext = jnp.where(inside, diagonal_of(coeff_ext, spacing), 1.0)
        contexts.append((spacing, coeff_ext, diagonal_ext, inside))

    def cycle(grid_level, right_side):
        context = contexts[grid_level]
        if grid_level == LEVELS - 1:
            return relax(context, right_side, None, COARSE_DEGREE, coarse_low, False)
        solution, residual = relax(context, right_side, None, DEGREE, smooth_low, True)
        correction, ignored = cycle(grid_level + 1, coarsen(residual))
        solution = solution + refine(correction)
        return relax(context, right_side, solution, DEGREE, smooth_low, grid_level == 0)

    return cycle(0, source)


def cells(shape, dim):
    return lax.broadcasted_iota(jnp.int32, shape, dim)


def ones_where(condition):
    return jnp.where(condition, 1.0, 0.0).astype(jnp.bfloat16)


def pick(dense, chosen):
    total = None
    for _ in range(3):
        part = dense.astype(jnp.bfloat16)
        dense = dense - part.astype(jnp.float32)
        term = jnp.dot(part, chosen, preferred_element_type=jnp.float32)
        total = term if total is None else total + term
    return total


def turn(values, shift):
    dim = len(values.shape) - 1
    return pltpu.roll(values, shift % values.shape[dim], dim)


def beside(values):
    low, high = turn(values, 1), turn(values, -1)
    tiles = values.shape[0]
    if tiles > 1:
        lane = cells(values.shape, 2)
        low = jnp.where(lane == 0, jnp.concatenate([low[tiles - 1 :], low[: tiles - 1]]), low)
        high = jnp.where(lane == 127, jnp.concatenate([high[1:], high[:1]]), high)
    return low + high


FACE = 14.0 / 3.0


def around_of(before, here, after, tiles):
    faces = before[0] + after[0] + here[1]
    edges = before[1] + after[1]
    inward = FACE * here[0] + faces + (1.0 / 3.0) * edges
    return (FACE * faces + edges)[:tiles] + beside(inward)[:tiles]


class Level:
    def __init__(self, refs, scale):
        self.ks, self.r, self.dg, self.di = refs[:4]
        self.now, self.new = refs[4:6], refs[6:8]
        self.scale = scale

    def grab(self, ref, p, row):
        return (
            ref[p, :, row : row + 8, :],
            ref[p, :, row - 1 : row + 7, :] + ref[p, :, row + 1 : row + 9, :],
        )

    def diagonal(self, raw, span, rows):
        base, count = span
        for row in rows:
            at = slice(row, row + 8)
            before, here = self.grab(raw, base - 1, row), self.grab(raw, base, row)
            for p in (base + j for j in range(count)):
                after = self.grab(raw, p + 1, row)
                near = around_of(before, here, after, raw.shape[1])
                total = self.scale * (128.0 * here[0] + 3.0 * near)
                self.dg[p, :, at, :] = total
                self.di[p, :, at, :] = jnp.where(here[0] > 0.0, 1.0 / total, 0.0)
                self.ks[p, :, at, :] = (3.0 * self.scale) * here[0]
                before, here = here, after

    def first_update(self, span, rows, centre):
        base, count = span
        for row in rows:
            at = slice(row, row + 8)
            for p in (base + j for j in range(count)):
                fresh = self.r[p, :, at, :] * self.di[p, :, at, :] * (1.0 / centre)
                self.now[0][p, :, at, :] = fresh
                self.now[1][p, :, at, :] = fresh * self.ks[p, :, at, :]

    def apply(self, span, rows, pair, tiles=None):
        base, count = span
        tiles = tiles or self.r.shape[1]
        some = slice(0, tiles)
        for row in rows:
            at = slice(row, row + 8)
            before = [self.grab(ref, base - 1, row) for ref in self.now]
            here = [self.grab(ref, base, row) for ref in self.now]
            for p in (base + j for j in range(count)):
                after = [self.grab(ref, p + 1, row) for ref in self.now]
                plain, heavy = (around_of(*parts, tiles) for parts in zip(before, here, after))
                coeff = self.ks[p, some, at, :]
                field = here[0][0][:tiles]
                left = self.dg[p, some, at, :] * field - (coeff * plain + heavy)
                left = self.r[p, some, at, :] - left
                self.r[p, some, at, :] = left
                if pair is not None:
                    fresh = pair[1] * (left * self.di[p, some, at, :])
                    if pair[0] != 0.0:
                        fresh = pair[0] * field + fresh
                    self.new[0][p, some, at, :] = fresh
                    self.new[1][p, some, at, :] = coeff * fresh
                before, here = here, after
        self.now, self.new = self.new, self.now


def kernel(sizes, block, *refs):
    (nx, ny, nz) = sizes
    (bx, by, bz) = block
    deep = 5
    cx, cy = bx // 2, by // 2
    (k_in, b_in, x_out, r_out) = refs[:4]
    (k_raw, k_mid, k_low) = refs[4:7]
    fine = Level(refs[7:15], 0.5 / 30.0)
    mid = Level(refs[15:23], 0.5 / 4.0 / 30.0)
    low = Level(refs[23:31], 0.5 / 16.0 / 30.0)
    (r_near, x_fine, x_mid, x_low, half_sum) = refs[31:36]
    (k_send, b_send, k_edge, b_edge, k_side, b_side) = refs[36:42]
    (z_send, z_got, zr_send, zr_got) = refs[42:46]
    (load_sem, send_sem, k_sem, b_sem, r_sem, z_sem, zr_sem) = refs[46:53]
    (far_send, far_k, far_b, chain) = refs[53:57]
    ix, iy, iz = lax.axis_index("gx"), lax.axis_index("gy"), lax.axis_index("gz")
    own = 1 + deep * ix
    other = (1 - ix, iy, iz)
    mine = (pl.ds(own, bx), pl.ds(0, 2), pl.ds(by, by), slice(None))

    def span(width):
        return (own - ix * width, bx + width)

    both, middle = (by // 2, by + by // 2), (by,)

    for ref, target, which in ((k_in, k_raw, 0), (b_in, fine.r, 1)):
        for t in range(2):
            pltpu.make_async_copy(
                ref.at[:, :, pl.ds(128 * t, 128)],
                target.at[pl.ds(own, bx), t, pl.ds(by, by), :],
                load_sem.at[which],
            ).start()

    barrier = pltpu.get_barrier_semaphore()
    z_there = {1: iz + 1 < nz, -1: iz > 0, 0: None}
    y_there = {1: iy + 1 < ny, -1: iy > 0, 0: None}

    def when(*conditions):
        kept = [c for c in conditions if c is not None]
        if not kept:
            return lambda f: f()
        total = kept[0]
        for c in kept[1:]:
            total = total & c
        return pl.when(total)

    def column(skip):
        for jx in range(nx):
            for jy in range(ny):
                if jx or jy or not skip:
                    yield ((ix + jx) % nx, (iy + jy) % ny)

    def counted(number, *conditions):
        for c in conditions:
            if c is not None:
                number = jnp.where(c, number, 0)
        return number

    def greet(target):
        pl.semaphore_signal(barrier, inc=1, device_id=target, device_id_type=MESH)

    peers = 0
    for dz in (0, 1, -1):
        for dy in (0, 1, -1):
            there = (z_there[dz], y_there[dy])
            near = [jx for jx in (ix, 1 - ix) if dz or dy or jx is not ix]

            @when(*there)
            def _():
                for jx in near:
                    greet((jx, iy + dy, iz + dz))

            peers = peers + counted(len(near), *there)

    def clear(ref, *at):
        for p in range(ref.shape[0]):
            ref[(p, *at)] = jnp.zeros(ref[(p, *at)].shape, jnp.float32)

    for p in (0, bx + deep + 1):
        k_raw[p] = jnp.zeros(k_raw.shape[1:], jnp.float32)
    for ref in (k_raw, fine.r, r_near):
        @pl.when(iy == 0)
        def _():
            clear(ref, slice(0, 2), slice(0, by))

        @pl.when(iy == ny - 1)
        def _():
            clear(ref, slice(0, 2), slice(2 * by, 3 * by))

    def blank(ref, dims):
        ref[dims] = jnp.zeros(ref[dims].shape, jnp.float32)

    for ref in (z_got, zr_got):
        for side, gone in ((0, iz == 0), (1, iz == nz - 1)):
            @pl.when(gone)
            def _():
                blank(ref, (side,))

        for j, gone in ((2, iy == 0), (0, iy == ny - 1)):
            @pl.when(gone)
            def _():
                for side in (0, 1):
                    blank(ref, (side, j))
    for ref in (k_side, b_side):
        for side, gone in ((0, iz == 0), (1, iz == nz - 1)):
            @pl.when(gone)
            def _():
                blank(ref, (side,))
    for ref in (*fine.now, *fine.new, *mid.now, *mid.new, *low.now, *low.new, k_low, x_mid):
        clear(ref)
    top = nx * cx + 1
    for p in (0, top):
        k_mid[p] = jnp.zeros(k_mid.shape[1:], jnp.float32)
    for row in (0, ny * cy + 1):
        clear(k_mid, slice(None), slice(row, row + 1))
    half_sum[...] = jnp.zeros(half_sum.shape, jnp.float32)

    lane = cells((8, 128), 1)
    shrink = ones_where(cells((256, 128), 0) >> 1 == cells((256, 128), 1))

    def wide(values):
        return jnp.concatenate([values[0], values[1]], axis=1)

    def coarse_block(ref, send, edge):
        for q in range(cx):
            p = own + 2 * q
            half_sum[q, :, 0:by, :] = (
                ref[p, 0:2, by : 2 * by, :] + ref[p + 1, 0:2, by : 2 * by, :]
            )
        rows = [
            wide(
                half_sum[q, :, pl.ds(0, by, stride=2), :]
                + half_sum[q, :, pl.ds(1, by, stride=2), :]
            )
            for q in range(cx)
        ]
        parts = (pick(jnp.concatenate(rows, axis=0), shrink) * 0.125).reshape(cx, by, 128)
        send[...] = parts
        low_part = parts[0]
        top_part = turn(parts[0], 32)
        for q in range(1, cx):
            here = (lane >> 5) == q
            low_part = jnp.where(here, turn(parts[q], 32 * q), low_part)
            top_part = jnp.where(here, turn(parts[q], 32 * q - 96), top_part)
        edge[0, 0:by] = top_part
        edge[1, 0:by] = low_part

    def pack_z(ref, kind, into):
        slot = lane >> 4
        front = (lane & 15) < 8
        packs = [jnp.zeros((8, 128), jnp.float32)] * 2 if into is None else into
        top, bottom = packs
        for q in range(bx):
            here = slot == q
            low_tile = ref[own + q, 0, by : 2 * by, :]
            top_tile = ref[own + q, 1, by : 2 * by, :]
            if kind == 0:
                top = jnp.where(here & front, turn(top_tile, 16 * q - 120), top)
                bottom = jnp.where(
                    here & jnp.logical_not(front), turn(low_tile, 16 * q + 8), bottom
                )
            else:
                after = slot == (q + 1) % 8
                top = jnp.where(
                    here & jnp.logical_not(front), turn(top_tile, 16 * q + 8 - 120), top
                )
                bottom = jnp.where(after & front, turn(low_tile, 16 * q + 16), bottom)
        return (top, bottom)

    def save_z(packs, send):
        for side in (0, 1):
            send[side, 0] = packs[side]
            moved = turn(packs[side], -16 * (bx - deep))
            send[side, 1] = jnp.where(ix == 0, moved, packs[side])

    def remote(source, target, out_sem, in_sem, device):
        return pltpu.make_async_remote_copy(
            src_ref=source,
            dst_ref=target,
            send_sem=out_sem,
            recv_sem=in_sem,
            device_id=device,
            device_id_type=MESH,
        )

    def near_views(ref, depth, dy, start_x, start_own, source):
        if dy == 0:
            rows = pl.ds(by, by)
        elif source:
            rows = pl.ds(2 * by - depth, depth) if dy == 1 else pl.ds(by, depth)
        else:
            rows = pl.ds(by - depth, depth) if dy == 1 else pl.ds(2 * by, depth)
        return [ref.at[pl.ds(start, planes), pl.ds(0, 2), rows, :]
                for start, planes in ((start_x, depth), (start_own, bx))]

    def near_start(source, target, depth, sems):
        start_from = jnp.where(ix == 0, bx + 1 - depth, deep + 1)
        start_to = jnp.where(ix == 0, deep + 1 - depth, bx + 1)
        for dy in (0, 1, -1):
            @when(y_there[dy])
            def _():
                froms = near_views(source, depth, dy, start_from, own, True)
                tos = near_views(target, depth, dy, start_to, own, False)
                args = (send_sem.at[0, dy + 1], sems.at[dy + 1])
                remote(froms[0], tos[0], *args, (1 - ix, iy + dy, iz)).start()
                if dy != 0:
                    remote(froms[1], tos[1], *args, (ix, iy + dy, iz)).start()

    def near_bytes(ref, depth, dy):
        if dy == 0:
            return ref.at[pl.ds(1, depth), pl.ds(0, 2), pl.ds(by, by), :]
        return ref.at[pl.ds(1, depth + bx), pl.ds(0, 2), pl.ds(by, depth), :]

    def near_wait(target, depth, sems):
        for dy in (0, 1, -1):
            @when(y_there[-dy])
            def _():
                view = near_bytes(target, depth, dy)
                remote(view, view, send_sem.at[0, dy + 1], sems.at[dy + 1], other).wait_recv()

    def near_sent(target, depths):
        for dy in (0, 1, -1):
            @when(y_there[dy])
            def _():
                for depth in depths:
                    view = near_bytes(target, depth, dy)
                    remote(view, view, send_sem.at[0, dy + 1], k_sem.at[dy + 1], other).wait_send()

    def z_start(send, got, sems):
        for side, dz in ((0, 1), (1, -1)):
            for dy in (0, 1, -1):
                @when(z_there[dz], y_there[dy])
                def _():
                    for xi in (0, 1):
                        remote(
                            send.at[side, xi],
                            got.at[side, dy + 1, xi],
                            send_sem.at[1 + side, dy + 1],
                            sems.at[side, dy + 1],
                            (ix if xi == 0 else 1 - ix, iy + dy, iz + dz),
                        ).start()

    def z_wait(got, sems, sent):
        for side, dz in ((0, 1), (1, -1)):
            for dy in (0, 1, -1):
                view = got.at[side, dy + 1]
                there = (z_there[dz], y_there[dy]) if sent else (z_there[-dz], y_there[-dy])

                @when(*there)
                def _():
                    args = (send_sem.at[1 + side, dy + 1], sems.at[side, dy + 1])
                    move = remote(view, view, *args, other)
                    if sent:
                        move.wait_send()
                    else:
                        move.wait_recv()

    def unpack_z(got, kind, target, count):
        front = (lane & 15) < 8
        kept = (lane < 8) | (lane >= 120)
        start_x = jnp.where(ix == 0, bx + 1, deep + 1 - count)
        skip = 0 if kind == 0 else 8
        for group in range(3):
            for xi, start, planes in ((0, own, bx), (1, None, deep)):
                lower, upper = got[0, 2 - group, xi], got[1, 2 - group, xi]
                pair = (lower, upper) if kind == 0 else (upper, lower)
                merged = jnp.where(front, *pair)
                first = own if xi == 0 else jnp.where(ix == 0, bx + 1, 1)
                for q in range(planes):
                    target[first + q, 2, by * group : by * group + by, :] = jnp.where(
                        kept, turn(merged, -(16 * q + 8 + skip)), 0.0
                    )

    def far_start(send, edge, target, side_target, sems):
        for jx, jy in column(True):
            remote(
                send.at[:, pl.ds(0, cy), :],
                target.at[pl.ds(1 + cx * ix, cx), 0, pl.ds(1 + cy * iy, cy), :],
                far_send.at[0],
                sems.at[0],
                (jx, jy, iz),
            ).start()
        for side, dz in ((0, 1), (1, -1)):
            @when(z_there[dz])
            def _():
                for jx, jy in column(False):
                    remote(
                        edge.at[side, pl.ds(0, cy), :],
                        side_target.at[side, ix, pl.ds(cy * iy, cy), :],
                        far_send.at[1 + side],
                        sems.at[1 + side],
                        (jx, jy, iz + dz),
                    ).start()

    def far_moves(target, side_target, sems, sent):
        view = target.at[pl.ds(1, nx * ny - 1), 0, pl.ds(1, cx * cy), :]
        move = remote(view, view, far_send.at[0], sems.at[0], other)
        yield None, move
        for side, dz in ((0, 1), (1, -1)):
            view = side_target.at[side]
            move = remote(view, view, far_send.at[1 + side], sems.at[1 + side], other)
            yield z_there[dz if sent else -dz], move

    def far_wait(target, side_target, sems):
        for there, move in far_moves(target, side_target, sems, False):
            when(there)(move.wait_recv)

    def far_sent(target, side_target, sems):
        for there, move in far_moves(target, side_target, sems, True):
            when(there)(move.wait_send)

    def keep_own(send, target):
        for jy in range(ny):
            @pl.when(iy == jy)
            def _():
                for q in range(cx):
                    rows = slice(1 + cy * jy, 1 + cy * jy + cy)
                    target[1 + cx * ix + q, 0, rows, :] = send[q, 0:cy, :]

    def unpack_far(side_target, target):
        shape = side_target.shape[2:]
        column_of = cells(shape, 1)
        for jx in range(nx):
            below, above = side_target[0, jx], side_target[1, jx]
            for q in range(cx):
                upper = jnp.where(column_of < 32, turn(above, -32 * q), 0.0)
                target[1 + cx * jx + q, 1, 1 : 1 + shape[0], :] = jnp.where(
                    column_of >= 96, turn(below, 96 - 32 * q), upper
                )

    for which, ref in ((0, k_raw), (1, fine.r)):
        view = ref.at[mine]
        pltpu.make_async_copy(view, view, load_sem.at[which]).wait()
    save_z(pack_z(fine.r, 1, pack_z(k_raw, 0, None)), z_send)
    pl.semaphore_wait(barrier, peers)

    def pass_on(step):
        for which, dy in ((0, 1), (1, -1)):
            behind = iy - dy * step

            @when(y_there[dy], behind >= 0, behind < ny)
            def _():
                pl.semaphore_signal(
                    chain.at[which], inc=1, device_id=(ix, iy + dy, iz), device_id_type=MESH
                )

    def pass_wait(step):
        for which, dy in ((0, 1), (1, -1)):
            behind = iy - dy * (step + 1)

            @when(behind >= 0, behind < ny)
            def _():
                pl.semaphore_wait(chain.at[which], 1)

    pass_on(1)
    z_start(z_send, z_got, z_sem)
    near_start(k_raw, k_raw, deep, k_sem)
    near_start(fine.r, fine.r, deep - 1, b_sem)
    coarse_block(k_raw, k_send, k_edge)
    keep_own(k_send, k_mid)
    for step in range(1, ny - 1):
        pass_wait(step)
        if step + 1 < ny - 1:
            pass_on(step + 1)
    far_start(k_send, k_edge, k_mid, k_side, far_k)

    near_wait(k_raw, deep, k_sem)
    z_wait(z_got, z_sem, False)
    unpack_z(z_got, 0, k_raw, deep)
    fine.diagonal(k_raw, span(4), both)
    unpack_z(z_got, 1, fine.r, deep)
    near_wait(fine.r, deep - 1, b_sem)
    near_sent(fine.r, (deep, deep - 1))
    z_wait(z_got, z_sem, True)

    own_fine = [(q, own + q) for q in range(bx)]
    own_rows = slice(by, 2 * by)

    def add_fine(ref, fresh=False):
        for q, p in own_fine:
            value = ref[p, 0:2, own_rows, :]
            x_fine[q] = value if fresh else x_fine[q] + value

    def smooth_fine():
        for number in range(DEGREE):
            pair = weights[number] if number < DEGREE - 1 else None
            width = DEGREE - 1 - number
            fine.apply(span(width), both if width else middle, pair, None if width else 2)
            if pair is not None:
                add_fine(fine.now[0])

    centre, weights = chebyshev_coefs(DEGREE, smooth_low)
    fine.first_update(span(4), both, centre)
    add_fine(fine.now[0], True)
    smooth_fine()

    coarse_block(fine.r, b_send, b_edge)
    far_sent(k_mid, k_side, far_k)
    far_start(b_send, b_edge, mid.r, b_side, far_b)
    keep_own(b_send, mid.r)
    save_z(pack_z(fine.r, 0, None), zr_send)
    near_start(fine.r, r_near, deep - 1, r_sem)
    z_start(zr_send, zr_got, zr_sem)
    for q, p in own_fine:
        r_near[p, 0:2, own_rows, :] = fine.r[p, 0:2, own_rows, :]

    mid_span, mid_rows = (1, nx * cx), tuple(range(1, ny * cy, 8))
    low_span, low_rows = (1, nx * cx // 2), tuple(range(1, ny * cy // 2, 8))
    lows = nx * cx // 2
    low_row = ny * cy // 2

    def to_low(ref, target):
        rows = []
        for q in range(lows):
            total = None
            for p in (1 + 2 * q, 2 + 2 * q):
                for row in (1, 2):
                    part = ref[p, :, pl.ds(row, low_row, stride=2), :]
                    total = part if total is None else total + part
            rows.append(wide(total))
        parts = pick(jnp.concatenate(rows, axis=0), shrink) * 0.125
        target[1 : 1 + lows, 0, 1 : 1 + low_row, :] = parts.reshape(lows, low_row, 128)

    far_wait(k_mid, k_side, far_k)
    unpack_far(k_side, k_mid)
    mid.diagonal(k_mid, mid_span, mid_rows)
    to_low(k_mid, k_low)
    low.diagonal(k_low, low_span, low_rows)

    far_wait(mid.r, b_side, far_b)
    unpack_far(b_side, mid.r)
    start = 8
    inside = (slice(1, 1 + nx * cx), slice(None), slice(1, 1 + ny * cy))

    def add_mid(ref, fresh=False):
        for q in range(nx * cx):
            value = ref[1 + q, :, 1 : 1 + ny * cy, :]
            at = (q, slice(None), slice(start, start + ny * cy))
            x_mid[at] = value if fresh else x_mid[at] + value

    mid.first_update(mid_span, mid_rows, centre)
    add_mid(mid.now[0], True)
    for number in range(DEGREE):
        pair = weights[number] if number < DEGREE - 1 else None
        mid.apply(mid_span, mid_rows, pair)
        if pair is not None:
            add_mid(mid.now[0])

    to_low(mid.r, low.r)
    low_centre, low_weights = chebyshev_coefs(COARSE_DEGREE, coarse_low)
    low.first_update(low_span, low_rows, low_centre)

    def low_now():
        return low.now[0][1 : 1 + lows, 0, 1 : 1 + low_row, :]

    x_low[...] = low_now()
    for pair in low_weights:
        low.apply(low_span, low_rows, pair)
        x_low[...] += low_now()

    spread = ones_where(cells((128, 256), 0) == cells((128, 256), 1) >> 1)
    fixed = pick(x_low[...].reshape(lows * low_row, 128), spread).reshape(lows, low_row, 256)
    for q in range(lows):
        for t in range(2):
            value = fixed[q, :, 128 * t : 128 * t + 128]
            for p in (1 + 2 * q, 2 + 2 * q):
                for row in (1, 2):
                    mid.now[0][p, t, pl.ds(row, low_row, stride=2), :] = value
    for p in range(1, 1 + nx * cx):
        at = (p, slice(None), slice(1, 1 + ny * cy))
        mid.now[1][at] = mid.ks[at] * mid.now[0][at]
    add_mid(mid.now[0])
    mid.apply(mid_span, mid_rows, (0.0, 1.0 / centre))
    add_mid(mid.now[0])
    for pair in weights:
        mid.apply(mid_span, mid_rows, pair)
        add_mid(mid.now[0])

    near_wait(r_near, deep - 1, r_sem)
    z_wait(zr_got, zr_sem, False)
    unpack_z(zr_got, 0, r_near, deep)
    shape = (256, 384)
    from_lane, to_lane = cells(shape, 0), cells(shape, 1)
    to_lane = jnp.where(
        to_lane < 256, to_lane >> 1, (to_lane >> 1) + jnp.where(to_lane < 320, 0, 64)
    )
    widen = ones_where(from_lane == to_lane)
    planes = (bx + deep + 1) // 2
    rows = []
    x_rows = 16
    for j in range(planes):
        from_row = start - 3 + cy * iy
        rows.append(wide(x_mid[ix + j, :, pl.ds(from_row, x_rows), :]))
    fixed = pick(jnp.concatenate(rows, axis=0), widen).reshape(planes, x_rows, 384)
    for j in range(planes):
        for t in range(3):
            value = fixed[j, :, 128 * t : 128 * t + 128]
            for p in (0, 1):
                for row in (0, 1):
                    at = 1 - ix + 2 * j + p
                    fine.now[0][at, t, pl.ds(2 + row, 8, stride=2), :] = value[0:8]
                    fine.now[0][at, t, pl.ds(18 + row, 2, stride=2), :] = value[8:10]
    for p in range(1, 1 + bx + deep):
        fine.now[1][p] = (3.0 * fine.scale) * k_raw[p] * fine.now[0][p]
    add_fine(fine.now[0])
    fine.r = r_near
    fine.apply(span(4), both, (0.0, 1.0 / centre))
    add_fine(fine.now[0])
    smooth_fine()
    for q, p in own_fine:
        for t in range(2):
            x_out[q, :, 128 * t : 128 * t + 128] = x_fine[q, t]
            r_out[q, :, 128 * t : 128 * t + 128] = fine.r[p, t, own_rows, :]
    near_sent(r_near, (deep - 1,))
    z_wait(zr_got, zr_sem, True)
    far_sent(mid.r, b_side, far_b)


def gathered(sizes, conductivity, source):
    (nx, ny, nz) = sizes
    (bx, by, bz) = conductivity.shape
    kept = lambda *shape: pltpu.VMEM(shape, jnp.float32)
    fine = kept(bx + 7, 3, 4 * by, 128)
    mid = kept(nx * bx // 2 + 2, 2, ny * by // 2 + 8, 128)
    low = kept(nx * bx // 4 + 2, 1, ny * by // 4 + 8, 128)
    cx, cy = bx // 2, by // 2
    scratch = [fine, mid, low] + [fine] * 8 + [mid] * 8 + [low] * 8
    scratch += [fine, kept(bx, 2, by, 128), kept(nx * cx, 2, ny * cy + 24, 128)]
    scratch += [kept(nx * cx // 2, ny * cy // 2, 128), kept(cx, 2, 2 * by, 128)]
    scratch += [kept(cx, by, 128)] * 2 + [kept(2, 2 * by, 128)] * 2
    scratch += [kept(2, nx, ny * cy, 128)] * 2
    scratch += [kept(2, 2, by, 128), kept(2, 3, 2, by, 128)] * 2
    dma = pltpu.SemaphoreType.DMA
    scratch += [dma((2,)), dma((3, 3)), dma((3,)), dma((3,)), dma((3,)), dma((2, 3)), dma((2, 3))]
    scratch += [dma((3,)), dma((3,)), dma((3,)), pltpu.SemaphoreType.REGULAR((2,))]
    shape = pltpu.VMEM((bx, by, bz), jnp.float32)
    vmem = pl.BlockSpec(memory_space=pltpu.VMEM)
    anywhere = pl.BlockSpec(memory_space=pltpu.HBM)
    return pl.pallas_call(
        functools.partial(kernel, sizes, (bx, by, bz)),
        out_shape=(shape, shape),
        in_specs=[anywhere, anywhere],
        out_specs=(vmem, vmem),
        scratch_shapes=scratch,
        compiler_params=pltpu.CompilerParams(
            collective_id=0, has_side_effects=True, vmem_limit_bytes=66879488
        ),
    )(conductivity, source)


def plan(conductivity, source):
    sizes = tuple(lax.axis_size(axis) for axis in ("gx", "gy", "gz"))
    (bx, by, bz) = conductivity.shape
    fits = (bx, by, bz) == (8, 8, 256) and sizes[0] == 2 and sizes[1] == 4
    if fits:
        return gathered(sizes, conductivity, source)
    return body(conductivity, source)


def solution(mesh):
    in_specs = (P("gx", "gy", "gz"), P("gx", "gy", "gz"))
    out_specs = (P("gx", "gy", "gz"), P("gx", "gy", "gz"))
    return jax.shard_map(plan, mesh=mesh, in_specs=in_specs, out_specs=out_specs, check_vma=False)
```

```python
import functools

import jax
import jax.numpy as jnp
from jax import lax
from jax.experimental import pallas as pl
from jax.experimental.pallas import tpu as pltpu
from jax.sharding import PartitionSpec as P

LEVELS = 3
DEGREE = 4
COARSE_DEGREE = 8
MESH = pl.DeviceIdType.MESH


weight_table = {1: 14.0 / 30.0, 2: 3.0 / 30.0, 3: 1.0 / 30.0}
neighbour_offsets = [
    (along_one, along_two, along_three)
    for along_one in (-1, 0, 1)
    for along_two in (-1, 0, 1)
    for along_three in (-1, 0, 1)
    if (along_one, along_two, along_three) != (0, 0, 0)
]
smooth_low = 0.5
coarse_low = 0.03
upper_bound = 2.0


def padded_2(block, sides, width):
    for axis, dim in sides:
        count = lax.axis_size(axis)
        forward = [(i, i + 1) for i in range(count - 1)]
        backward = [(target, source) for source, target in forward]
        low = lax.ppermute(
            lax.slice_in_dim(block, block.shape[dim] - width, None, axis=dim), axis, forward
        )
        high = lax.ppermute(lax.slice_in_dim(block, 0, width, axis=dim), axis, backward)
        block = jnp.concatenate([low, block, high], axis=dim)
    return block


def shifted(padded, offset):
    return padded[
        1 + offset[0] : padded.shape[0] - 1 + offset[0],
        1 + offset[1] : padded.shape[1] - 1 + offset[1],
        1 + offset[2] : padded.shape[2] - 1 + offset[2],
    ]


def inner(values, margin):
    return values[
        margin : values.shape[0] - margin,
        margin : values.shape[1] - margin,
        margin : values.shape[2] - margin,
    ]


def stencil(field_pad, coeff_pad, spacing):
    centre_field = shifted(field_pad, (0, 0, 0))
    centre_coeff = shifted(coeff_pad, (0, 0, 0))
    total = jnp.zeros(centre_field.shape, jnp.float32)
    for offset in neighbour_offsets:
        weight = weight_table[abs(offset[0]) + abs(offset[1]) + abs(offset[2])]
        total = total + weight * (centre_coeff + shifted(coeff_pad, offset)) * (
            centre_field - shifted(field_pad, offset)
        )
    return total * (0.5 / spacing)


def diagonal_of(coeff_pad, spacing):
    centre_coeff = shifted(coeff_pad, (0, 0, 0))
    total = jnp.zeros(centre_coeff.shape, jnp.float32)
    for offset in neighbour_offsets:
        weight = weight_table[abs(offset[0]) + abs(offset[1]) + abs(offset[2])]
        total = total + weight * (centre_coeff + shifted(coeff_pad, offset))
    return total * (0.5 / spacing)


def coarsen(values):
    extent = values.shape
    return values.reshape(extent[0] // 2, 2, extent[1] // 2, 2, extent[2] // 2, 2).mean(
        axis=(1, 3, 5)
    )


def refine(values):
    return jnp.repeat(jnp.repeat(jnp.repeat(values, 2, axis=0), 2, axis=1), 2, axis=2)


def chebyshev_coefs(degree, lower):
    centre = (upper_bound + lower) / 2.0
    half_width = (upper_bound - lower) / 2.0
    ratio_term = centre / half_width
    rho_prev = 1.0 / ratio_term
    weights = []
    for number in range(1, degree):
        rho_next = 1.0 / (2.0 * ratio_term - rho_prev)
        weights.append((rho_next * rho_prev, 2.0 * rho_next / half_width))
        rho_prev = rho_next
    return (centre, weights)


def inside_mask(extent, margin):
    first_pos = (
        lax.axis_index("gx") * extent[0]
        + jnp.arange(extent[0] + 2 * margin, dtype=jnp.int32)
        - margin
    )
    second_pos = (
        lax.axis_index("gy") * extent[1]
        + jnp.arange(extent[1] + 2 * margin, dtype=jnp.int32)
        - margin
    )
    third_pos = (
        lax.axis_index("gz") * extent[2]
        + jnp.arange(extent[2] + 2 * margin, dtype=jnp.int32)
        - margin
    )
    first_ok = (first_pos >= 0) & (first_pos < extent[0] * lax.axis_size("gx"))
    second_ok = (second_pos >= 0) & (second_pos < extent[1] * lax.axis_size("gy"))
    third_ok = (third_pos >= 0) & (third_pos < extent[2] * lax.axis_size("gz"))
    return first_ok[:, None, None] & second_ok[None, :, None] & third_ok[None, None, :]


def operate_near(context, field):
    spacing, coeff_ext, diagonal_ext, inside = context
    padded = padded_2(field, (("gx", 0), ("gy", 1), ("gz", 2)), 1)
    return stencil(padded, inner(coeff_ext, 1), spacing)


def two_steps(context, solution, residual, update, first_pair, second_pair):
    spacing, coeff_ext, diagonal_ext, inside = context
    diagonal = inner(diagonal_ext, 1)
    stacked = jnp.stack([update, residual])
    padded = padded_2(stacked, (("gx", 1), ("gy", 2), ("gz", 3)), 2)
    update_wide = padded[0]
    residual_wide = padded[1]
    residual_near = inner(residual_wide, 1) - stencil(update_wide, coeff_ext, spacing)
    update_near = (
        first_pair[0] * inner(update_wide, 1) + first_pair[1] * residual_near / diagonal_ext
    )
    update_near = jnp.where(inside, update_near, 0.0)
    solution = solution + inner(update_near, 1)
    residual = inner(residual_near, 1) - stencil(update_near, inner(coeff_ext, 1), spacing)
    if second_pair is None:
        update = inner(update_near, 1)
    else:
        update = second_pair[0] * inner(update_near, 1) + second_pair[1] * residual / diagonal
        solution = solution + update
    return (solution, residual, update)


def relax(context, right_side, start, degree, lower, final):
    diagonal = inner(context[2], 1)
    centre, weights = chebyshev_coefs(degree, lower)
    if start is None:
        residual = right_side
    else:
        residual = right_side - operate_near(context, start)
    update = residual / (centre * diagonal)
    solution = update if start is None else start + update
    plan_list = list(weights) + ([None] if final else [])
    position = 0
    while position + 1 < len(plan_list):
        solution, residual, update = two_steps(
            context, solution, residual, update, plan_list[position], plan_list[position + 1]
        )
        position = position + 2
    leftover = plan_list[position:]
    for pair in leftover:
        residual = residual - operate_near(context, update)
        update = pair[0] * update + pair[1] * residual / diagonal
        solution = solution + update
    return (solution, residual)


def body(conductivity, source):
    coeff_now = conductivity
    contexts = []
    for grid_level in range(LEVELS):
        if grid_level > 0:
            coeff_now = coarsen(coeff_now)
        spacing = float(4**grid_level)
        coeff_ext = padded_2(coeff_now, (("gx", 0), ("gy", 1), ("gz", 2)), 2)
        inside = inside_mask(coeff_now.shape, 1)
        diagonal_ext = jnp.where(inside, diagonal_of(coeff_ext, spacing), 1.0)
        contexts.append((spacing, coeff_ext, diagonal_ext, inside))

    def cycle(grid_level, right_side):
        context = contexts[grid_level]
        if grid_level == LEVELS - 1:
            return relax(context, right_side, None, COARSE_DEGREE, coarse_low, False)
        solution, residual = relax(context, right_side, None, DEGREE, smooth_low, True)
        correction, ignored = cycle(grid_level + 1, coarsen(residual))
        solution = solution + refine(correction)
        return relax(context, right_side, solution, DEGREE, smooth_low, grid_level == 0)

    return cycle(0, source)


def cells(shape, dim):
    return lax.broadcasted_iota(jnp.int32, shape, dim)


def ones_where(condition):
    return jnp.where(condition, 1.0, 0.0).astype(jnp.bfloat16)


def pick(dense, chosen):
    total = None
    for _ in range(3):
        part = dense.astype(jnp.bfloat16)
        dense = dense - part.astype(jnp.float32)
        term = jnp.dot(part, chosen, preferred_element_type=jnp.float32)
        total = term if total is None else total + term
    return total


def turn(values, shift):
    dim = len(values.shape) - 1
    return pltpu.roll(values, shift % values.shape[dim], dim)


def beside(values):
    low, high = turn(values, 1), turn(values, -1)
    tiles = values.shape[0]
    if tiles > 1:
        lane = cells(values.shape, 2)
        low = jnp.where(lane == 0, jnp.concatenate([low[tiles - 1 :], low[: tiles - 1]]), low)
        high = jnp.where(lane == 127, jnp.concatenate([high[1:], high[:1]]), high)
    return low + high


FACE = 14.0 / 3.0


def around_of(before, here, after, tiles):
    faces = before[0] + after[0] + here[1]
    edges = before[1] + after[1]
    inward = FACE * here[0] + faces + (1.0 / 3.0) * edges
    return (FACE * faces + edges)[:tiles] + beside(inward)[:tiles]


class Level:
    def __init__(self, refs, scale):
        self.ks, self.r, self.dg, self.di = refs[:4]
        self.now, self.new = refs[4:6], refs[6:8]
        self.scale = scale

    def grab(self, ref, p, row):
        return (
            ref[p, :, row : row + 8, :],
            ref[p, :, row - 1 : row + 7, :] + ref[p, :, row + 1 : row + 9, :],
        )

    def diagonal(self, raw, span, rows):
        base, count = span
        for row in rows:
            at = slice(row, row + 8)
            before, here = self.grab(raw, base - 1, row), self.grab(raw, base, row)
            for p in (base + j for j in range(count)):
                after = self.grab(raw, p + 1, row)
                near = around_of(before, here, after, raw.shape[1])
                total = self.scale * (128.0 * here[0] + 3.0 * near)
                self.dg[p, :, at, :] = total
                self.di[p, :, at, :] = jnp.where(here[0] > 0.0, 1.0 / total, 0.0)
                self.ks[p, :, at, :] = (3.0 * self.scale) * here[0]
                before, here = here, after

    def first_update(self, span, rows, centre):
        base, count = span
        for row in rows:
            at = slice(row, row + 8)
            for p in (base + j for j in range(count)):
                scaled = self.r[p, :, at, :] * self.di[p, :, at, :]
                self.r[p, :, at, :] = scaled
                fresh = scaled * (1.0 / centre)
                self.now[0][p, :, at, :] = fresh
                self.now[1][p, :, at, :] = fresh * self.ks[p, :, at, :]

    def apply(self, span, rows, pair, tiles=None):
        base, count = span
        tiles = tiles or self.r.shape[1]
        some = slice(0, tiles)
        for row in rows:
            at = slice(row, row + 8)
            before = [self.grab(ref, base - 1, row) for ref in self.now]
            here = [self.grab(ref, base, row) for ref in self.now]
            for p in (base + j for j in range(count)):
                after = [self.grab(ref, p + 1, row) for ref in self.now]
                plain, heavy = (around_of(*parts, tiles) for parts in zip(before, here, after))
                coeff = self.ks[p, some, at, :]
                field = here[0][0][:tiles]
                left = field - self.di[p, some, at, :] * (coeff * plain + heavy)
                left = self.r[p, some, at, :] - left
                self.r[p, some, at, :] = left
                if pair is not None:
                    fresh = pair[1] * left
                    if pair[0] != 0.0:
                        fresh = pair[0] * field + fresh
                    self.new[0][p, some, at, :] = fresh
                    self.new[1][p, some, at, :] = coeff * fresh
                before, here = here, after
        self.now, self.new = self.new, self.now


def kernel(sizes, block, *refs):
    (nx, ny, nz) = sizes
    (bx, by, bz) = block
    deep = 5
    cx, cy = bx // 2, by // 2
    (k_in, b_in, x_out, r_out) = refs[:4]
    (k_raw, k_mid, k_low) = refs[4:7]
    fine = Level(refs[7:15], 0.5 / 30.0)
    mid = Level(refs[15:23], 0.5 / 4.0 / 30.0)
    low = Level(refs[23:31], 0.5 / 16.0 / 30.0)
    (r_near, x_fine, x_mid, x_low, half_sum) = refs[31:36]
    (k_send, b_send, k_edge, b_edge, k_side, b_side) = refs[36:42]
    (z_send, z_got, zr_send, zr_got) = refs[42:46]
    (load_sem, near_send, near_sem, z_sem, zr_sem, far_send, far_sem, chain) = refs[46:54]
    ix, iy, iz = lax.axis_index("gx"), lax.axis_index("gy"), lax.axis_index("gz")
    own = 1 + deep * ix
    other = (1 - ix, iy, iz)
    mine = (pl.ds(own, bx), pl.ds(0, 2), pl.ds(by, by), slice(None))

    def span(width):
        return (own - ix * width, bx + width)

    both, middle = (by // 2, by + by // 2), (by,)

    for ref, target, which in ((k_in, k_raw, 0), (b_in, r_near, 1), (b_in, fine.r, 2)):
        for t in range(2):
            pltpu.make_async_copy(
                ref.at[:, :, pl.ds(128 * t, 128)],
                target.at[pl.ds(own, bx), t, pl.ds(by, by), :],
                load_sem.at[which],
            ).start()

    barrier = pltpu.get_barrier_semaphore()
    z_there = {1: iz + 1 < nz, -1: iz > 0, 0: None}
    y_there = {1: iy + 1 < ny, -1: iy > 0, 0: None}

    def when(*conditions):
        kept = [c for c in conditions if c is not None]
        if not kept:
            return lambda f: f()
        total = kept[0]
        for c in kept[1:]:
            total = total & c
        return pl.when(total)

    def column(skip):
        for jx in range(nx):
            for jy in range(ny):
                if jx or jy or not skip:
                    yield ((ix + jx) % nx, (iy + jy) % ny)

    def counted(number, *conditions):
        for c in conditions:
            if c is not None:
                number = jnp.where(c, number, 0)
        return number

    def greet(target):
        pl.semaphore_signal(barrier, inc=1, device_id=target, device_id_type=MESH)

    peers = 0
    for dz in (0, 1, -1):
        for dy in (0, 1, -1):
            there = (z_there[dz], y_there[dy])
            near = [jx for jx in (ix, 1 - ix) if dz or dy or jx is not ix]

            @when(*there)
            def _():
                for jx in near:
                    greet((jx, iy + dy, iz + dz))

            peers = peers + counted(len(near), *there)

    def clear(ref, *at):
        for p in range(ref.shape[0]):
            ref[(p, *at)] = jnp.zeros(ref[(p, *at)].shape, jnp.float32)

    for p in (0, bx + deep + 1):
        k_raw[p] = jnp.zeros(k_raw.shape[1:], jnp.float32)
    for ref in (k_raw, fine.r, r_near):
        @pl.when(iy == 0)
        def _():
            clear(ref, slice(0, 2), slice(0, by))

        @pl.when(iy == ny - 1)
        def _():
            clear(ref, slice(0, 2), slice(2 * by, 3 * by))

    def blank(ref, dims):
        ref[dims] = jnp.zeros(ref[dims].shape, jnp.float32)

    for ref in (z_got, zr_got):
        for side, gone in ((0, iz == 0), (1, iz == nz - 1)):
            @pl.when(gone)
            def _():
                blank(ref, (side,))

        for j, gone in ((2, iy == 0), (0, iy == ny - 1)):
            @pl.when(gone)
            def _():
                for side in (0, 1):
                    blank(ref, (side, j))
    for ref in (k_side, b_side):
        for side, gone in ((0, iz == 0), (1, iz == nz - 1)):
            @pl.when(gone)
            def _():
                blank(ref, (side,))
    for ref in (*fine.now, *fine.new, *mid.now, *mid.new, *low.now, *low.new, k_low, x_mid):
        clear(ref)
    top = nx * cx + 1
    for p in (0, top):
        k_mid[p] = jnp.zeros(k_mid.shape[1:], jnp.float32)
    for row in (0, ny * cy + 1):
        clear(k_mid, slice(None), slice(row, row + 1))
    half_sum[...] = jnp.zeros(half_sum.shape, jnp.float32)

    own_rows = slice(by, 2 * by)
    lane = cells((8, 128), 1)

    def residual_of(p):
        return fine.r[p, 0:2, own_rows, :] * fine.dg[p, 0:2, own_rows, :]
    shrink = ones_where(cells((256, 128), 0) >> 1 == cells((256, 128), 1))

    def wide(values):
        return jnp.concatenate([values[0], values[1]], axis=1)

    def coarse_block(read, send, edge):
        for q in range(cx):
            p = own + 2 * q
            half_sum[q, :, 0:by, :] = read(p) + read(p + 1)
        rows = [
            wide(
                half_sum[q, :, pl.ds(0, by, stride=2), :]
                + half_sum[q, :, pl.ds(1, by, stride=2), :]
            )
            for q in range(cx)
        ]
        parts = (pick(jnp.concatenate(rows, axis=0), shrink) * 0.125).reshape(cx, by, 128)
        send[...] = parts
        low_part = parts[0]
        top_part = turn(parts[0], 32)
        for q in range(1, cx):
            here = (lane >> 5) == q
            low_part = jnp.where(here, turn(parts[q], 32 * q), low_part)
            top_part = jnp.where(here, turn(parts[q], 32 * q - 96), top_part)
        edge[0, 0:by] = top_part
        edge[1, 0:by] = low_part

    def pack_z(ref, kind, into):
        slot = lane >> 4
        front = (lane & 15) < 8
        packs = [jnp.zeros((8, 128), jnp.float32)] * 2 if into is None else into
        top, bottom = packs
        for q in range(bx):
            here = slot == q
            low_tile = ref[own + q, 0, by : 2 * by, :]
            top_tile = ref[own + q, 1, by : 2 * by, :]
            if kind == 0:
                top = jnp.where(here & front, turn(top_tile, 16 * q - 120), top)
                bottom = jnp.where(
                    here & jnp.logical_not(front), turn(low_tile, 16 * q + 8), bottom
                )
            else:
                after = slot == (q + 1) % 8
                top = jnp.where(
                    here & jnp.logical_not(front), turn(top_tile, 16 * q + 8 - 120), top
                )
                bottom = jnp.where(after & front, turn(low_tile, 16 * q + 16), bottom)
        return (top, bottom)

    def save_z(packs, send):
        for side in (0, 1):
            send[side, 0] = packs[side]
            moved = turn(packs[side], -16 * (bx - deep))
            send[side, 1] = jnp.where(ix == 0, moved, packs[side])

    def remote(source, target, out_sem, in_sem, device):
        return pltpu.make_async_remote_copy(
            src_ref=source,
            dst_ref=target,
            send_sem=out_sem,
            recv_sem=in_sem,
            device_id=device,
            device_id_type=MESH,
        )

    def near_views(ref, depth, dy, start_x, source):
        if dy == 0:
            rows = pl.ds(by, by)
        elif source:
            rows = pl.ds(2 * by - depth, depth) if dy == 1 else pl.ds(by, depth)
        else:
            rows = pl.ds(by - depth, depth) if dy == 1 else pl.ds(2 * by, depth)
        return [
            ref.at[pl.ds(start, planes), pl.ds(0, 2), rows, :]
            for start, planes in ((start_x, depth), (own, bx))
        ]

    def near_start(source, target, depth, along_x, in_sem):
        start_from = jnp.where(ix == 0, bx + 1 - depth, deep + 1)
        start_to = jnp.where(ix == 0, deep + 1 - depth, bx + 1)
        for dy in (0, 1, -1) if along_x else (1, -1):
            @when(y_there[dy])
            def _():
                which = 0 if along_x else 1
                remote(
                    near_views(source, depth, dy, start_from, True)[which],
                    near_views(target, depth, dy, start_to, False)[which],
                    near_send.at[0],
                    in_sem,
                    (1 - ix if along_x else ix, iy + dy, iz),
                ).start()

    inner_y = (iy > 0) & (iy + 1 < ny)
    inner_z = (iz > 0) & (iz + 1 < nz)

    def part_of(ref, rows):
        (p, t, n) = ref.shape[:3]
        sizes = [
            (a, b, rows // (a * b))
            for a in range(1, p + 1)
            for b in range(1, t + 1)
            if rows % (a * b) == 0 and rows // (a * b) <= n
        ]
        (a, b, c) = sizes[0]
        return ref.at[pl.ds(0, a), pl.ds(0, b), pl.ds(0, c), :]

    def wait_rows(ref, out_sem, in_sem, sent, inner, base, each):
        for condition, number in ((inner, 2), (jnp.logical_not(inner), 1)):
            @pl.when(condition)
            def _():
                view = part_of(ref, base + number * each)
                move = remote(view, view, out_sem, in_sem, other)
                if sent:
                    move.wait_send()
                else:
                    move.wait_recv()

    def near_rows(depth, along_x):
        if along_x:
            return 2 * depth * by, 2 * depth * depth
        return 0, 2 * bx * depth

    def near_wait(depth, kinds, in_sem):
        base = sum(near_rows(depth, kind)[0] for kind in kinds)
        each = sum(near_rows(depth, kind)[1] for kind in kinds)
        wait_rows(k_raw, near_send.at[0], in_sem, False, inner_y, base, each)

    def near_sent(depths):
        for depth in depths:
            kinds = [near_rows(depth, kind) for kind in (True, False)]
            base, each = sum(k[0] for k in kinds), sum(k[1] for k in kinds)
            wait_rows(k_raw, near_send.at[0], near_sem.at[0], True, inner_y, base, each)

    def z_start(send, got, sems):
        for side, dz in ((0, 1), (1, -1)):
            for dy in (0, 1, -1):
                @when(z_there[dz], y_there[dy])
                def _():
                    for xi in (0, 1):
                        remote(
                            send.at[side, xi],
                            got.at[side, dy + 1, xi],
                            near_send.at[1 + side],
                            sems.at[side],
                            (ix if xi == 0 else 1 - ix, iy + dy, iz + dz),
                        ).start()

    def z_wait(sems, sent):
        for side, dz in ((0, 1), (1, -1)):
            @pl.when(z_there[dz if sent else -dz])
            def _():
                args = (near_send.at[1 + side], sems.at[side], sent, inner_y, 2 * by, 2 * by)
                wait_rows(k_raw, *args)

    def unpack_z(got, kind, target, count):
        front = (lane & 15) < 8
        kept = (lane < 8) | (lane >= 120)
        start_x = jnp.where(ix == 0, bx + 1, deep + 1 - count)
        skip = 0 if kind == 0 else 8
        for group in range(3):
            for xi, start, planes in ((0, own, bx), (1, None, deep)):
                lower, upper = got[0, 2 - group, xi], got[1, 2 - group, xi]
                pair = (lower, upper) if kind == 0 else (upper, lower)
                merged = jnp.where(front, *pair)
                first = own if xi == 0 else jnp.where(ix == 0, bx + 1, 1)
                for q in range(planes):
                    target[first + q, 2, by * group : by * group + by, :] = jnp.where(
                        kept, turn(merged, -(16 * q + 8 + skip)), 0.0
                    )

    def far_start(send, edge, target, side_target, in_sem):
        for jx, jy in column(True):
            remote(
                send.at[:, pl.ds(0, cy), :],
                target.at[pl.ds(1 + cx * ix, cx), 0, pl.ds(1 + cy * iy, cy), :],
                far_send.at[0],
                in_sem,
                (jx, jy, iz),
            ).start()
        for side, dz in ((0, 1), (1, -1)):
            @when(z_there[dz])
            def _():
                for jx, jy in column(False):
                    remote(
                        edge.at[side, pl.ds(0, cy), :],
                        side_target.at[side, ix, pl.ds(cy * iy, cy), :],
                        far_send.at[0],
                        in_sem,
                        (jx, jy, iz + dz),
                    ).start()

    def far_wait(in_sem, sent=False):
        main, each = (nx * ny - 1) * cx * cy, nx * ny * cy
        wait_rows(k_raw, far_send.at[0], in_sem, sent, inner_z, main, each)

    def keep_own(send, target):
        for jy in range(ny):
            @pl.when(iy == jy)
            def _():
                for q in range(cx):
                    rows = slice(1 + cy * jy, 1 + cy * jy + cy)
                    target[1 + cx * ix + q, 0, rows, :] = send[q, 0:cy, :]

    def unpack_far(side_target, target):
        shape = side_target.shape[2:]
        column_of = cells(shape, 1)
        for jx in range(nx):
            below, above = side_target[0, jx], side_target[1, jx]
            for q in range(cx):
                upper = jnp.where(column_of < 32, turn(above, -32 * q), 0.0)
                target[1 + cx * jx + q, 1, 1 : 1 + shape[0], :] = jnp.where(
                    column_of >= 96, turn(below, 96 - 32 * q), upper
                )

    for which, ref in ((0, k_raw), (1, r_near), (2, fine.r)):
        view = ref.at[mine]
        pltpu.make_async_copy(view, view, load_sem.at[which]).wait()
    save_z(pack_z(fine.r, 1, pack_z(k_raw, 0, None)), z_send)
    pl.semaphore_wait(barrier, peers)

    def pass_on(step):
        for which, dy in ((0, 1), (1, -1)):
            behind = iy - dy * step

            @when(y_there[dy], behind >= 0, behind < ny)
            def _():
                pl.semaphore_signal(
                    chain.at[which], inc=1, device_id=(ix, iy + dy, iz), device_id_type=MESH
                )

    def pass_wait(step):
        for which, dy in ((0, 1), (1, -1)):
            behind = iy - dy * (step + 1)

            @when(behind >= 0, behind < ny)
            def _():
                pl.semaphore_wait(chain.at[which], 1)

    pass_on(1)
    z_start(z_send, z_got, z_sem)
    near_start(k_raw, k_raw, deep, True, near_sem.at[0])
    near_start(k_raw, k_raw, deep, False, near_sem.at[0])
    near_start(r_near, fine.r, deep - 1, False, near_sem.at[1])
    near_start(r_near, fine.r, deep - 1, True, near_sem.at[2])
    coarse_block(lambda p: k_raw[p, 0:2, own_rows, :], k_send, k_edge)
    keep_own(k_send, k_mid)
    for step in range(1, ny - 1):
        pass_wait(step)
        if step + 1 < ny - 1:
            pass_on(step + 1)
    far_start(k_send, k_edge, k_mid, k_side, far_sem.at[0])

    near_wait(deep, (True, False), near_sem.at[0])
    z_wait(z_sem, False)
    unpack_z(z_got, 0, k_raw, deep)
    fine.diagonal(k_raw, span(4), both)
    unpack_z(z_got, 1, fine.r, deep)
    near_wait(deep - 1, (False,), near_sem.at[1])

    def strip(first, last):
        return (bx - last + ix * (deep + 1 + first - bx + last), last - first + 1)

    def add_fine(ref, first=0, last=bx - 1, fresh=False):
        for a in range(first, last + 1):
            q = bx - 1 - a + ix * (2 * a - bx + 1)
            value = ref[own + q, 0:2, own_rows, :]
            x_fine[q] = value if fresh else x_fine[q] + value

    def smooth_fine(first, last, grow):
        for number in range(DEGREE):
            pair = weights[number] if number < DEGREE - 1 else None
            rows, tiles = (both, None) if number < DEGREE - 1 else (middle, 2)
            fine.apply(strip(first, last), rows, pair, tiles)
            if pair is not None:
                add_fine(fine.now[0], max(first, 0), min(last, bx - 1))
            first, last = first + 1, last + grow

    centre, weights = chebyshev_coefs(DEGREE, smooth_low)
    fine.first_update(strip(0, bx - 1), both, centre)
    add_fine(fine.now[0], fresh=True)
    smooth_fine(1, bx - 1, 0)
    near_wait(deep - 1, (True,), near_sem.at[2])
    fine.first_update(strip(-DEGREE, -1), both, centre)
    smooth_fine(1 - DEGREE, 0, 1)

    near_sent((deep, deep - 1))
    z_wait(z_sem, True)
    coarse_block(residual_of, b_send, b_edge)
    far_wait(far_sem.at[0], True)
    far_start(b_send, b_edge, mid.r, b_side, far_sem.at[1])
    keep_own(b_send, mid.r)
    save_z(pack_z(fine.r, 0, None), zr_send)
    z_start(zr_send, zr_got, zr_sem)
    near_start(fine.r, r_near, deep - 1, True, near_sem.at[3])
    near_start(fine.r, r_near, deep - 1, False, near_sem.at[3])
    own_fine = [(q, own + q) for q in range(bx)]
    for q, p in own_fine:
        r_near[p, 0:2, own_rows, :] = fine.r[p, 0:2, own_rows, :]

    mid_span, mid_rows = (1, nx * cx), tuple(range(1, ny * cy, 8))
    low_span, low_rows = (1, nx * cx // 2), tuple(range(1, ny * cy // 2, 8))
    lows = nx * cx // 2
    low_row = ny * cy // 2

    def to_low(read, target):
        rows = []
        for q in range(lows):
            total = None
            for p in (1 + 2 * q, 2 + 2 * q):
                for row in (1, 2):
                    part = read(p, pl.ds(row, low_row, stride=2))
                    total = part if total is None else total + part
            rows.append(wide(total))
        parts = pick(jnp.concatenate(rows, axis=0), shrink) * 0.125
        target[1 : 1 + lows, 0, 1 : 1 + low_row, :] = parts.reshape(lows, low_row, 128)

    far_wait(far_sem.at[0])
    unpack_far(k_side, k_mid)
    mid.diagonal(k_mid, mid_span, mid_rows)
    to_low(lambda p, rows: k_mid[p, :, rows, :], k_low)
    low.diagonal(k_low, low_span, low_rows)

    far_wait(far_sem.at[1])
    unpack_far(b_side, mid.r)
    start = 8
    inside = (slice(1, 1 + nx * cx), slice(None), slice(1, 1 + ny * cy))

    def add_mid(ref, fresh=False):
        for q in range(nx * cx):
            value = ref[1 + q, :, 1 : 1 + ny * cy, :]
            at = (q, slice(None), slice(start, start + ny * cy))
            x_mid[at] = value if fresh else x_mid[at] + value

    mid.first_update(mid_span, mid_rows, centre)
    add_mid(mid.now[0], True)
    for number in range(DEGREE):
        pair = weights[number] if number < DEGREE - 1 else None
        mid.apply(mid_span, mid_rows, pair)
        if pair is not None:
            add_mid(mid.now[0])

    to_low(lambda p, rows: mid.r[p, :, rows, :] * mid.dg[p, :, rows, :], low.r)
    low_centre, low_weights = chebyshev_coefs(COARSE_DEGREE, coarse_low)
    low.first_update(low_span, low_rows, low_centre)

    def low_now():
        return low.now[0][1 : 1 + lows, 0, 1 : 1 + low_row, :]

    x_low[...] = low_now()
    for pair in low_weights:
        low.apply(low_span, low_rows, pair)
        x_low[...] += low_now()

    spread = ones_where(cells((128, 256), 0) == cells((128, 256), 1) >> 1)
    fixed = pick(x_low[...].reshape(lows * low_row, 128), spread).reshape(lows, low_row, 256)
    for q in range(lows):
        for t in range(2):
            value = fixed[q, :, 128 * t : 128 * t + 128]
            for p in (1 + 2 * q, 2 + 2 * q):
                for row in (1, 2):
                    mid.now[0][p, t, pl.ds(row, low_row, stride=2), :] = value
    for p in range(1, 1 + nx * cx):
        at = (p, slice(None), slice(1, 1 + ny * cy))
        mid.now[1][at] = mid.ks[at] * mid.now[0][at]
    add_mid(mid.now[0])
    mid.apply(mid_span, mid_rows, (0.0, 1.0 / centre))
    add_mid(mid.now[0])
    for pair in weights:
        mid.apply(mid_span, mid_rows, pair)
        add_mid(mid.now[0])

    near_wait(deep - 1, (True, False), near_sem.at[3])
    z_wait(zr_sem, False)
    unpack_z(zr_got, 0, r_near, deep)
    shape = (256, 384)
    from_lane, to_lane = cells(shape, 0), cells(shape, 1)
    to_lane = jnp.where(
        to_lane < 256, to_lane >> 1, (to_lane >> 1) + jnp.where(to_lane < 320, 0, 64)
    )
    widen = ones_where(from_lane == to_lane)
    planes = (bx + deep + 1) // 2
    rows = []
    x_rows = 16
    for j in range(planes):
        from_row = start - 3 + cy * iy
        rows.append(wide(x_mid[ix + j, :, pl.ds(from_row, x_rows), :]))
    fixed = pick(jnp.concatenate(rows, axis=0), widen).reshape(planes, x_rows, 384)
    for j in range(planes):
        for t in range(3):
            value = fixed[j, :, 128 * t : 128 * t + 128]
            for p in (0, 1):
                for row in (0, 1):
                    at = 1 - ix + 2 * j + p
                    fine.now[0][at, t, pl.ds(2 + row, 8, stride=2), :] = value[0:8]
                    fine.now[0][at, t, pl.ds(18 + row, 2, stride=2), :] = value[8:10]
    for p in range(1, 1 + bx + deep):
        fine.now[1][p] = (3.0 * fine.scale) * k_raw[p] * fine.now[0][p]
    add_fine(fine.now[0])
    fine.r = r_near
    fine.apply(span(4), both, (0.0, 1.0 / centre))
    add_fine(fine.now[0])
    smooth_fine(1 - DEGREE, bx - 1, 0)
    for q, p in own_fine:
        for t in range(2):
            x_out[q, :, 128 * t : 128 * t + 128] = x_fine[q, t]
            r_out[q, :, 128 * t : 128 * t + 128] = residual_of(p)[t]
    near_sent((deep - 1,))
    z_wait(zr_sem, True)
    far_wait(far_sem.at[1], True)


def gathered(sizes, conductivity, source):
    (nx, ny, nz) = sizes
    (bx, by, bz) = conductivity.shape
    kept = lambda *shape: pltpu.VMEM(shape, jnp.float32)
    fine = kept(bx + 7, 3, 4 * by, 128)
    mid = kept(nx * bx // 2 + 2, 2, ny * by // 2 + 8, 128)
    low = kept(nx * bx // 4 + 2, 1, ny * by // 4 + 8, 128)
    cx, cy = bx // 2, by // 2
    scratch = [fine, mid, low] + [fine] * 8 + [mid] * 8 + [low] * 8
    scratch += [fine, kept(bx, 2, by, 128), kept(nx * cx, 2, ny * cy + 24, 128)]
    scratch += [kept(nx * cx // 2, ny * cy // 2, 128), kept(cx, 2, 2 * by, 128)]
    scratch += [kept(cx, by, 128)] * 2 + [kept(2, 2 * by, 128)] * 2
    scratch += [kept(2, nx, ny * cy, 128)] * 2
    scratch += [kept(2, 2, by, 128), kept(2, 3, 2, by, 128)] * 2
    dma = pltpu.SemaphoreType.DMA
    scratch += [dma((3,)), dma((3,)), dma((4,)), dma((2,)), dma((2,)), dma((1,)), dma((2,))]
    scratch += [pltpu.SemaphoreType.REGULAR((2,))]
    shape = pltpu.VMEM((bx, by, bz), jnp.float32)
    vmem = pl.BlockSpec(memory_space=pltpu.VMEM)
    anywhere = pl.BlockSpec(memory_space=pltpu.HBM)
    return pl.pallas_call(
        functools.partial(kernel, sizes, (bx, by, bz)),
        out_shape=(shape, shape),
        in_specs=[anywhere, anywhere],
        out_specs=(vmem, vmem),
        scratch_shapes=scratch,
        compiler_params=pltpu.CompilerParams(
            collective_id=0, has_side_effects=True, vmem_limit_bytes=66879488
        ),
    )(conductivity, source)


def plan(conductivity, source):
    sizes = tuple(lax.axis_size(axis) for axis in ("gx", "gy", "gz"))
    (bx, by, bz) = conductivity.shape
    fits = (bx, by, bz) == (8, 8, 256) and sizes[0] == 2 and sizes[1] == 4
    if fits:
        return gathered(sizes, conductivity, source)
    return body(conductivity, source)


def solution(mesh):
    in_specs = (P("gx", "gy", "gz"), P("gx", "gy", "gz"))
    out_specs = (P("gx", "gy", "gz"), P("gx", "gy", "gz"))
    return jax.shard_map(plan, mesh=mesh, in_specs=in_specs, out_specs=out_specs, check_vma=False)
```

```python
import functools

import jax
import jax.numpy as jnp
from jax import lax
from jax.experimental import pallas as pl
from jax.experimental.pallas import tpu as pltpu
from jax.sharding import PartitionSpec as P

LEVELS = 3
DEGREE = 4
COARSE_DEGREE = 8
MESH = pl.DeviceIdType.MESH


weight_table = {1: 14.0 / 30.0, 2: 3.0 / 30.0, 3: 1.0 / 30.0}
neighbour_offsets = [
    (along_one, along_two, along_three)
    for along_one in (-1, 0, 1)
    for along_two in (-1, 0, 1)
    for along_three in (-1, 0, 1)
    if (along_one, along_two, along_three) != (0, 0, 0)
]
smooth_low = 0.5
coarse_low = 0.03
upper_bound = 2.0


def padded_2(block, sides, width):
    for axis, dim in sides:
        count = lax.axis_size(axis)
        forward = [(i, i + 1) for i in range(count - 1)]
        backward = [(target, source) for source, target in forward]
        low = lax.ppermute(
            lax.slice_in_dim(block, block.shape[dim] - width, None, axis=dim), axis, forward
        )
        high = lax.ppermute(lax.slice_in_dim(block, 0, width, axis=dim), axis, backward)
        block = jnp.concatenate([low, block, high], axis=dim)
    return block


def shifted(padded, offset):
    return padded[
        1 + offset[0] : padded.shape[0] - 1 + offset[0],
        1 + offset[1] : padded.shape[1] - 1 + offset[1],
        1 + offset[2] : padded.shape[2] - 1 + offset[2],
    ]


def inner(values, margin):
    return values[
        margin : values.shape[0] - margin,
        margin : values.shape[1] - margin,
        margin : values.shape[2] - margin,
    ]


def stencil(field_pad, coeff_pad, spacing):
    centre_field = shifted(field_pad, (0, 0, 0))
    centre_coeff = shifted(coeff_pad, (0, 0, 0))
    total = jnp.zeros(centre_field.shape, jnp.float32)
    for offset in neighbour_offsets:
        weight = weight_table[abs(offset[0]) + abs(offset[1]) + abs(offset[2])]
        total = total + weight * (centre_coeff + shifted(coeff_pad, offset)) * (
            centre_field - shifted(field_pad, offset)
        )
    return total * (0.5 / spacing)


def diagonal_of(coeff_pad, spacing):
    centre_coeff = shifted(coeff_pad, (0, 0, 0))
    total = jnp.zeros(centre_coeff.shape, jnp.float32)
    for offset in neighbour_offsets:
        weight = weight_table[abs(offset[0]) + abs(offset[1]) + abs(offset[2])]
        total = total + weight * (centre_coeff + shifted(coeff_pad, offset))
    return total * (0.5 / spacing)


def coarsen(values):
    extent = values.shape
    return values.reshape(extent[0] // 2, 2, extent[1] // 2, 2, extent[2] // 2, 2).mean(
        axis=(1, 3, 5)
    )


def refine(values):
    return jnp.repeat(jnp.repeat(jnp.repeat(values, 2, axis=0), 2, axis=1), 2, axis=2)


def chebyshev_coefs(degree, lower):
    centre = (upper_bound + lower) / 2.0
    half_width = (upper_bound - lower) / 2.0
    ratio_term = centre / half_width
    rho_prev = 1.0 / ratio_term
    weights = []
    for number in range(1, degree):
        rho_next = 1.0 / (2.0 * ratio_term - rho_prev)
        weights.append((rho_next * rho_prev, 2.0 * rho_next / half_width))
        rho_prev = rho_next
    return (centre, weights)


def inside_mask(extent, margin):
    first_pos = (
        lax.axis_index("gx") * extent[0]
        + jnp.arange(extent[0] + 2 * margin, dtype=jnp.int32)
        - margin
    )
    second_pos = (
        lax.axis_index("gy") * extent[1]
        + jnp.arange(extent[1] + 2 * margin, dtype=jnp.int32)
        - margin
    )
    third_pos = (
        lax.axis_index("gz") * extent[2]
        + jnp.arange(extent[2] + 2 * margin, dtype=jnp.int32)
        - margin
    )
    first_ok = (first_pos >= 0) & (first_pos < extent[0] * lax.axis_size("gx"))
    second_ok = (second_pos >= 0) & (second_pos < extent[1] * lax.axis_size("gy"))
    third_ok = (third_pos >= 0) & (third_pos < extent[2] * lax.axis_size("gz"))
    return first_ok[:, None, None] & second_ok[None, :, None] & third_ok[None, None, :]


def operate_near(context, field):
    spacing, coeff_ext, diagonal_ext, inside = context
    padded = padded_2(field, (("gx", 0), ("gy", 1), ("gz", 2)), 1)
    return stencil(padded, inner(coeff_ext, 1), spacing)


def two_steps(context, solution, residual, update, first_pair, second_pair):
    spacing, coeff_ext, diagonal_ext, inside = context
    diagonal = inner(diagonal_ext, 1)
    stacked = jnp.stack([update, residual])
    padded = padded_2(stacked, (("gx", 1), ("gy", 2), ("gz", 3)), 2)
    update_wide = padded[0]
    residual_wide = padded[1]
    residual_near = inner(residual_wide, 1) - stencil(update_wide, coeff_ext, spacing)
    update_near = (
        first_pair[0] * inner(update_wide, 1) + first_pair[1] * residual_near / diagonal_ext
    )
    update_near = jnp.where(inside, update_near, 0.0)
    solution = solution + inner(update_near, 1)
    residual = inner(residual_near, 1) - stencil(update_near, inner(coeff_ext, 1), spacing)
    if second_pair is None:
        update = inner(update_near, 1)
    else:
        update = second_pair[0] * inner(update_near, 1) + second_pair[1] * residual / diagonal
        solution = solution + update
    return (solution, residual, update)


def relax(context, right_side, start, degree, lower, final):
    diagonal = inner(context[2], 1)
    centre, weights = chebyshev_coefs(degree, lower)
    if start is None:
        residual = right_side
    else:
        residual = right_side - operate_near(context, start)
    update = residual / (centre * diagonal)
    solution = update if start is None else start + update
    plan_list = list(weights) + ([None] if final else [])
    position = 0
    while position + 1 < len(plan_list):
        solution, residual, update = two_steps(
            context, solution, residual, update, plan_list[position], plan_list[position + 1]
        )
        position = position + 2
    leftover = plan_list[position:]
    for pair in leftover:
        residual = residual - operate_near(context, update)
        update = pair[0] * update + pair[1] * residual / diagonal
        solution = solution + update
    return (solution, residual)


def body(conductivity, source):
    coeff_now = conductivity
    contexts = []
    for grid_level in range(LEVELS):
        if grid_level > 0:
            coeff_now = coarsen(coeff_now)
        spacing = float(4**grid_level)
        coeff_ext = padded_2(coeff_now, (("gx", 0), ("gy", 1), ("gz", 2)), 2)
        inside = inside_mask(coeff_now.shape, 1)
        diagonal_ext = jnp.where(inside, diagonal_of(coeff_ext, spacing), 1.0)
        contexts.append((spacing, coeff_ext, diagonal_ext, inside))

    def cycle(grid_level, right_side):
        context = contexts[grid_level]
        if grid_level == LEVELS - 1:
            return relax(context, right_side, None, COARSE_DEGREE, coarse_low, False)
        solution, residual = relax(context, right_side, None, DEGREE, smooth_low, True)
        correction, ignored = cycle(grid_level + 1, coarsen(residual))
        solution = solution + refine(correction)
        return relax(context, right_side, solution, DEGREE, smooth_low, grid_level == 0)

    return cycle(0, source)


def cells(shape, dim):
    return lax.broadcasted_iota(jnp.int32, shape, dim)


def ones_where(condition):
    return jnp.where(condition, 1.0, 0.0).astype(jnp.bfloat16)


def pick(dense, chosen):
    total = None
    for _ in range(3):
        part = dense.astype(jnp.bfloat16)
        dense = dense - part.astype(jnp.float32)
        term = jnp.dot(part, chosen, preferred_element_type=jnp.float32)
        total = term if total is None else total + term
    return total


def turn(values, shift):
    dim = len(values.shape) - 1
    return pltpu.roll(values, shift % values.shape[dim], dim)


def beside(values):
    low, high = turn(values, 1), turn(values, -1)
    tiles = values.shape[0]
    if tiles > 1:
        lane = cells(values.shape, 2)
        low = jnp.where(lane == 0, jnp.concatenate([low[tiles - 1 :], low[: tiles - 1]]), low)
        high = jnp.where(lane == 127, jnp.concatenate([high[1:], high[:1]]), high)
    return low + high


FACE = 14.0 / 3.0


def around_of(before, here, after, tiles):
    faces = before[0] + after[0] + here[1]
    edges = before[1] + after[1]
    inward = FACE * here[0] + faces + (1.0 / 3.0) * edges
    return (FACE * faces + edges)[:tiles] + beside(inward)[:tiles]


class Level:
    def __init__(self, refs, scale):
        self.ks, self.r, self.dg, self.di = refs[:4]
        self.now, self.new = refs[4:6], refs[6:8]
        self.scale = scale

    def grab(self, ref, p, row):
        return (
            ref[p, :, row : row + 8, :],
            ref[p, :, row - 1 : row + 7, :] + ref[p, :, row + 1 : row + 9, :],
        )

    def diagonal(self, raw, span, rows):
        base, count = span
        for row in rows:
            at = slice(row, row + 8)
            before, here = self.grab(raw, base - 1, row), self.grab(raw, base, row)
            for p in (base + j for j in range(count)):
                after = self.grab(raw, p + 1, row)
                near = around_of(before, here, after, raw.shape[1])
                total = self.scale * (128.0 * here[0] + 3.0 * near)
                self.dg[p, :, at, :] = total
                self.di[p, :, at, :] = jnp.where(here[0] > 0.0, 1.0 / total, 0.0)
                self.ks[p, :, at, :] = (3.0 * self.scale) * here[0]
                before, here = here, after

    def first_update(self, span, rows, centre):
        base, count = span
        for row in rows:
            at = slice(row, row + 8)
            for p in (base + j for j in range(count)):
                scaled = self.r[p, :, at, :] * self.di[p, :, at, :]
                self.r[p, :, at, :] = scaled
                fresh = scaled * (1.0 / centre)
                self.now[0][p, :, at, :] = fresh
                self.now[1][p, :, at, :] = fresh * self.ks[p, :, at, :]

    def apply(self, span, rows, pair, tiles=None):
        base, count = span
        tiles = tiles or self.r.shape[1]
        some = slice(0, tiles)
        for row in rows:
            at = slice(row, row + 8)
            before = [self.grab(ref, base - 1, row) for ref in self.now]
            here = [self.grab(ref, base, row) for ref in self.now]
            for p in (base + j for j in range(count)):
                after = [self.grab(ref, p + 1, row) for ref in self.now]
                plain, heavy = (around_of(*parts, tiles) for parts in zip(before, here, after))
                coeff = self.ks[p, some, at, :]
                field = here[0][0][:tiles]
                left = field - self.di[p, some, at, :] * (coeff * plain + heavy)
                left = self.r[p, some, at, :] - left
                self.r[p, some, at, :] = left
                if pair is not None:
                    fresh = pair[1] * left
                    if pair[0] != 0.0:
                        fresh = pair[0] * field + fresh
                    self.new[0][p, some, at, :] = fresh
                    self.new[1][p, some, at, :] = coeff * fresh
                before, here = here, after
        self.now, self.new = self.new, self.now


def kernel(sizes, block, *refs):
    (nx, ny, nz) = sizes
    (bx, by, bz) = block
    deep = 5
    cx, cy = bx // 2, by // 2
    (k_in, b_in, x_out, r_out, d_out) = refs[:5]
    refs = refs[1:]
    (k_raw, k_mid, k_low) = refs[4:7]
    fine = Level(refs[7:15], 0.5 / 30.0)
    mid = Level(refs[15:23], 0.5 / 4.0 / 30.0)
    low = Level(refs[23:31], 0.5 / 16.0 / 30.0)
    (r_near, x_fine, x_mid, x_low, half_sum) = refs[31:36]
    (k_send, b_send, k_edge, b_edge, k_side, b_side) = refs[36:42]
    (z_send, z_passed, z_got, zr_send, zr_passed, zr_got) = refs[42:48]
    (load_sem, near_send, near_sem, z_sem, zr_sem, far_send, far_sem, chain) = refs[48:56]
    ix, iy, iz = lax.axis_index("gx"), lax.axis_index("gy"), lax.axis_index("gz")
    own = 1 + deep * ix
    other = (1 - ix, iy, iz)
    mine = (pl.ds(own, bx), pl.ds(0, 2), pl.ds(by, by), slice(None))

    def span(width):
        return (own - ix * width, bx + width)

    both, middle = (by // 2, by + by // 2), (by,)

    for ref, target, which in ((k_in, k_raw, 0), (b_in, r_near, 1), (b_in, fine.r, 2)):
        for t in range(2):
            pltpu.make_async_copy(
                ref.at[:, :, pl.ds(128 * t, 128)],
                target.at[pl.ds(own, bx), t, pl.ds(by, by), :],
                load_sem.at[which],
            ).start()

    barrier = pltpu.get_barrier_semaphore()
    z_there = {1: iz + 1 < nz, -1: iz > 0, 0: None}
    y_there = {1: iy + 1 < ny, -1: iy > 0, 0: None}

    def when(*conditions):
        kept = [c for c in conditions if c is not None]
        if not kept:
            return lambda f: f()
        total = kept[0]
        for c in kept[1:]:
            total = total & c
        return pl.when(total)

    def column(skip):
        for jx in range(nx):
            for jy in range(ny):
                if jx or jy or not skip:
                    yield ((ix + jx) % nx, (iy + jy) % ny)

    def counted(number, *conditions):
        for c in conditions:
            if c is not None:
                number = jnp.where(c, number, 0)
        return number

    def greet(target):
        pl.semaphore_signal(barrier, inc=1, device_id=target, device_id_type=MESH)

    peers = 0
    for dz, dys in ((0, (0, 1, -1)), (1, (0,)), (-1, (0,))):
        for dy in dys:
            there = (z_there[dz], y_there[dy])
            near = [ix] if dz else [jx for jx in (ix, 1 - ix) if dy or jx is not ix]

            @when(*there)
            def _():
                for jx in near:
                    greet((jx, iy + dy, iz + dz))

            peers = peers + counted(len(near), *there)

    def clear(ref, *at):
        for p in range(ref.shape[0]):
            ref[(p, *at)] = jnp.zeros(ref[(p, *at)].shape, jnp.float32)

    for p in (0, bx + deep + 1):
        k_raw[p] = jnp.zeros(k_raw.shape[1:], jnp.float32)
    for ref in (k_raw, fine.r, r_near):
        @pl.when(iy == 0)
        def _():
            clear(ref, slice(0, 2), slice(0, by))

        @pl.when(iy == ny - 1)
        def _():
            clear(ref, slice(0, 2), slice(2 * by, 3 * by))

    def blank(ref, dims):
        ref[dims] = jnp.zeros(ref[dims].shape, jnp.float32)

    for ref, passed in ((z_got, z_passed), (zr_got, zr_passed)):
        for side, gone in ((0, iz == 0), (1, iz == nz - 1)):
            @pl.when(gone)
            def _():
                blank(ref, (side,))
                blank(passed, (side,))

        for j, gone in ((2, iy == 0), (0, iy == ny - 1)):
            @pl.when(gone)
            def _():
                for side in (0, 1):
                    blank(ref, (side, j))
    for ref in (k_side, b_side):
        for side, gone in ((0, iz == 0), (1, iz == nz - 1)):
            @pl.when(gone)
            def _():
                blank(ref, (side,))
    for ref in (*fine.now, *fine.new, *mid.now, *mid.new, *low.now, *low.new, k_low, x_mid):
        clear(ref)
    top = nx * cx + 1
    for p in (0, top):
        k_mid[p] = jnp.zeros(k_mid.shape[1:], jnp.float32)
    for row in (0, ny * cy + 1):
        clear(k_mid, slice(None), slice(row, row + 1))
    half_sum[...] = jnp.zeros(half_sum.shape, jnp.float32)

    own_rows = slice(by, 2 * by)
    lane = cells((8, 128), 1)

    def residual_of(p):
        return fine.r[p, 0:2, own_rows, :] * fine.dg[p, 0:2, own_rows, :]
    shrink = ones_where(cells((256, 128), 0) >> 1 == cells((256, 128), 1))

    def wide(values):
        return jnp.concatenate([values[0], values[1]], axis=1)

    def coarse_block(read, send):
        for q in range(cx):
            p = own + 2 * q
            half_sum[q, :, 0:by, :] = read(p) + read(p + 1)
        rows = [
            wide(
                half_sum[q, :, pl.ds(0, by, stride=2), :]
                + half_sum[q, :, pl.ds(1, by, stride=2), :]
            )
            for q in range(cx)
        ]
        parts = (pick(jnp.concatenate(rows, axis=0), shrink) * 0.125).reshape(cx, by, 128)
        send[...] = parts
        return parts

    def coarse_edge(parts, edge):
        low_part = parts[0]
        top_part = turn(parts[0], 32)
        for q in range(1, cx):
            here = (lane >> 5) == q
            low_part = jnp.where(here, turn(parts[q], 32 * q), low_part)
            top_part = jnp.where(here, turn(parts[q], 32 * q - 96), top_part)
        edge[0, 0:by] = top_part
        edge[1, 0:by] = low_part

    def pack_z(ref, kind, into):
        slot = lane >> 4
        front = (lane & 15) < 8
        packs = [jnp.zeros((8, 128), jnp.float32)] * 2 if into is None else into
        top, bottom = packs
        for q in range(bx):
            here = slot == q
            low_tile = ref[own + q, 0, by : 2 * by, :]
            top_tile = ref[own + q, 1, by : 2 * by, :]
            if kind == 0:
                top = jnp.where(here & front, turn(top_tile, 16 * q - 120), top)
                bottom = jnp.where(
                    here & jnp.logical_not(front), turn(low_tile, 16 * q + 8), bottom
                )
            else:
                after = slot == (q + 1) % 8
                top = jnp.where(
                    here & jnp.logical_not(front), turn(top_tile, 16 * q + 8 - 120), top
                )
                bottom = jnp.where(after & front, turn(low_tile, 16 * q + 16), bottom)
        return (top, bottom)

    def save_z(packs, send):
        for side in (0, 1):
            send[side, 0] = packs[side]
            moved = turn(packs[side], -16 * (bx - deep))
            send[side, 1] = jnp.where(ix == 0, moved, packs[side])

    def remote(source, target, out_sem, in_sem, device):
        return pltpu.make_async_remote_copy(
            src_ref=source,
            dst_ref=target,
            send_sem=out_sem,
            recv_sem=in_sem,
            device_id=device,
            device_id_type=MESH,
        )

    def near_views(ref, depth, dy, start_x, source):
        if dy == 0:
            rows = pl.ds(by, by)
        elif source:
            rows = pl.ds(2 * by - depth, depth) if dy == 1 else pl.ds(by, depth)
        else:
            rows = pl.ds(by - depth, depth) if dy == 1 else pl.ds(2 * by, depth)
        return [
            ref.at[pl.ds(start, planes), pl.ds(0, 2), rows, :]
            for start, planes in ((start_x, depth), (own, bx))
        ]

    def near_start(source, target, depth, along_x, in_sem):
        start_from = jnp.where(ix == 0, bx + 1 - depth, deep + 1)
        start_to = jnp.where(ix == 0, deep + 1 - depth, bx + 1)
        for dy in (0, 1, -1) if along_x else (1, -1):
            @when(y_there[dy])
            def _():
                which = 0 if along_x else 1
                remote(
                    near_views(source, depth, dy, start_from, True)[which],
                    near_views(target, depth, dy, start_to, False)[which],
                    near_send.at[0],
                    in_sem,
                    (1 - ix if along_x else ix, iy + dy, iz),
                ).start()

    inner_y = (iy > 0) & (iy + 1 < ny)
    inner_z = (iz > 0) & (iz + 1 < nz)

    def part_of(ref, rows):
        (p, t, n) = ref.shape[:3]
        sizes = [
            (a, b, rows // (a * b))
            for a in range(1, p + 1)
            for b in range(1, t + 1)
            if rows % (a * b) == 0 and rows // (a * b) <= n
        ]
        (a, b, c) = sizes[0]
        return ref.at[pl.ds(0, a), pl.ds(0, b), pl.ds(0, c), :]

    def wait_rows(ref, out_sem, in_sem, sent, inner, base, each):
        for condition, number in ((inner, 2), (jnp.logical_not(inner), 1)):
            @pl.when(condition)
            def _():
                view = part_of(ref, base + number * each)
                move = remote(view, view, out_sem, in_sem, other)
                if sent:
                    move.wait_send()
                else:
                    move.wait_recv()

    def near_rows(depth, along_x):
        if along_x:
            return 2 * depth * by, 2 * depth * depth
        return 0, 2 * bx * depth

    def near_wait(depth, kinds, in_sem):
        base = sum(near_rows(depth, kind)[0] for kind in kinds)
        each = sum(near_rows(depth, kind)[1] for kind in kinds)
        wait_rows(k_raw, near_send.at[0], in_sem, False, inner_y, base, each)

    def near_sent(depths):
        for depth in depths:
            kinds = [near_rows(depth, kind) for kind in (True, False)]
            base, each = sum(k[0] for k in kinds), sum(k[1] for k in kinds)
            wait_rows(k_raw, near_send.at[0], near_sem.at[0], True, inner_y, base, each)

    def z_start(send, passed, sems):
        for side, dz in ((0, 1), (1, -1)):
            @pl.when(z_there[dz])
            def _():
                remote(
                    send.at[side],
                    passed.at[side],
                    near_send.at[1 + side],
                    sems.at[side],
                    (ix, iy, iz + dz),
                ).start()

    def z_pass_on(passed, got, sems):
        for side, dz in ((0, 1), (1, -1)):
            @pl.when(z_there[-dz])
            def _():
                view = passed.at[side]
                remote(view, view, near_send.at[1 + side], sems.at[side], other).wait_recv()
                for dy in (0, 1, -1):
                    @when(y_there[dy])
                    def _():
                        for xi in (0, 1) if dy else (1,):
                            remote(
                                passed.at[side, xi],
                                got.at[side, dy + 1, xi],
                                near_send.at[3 + side],
                                sems.at[2 + side],
                                (ix if xi == 0 else 1 - ix, iy + dy, iz),
                            ).start()

    def z_wait(passed, sems, sent):
        for side, dz in ((0, 1), (1, -1)):
            @pl.when(z_there[-dz])
            def _():
                args = (near_send.at[3 + side], sems.at[2 + side], sent, inner_y, by, 2 * by)
                wait_rows(k_raw, *args)

            if sent:
                @pl.when(z_there[dz])
                def _():
                    view = passed.at[side]
                    remote(view, view, near_send.at[1 + side], sems.at[side], other).wait_send()

    def unpack_z(passed, got, kind, target):
        front = (lane & 15) < 8
        kept = (lane < 8) | (lane >= 120)
        skip = 0 if kind == 0 else 8
        for group in range(3):
            for xi, planes in ((0, bx), (1, deep)):
                straight = group == 1 and xi == 0
                lower, upper = (
                    passed[side, 0] if straight else got[side, 2 - group, xi] for side in (0, 1)
                )
                pair = (lower, upper) if kind == 0 else (upper, lower)
                merged = jnp.where(front, *pair)
                first = own if xi == 0 else jnp.where(ix == 0, bx + 1, 1)
                for q in range(planes):
                    target[first + q, 2, by * group : by * group + by, :] = jnp.where(
                        kept, turn(merged, -(16 * q + 8 + skip)), 0.0
                    )

    def far_start(send, target, in_sem):
        for jx, jy in reversed(list(column(True))):
            remote(
                send.at[:, pl.ds(0, cy), :],
                target.at[pl.ds(1 + cx * ix, cx), 0, pl.ds(1 + cy * iy, cy), :],
                far_send.at[0],
                in_sem,
                (jx, jy, iz),
            ).start()

    def far_start_sides(edge, side_target, in_sem):
        for side, dz in ((0, 1), (1, -1)):
            @when(z_there[dz])
            def _():
                for jx, jy in reversed(list(column(False))):
                    remote(
                        edge.at[side, pl.ds(0, cy), :],
                        side_target.at[side, ix, pl.ds(cy * iy, cy), :],
                        far_send.at[0],
                        in_sem,
                        (jx, jy, iz + dz),
                    ).start()

    def far_wait(in_sem, sent=False):
        main, each = (nx * ny - 1) * cx * cy, nx * ny * cy
        wait_rows(k_raw, far_send.at[0], in_sem, sent, inner_z, main, each)

    def keep_own(send, target):
        for jy in range(ny):
            @pl.when(iy == jy)
            def _():
                for q in range(cx):
                    rows = slice(1 + cy * jy, 1 + cy * jy + cy)
                    target[1 + cx * ix + q, 0, rows, :] = send[q, 0:cy, :]

    def unpack_far(side_target, target):
        shape = side_target.shape[2:]
        column_of = cells(shape, 1)
        for jx in range(nx):
            below, above = side_target[0, jx], side_target[1, jx]
            for q in range(cx):
                upper = jnp.where(column_of < 32, turn(above, -32 * q), 0.0)
                target[1 + cx * jx + q, 1, 1 : 1 + shape[0], :] = jnp.where(
                    column_of >= 96, turn(below, 96 - 32 * q), upper
                )

    for which, ref in ((0, k_raw), (1, r_near), (2, fine.r)):
        view = ref.at[mine]
        pltpu.make_async_copy(view, view, load_sem.at[which]).wait()
    save_z(pack_z(fine.r, 1, pack_z(k_raw, 0, None)), z_send)
    pl.semaphore_wait(barrier, peers)

    def pass_on(step):
        for which, dy in ((0, 1), (1, -1)):
            behind = iy - dy * step

            @when(y_there[dy], behind >= 0, behind < ny)
            def _():
                pl.semaphore_signal(
                    chain.at[which], inc=1, device_id=(ix, iy + dy, iz), device_id_type=MESH
                )

    def pass_wait(step):
        for which, dy in ((0, 1), (1, -1)):
            behind = iy - dy * (step + 1)

            @when(behind >= 0, behind < ny)
            def _():
                pl.semaphore_wait(chain.at[which], 1)

    z_start(z_send, z_passed, z_sem)
    near_start(k_raw, k_raw, deep, True, near_sem.at[0])
    near_start(k_raw, k_raw, deep, False, near_sem.at[0])
    pass_on(1)
    coarse_edge(coarse_block(lambda p: k_raw[p, 0:2, own_rows, :], k_send), k_edge)
    keep_own(k_send, k_mid)
    z_pass_on(z_passed, z_got, z_sem)
    near_start(r_near, fine.r, deep - 1, False, near_sem.at[1])
    near_start(r_near, fine.r, deep - 1, True, near_sem.at[2])
    for step in range(1, ny - 1):
        pass_wait(step)
        if step + 1 < ny - 1:
            pass_on(step + 1)
    for side, dz in ((0, 1), (1, -1)):
        @pl.when(z_there[dz])
        def _():
            pl.semaphore_signal(
                chain.at[2 + side], inc=1, device_id=(ix, iy, iz + dz), device_id_type=MESH
            )

    near_wait(deep, (True, False), near_sem.at[0])
    for side, dz in ((0, 1), (1, -1)):
        @pl.when(z_there[-dz])
        def _():
            pl.semaphore_wait(chain.at[2 + side], 1)

    far_start(k_send, k_mid, far_sem.at[0])
    far_start_sides(k_edge, k_side, far_sem.at[0])
    z_wait(z_passed, z_sem, False)
    unpack_z(z_passed, z_got, 0, k_raw)
    fine.diagonal(k_raw, span(4), both)
    unpack_z(z_passed, z_got, 1, fine.r)
    near_wait(deep - 1, (False,), near_sem.at[1])

    def strip(first, last):
        return (bx - last + ix * (deep + 1 + first - bx + last), last - first + 1)

    def add_fine(ref, first=0, last=bx - 1, fresh=False):
        for a in range(first, last + 1):
            q = bx - 1 - a + ix * (2 * a - bx + 1)
            value = ref[own + q, 0:2, own_rows, :]
            x_fine[q] = value if fresh else x_fine[q] + value

    def smooth_fine(first, last, grow, added):
        for number in range(DEGREE):
            pair = weights[number] if number < DEGREE - 1 else None
            rows, tiles = (both, None) if number < DEGREE - 1 else (middle, 2)
            fine.apply(strip(first, last), rows, pair, tiles)
            if pair is not None and number < added:
                add_fine(fine.now[0], max(first, 0), min(last, bx - 1))
            first, last = first + 1, last + grow

    centre, weights = chebyshev_coefs(DEGREE, smooth_low)
    near_wait(deep - 1, (True,), near_sem.at[2])
    fine.first_update(strip(-DEGREE, bx - 1), both, centre)
    add_fine(fine.now[0], fresh=True)
    smooth_fine(1 - DEGREE, bx - 1, 0, DEGREE)

    far_wait(far_sem.at[0], True)
    parts = coarse_block(residual_of, b_send)
    far_start(b_send, mid.r, far_sem.at[1])
    coarse_edge(parts, b_edge)
    far_start_sides(b_edge, b_side, far_sem.at[1])
    near_sent((deep, deep - 1))
    z_wait(z_passed, z_sem, True)
    keep_own(b_send, mid.r)
    save_z(pack_z(fine.r, 0, None), zr_send)
    z_start(zr_send, zr_passed, zr_sem)
    near_start(fine.r, r_near, deep - 1, True, near_sem.at[3])
    near_start(fine.r, r_near, deep - 1, False, near_sem.at[3])
    own_fine = [(q, own + q) for q in range(bx)]
    for q, p in own_fine:
        r_near[p, 0:2, own_rows, :] = fine.r[p, 0:2, own_rows, :]

    mid_span, mid_rows = (1, nx * cx), tuple(range(1, ny * cy, 8))
    low_span, low_rows = (1, nx * cx // 2), tuple(range(1, ny * cy // 2, 8))
    lows = nx * cx // 2
    low_row = ny * cy // 2

    def to_low(read, target):
        rows = []
        for q in range(lows):
            total = None
            for p in (1 + 2 * q, 2 + 2 * q):
                for row in (1, 2):
                    part = read(p, pl.ds(row, low_row, stride=2))
                    total = part if total is None else total + part
            rows.append(wide(total))
        parts = pick(jnp.concatenate(rows, axis=0), shrink) * 0.125
        target[1 : 1 + lows, 0, 1 : 1 + low_row, :] = parts.reshape(lows, low_row, 128)

    far_wait(far_sem.at[0])
    unpack_far(k_side, k_mid)
    mid.diagonal(k_mid, mid_span, mid_rows)
    to_low(lambda p, rows: k_mid[p, :, rows, :], k_low)
    low.diagonal(k_low, low_span, low_rows)

    z_pass_on(zr_passed, zr_got, zr_sem)
    far_wait(far_sem.at[1])
    unpack_far(b_side, mid.r)
    start = 8
    inside = (slice(1, 1 + nx * cx), slice(None), slice(1, 1 + ny * cy))

    def add_mid(ref, fresh=False):
        for q in range(nx * cx):
            value = ref[1 + q, :, 1 : 1 + ny * cy, :]
            at = (q, slice(None), slice(start, start + ny * cy))
            x_mid[at] = value if fresh else x_mid[at] + value

    mid.first_update(mid_span, mid_rows, centre)
    add_mid(mid.now[0], True)
    for number in range(DEGREE):
        pair = weights[number] if number < DEGREE - 1 else None
        mid.apply(mid_span, mid_rows, pair)
        if pair is not None:
            add_mid(mid.now[0])

    to_low(lambda p, rows: mid.r[p, :, rows, :] * mid.dg[p, :, rows, :], low.r)
    low_centre, low_weights = chebyshev_coefs(COARSE_DEGREE, coarse_low)
    near_wait(deep - 1, (True, False), near_sem.at[3])
    z_wait(zr_passed, zr_sem, False)
    low.first_update(low_span, low_rows, low_centre)
    unpack_z(zr_passed, zr_got, 0, r_near)

    def low_now():
        return low.now[0][1 : 1 + lows, 0, 1 : 1 + low_row, :]

    x_low[...] = low_now()
    for pair in low_weights:
        low.apply(low_span, low_rows, pair)
        x_low[...] += low_now()

    spread = ones_where(cells((128, 256), 0) == cells((128, 256), 1) >> 1)
    fixed = pick(x_low[...].reshape(lows * low_row, 128), spread).reshape(lows, low_row, 256)
    for q in range(lows):
        for t in range(2):
            value = fixed[q, :, 128 * t : 128 * t + 128]
            for p in (1 + 2 * q, 2 + 2 * q):
                for row in (1, 2):
                    mid.now[0][p, t, pl.ds(row, low_row, stride=2), :] = value
    for p in range(1, 1 + nx * cx):
        at = (p, slice(None), slice(1, 1 + ny * cy))
        mid.now[1][at] = mid.ks[at] * mid.now[0][at]
    add_mid(mid.now[0])
    mid.apply(mid_span, mid_rows, (0.0, 1.0 / centre))
    add_mid(mid.now[0])
    for pair in weights:
        mid.apply(mid_span, mid_rows, pair)
        add_mid(mid.now[0])

    shape = (256, 384)
    from_lane, to_lane = cells(shape, 0), cells(shape, 1)
    to_lane = jnp.where(
        to_lane < 256, to_lane >> 1, (to_lane >> 1) + jnp.where(to_lane < 320, 0, 64)
    )
    widen = ones_where(from_lane == to_lane)
    planes = (bx + deep + 1) // 2
    rows = []
    x_rows = 16
    for j in range(planes):
        from_row = start - 3 + cy * iy
        rows.append(wide(x_mid[ix + j, :, pl.ds(from_row, x_rows), :]))
    fixed = pick(jnp.concatenate(rows, axis=0), widen).reshape(planes, x_rows, 384)
    for j in range(planes):
        for t in range(3):
            value = fixed[j, :, 128 * t : 128 * t + 128]
            for p in (0, 1):
                for row in (0, 1):
                    at = 1 - ix + 2 * j + p
                    fine.now[0][at, t, pl.ds(2 + row, 8, stride=2), :] = value[0:8]
                    fine.now[0][at, t, pl.ds(18 + row, 2, stride=2), :] = value[8:10]
    for p in range(1, 1 + bx + deep):
        fine.now[1][p] = (3.0 * fine.scale) * k_raw[p] * fine.now[0][p]
    add_fine(fine.now[0])
    fine.r = r_near
    fine.apply(span(4), both, (0.0, 1.0 / centre))
    add_fine(fine.now[0])
    smooth_fine(1 - DEGREE, bx - 1, 0, DEGREE - 2)
    for q, p in own_fine:
        last, left = fine.new[0][p, 0:2, own_rows, :], residual_of(p)
        for t in range(2):
            at = (q, slice(None), slice(128 * t, 128 * t + 128))
            x_out[at] = x_fine[q, t]
            d_out[at] = last[t]
            r_out[at] = left[t] - last[t]
    near_sent((deep - 1,))
    z_wait(zr_passed, zr_sem, True)
    far_wait(far_sem.at[1], True)


def gathered(sizes, conductivity, source):
    (nx, ny, nz) = sizes
    (bx, by, bz) = conductivity.shape
    kept = lambda *shape: pltpu.VMEM(shape, jnp.float32)
    fine = kept(bx + 7, 3, 3 * by, 128)
    mid = kept(nx * bx // 2 + 2, 2, ny * by // 2 + 8, 128)
    low = kept(nx * bx // 4 + 2, 1, ny * by // 4 + 8, 128)
    cx, cy = bx // 2, by // 2
    scratch = [fine, mid, low] + [fine] * 8 + [mid] * 8 + [low] * 8
    scratch += [fine, kept(bx, 2, by, 128), kept(nx * cx, 2, ny * cy + 24, 128)]
    scratch += [kept(nx * cx // 2, ny * cy // 2, 128), kept(cx, 2, 2 * by, 128)]
    scratch += [kept(cx, by, 128)] * 2 + [kept(2, 2 * by, 128)] * 2
    scratch += [kept(2, nx, ny * cy, 128)] * 2
    scratch += [kept(2, 2, by, 128), kept(2, 2, by, 128), kept(2, 3, 2, by, 128)] * 2
    dma = pltpu.SemaphoreType.DMA
    scratch += [dma((3,)), dma((5,)), dma((4,)), dma((4,)), dma((4,)), dma((1,)), dma((2,))]
    scratch += [pltpu.SemaphoreType.REGULAR((4,))]
    shape = pltpu.VMEM((bx, by, bz), jnp.float32)
    vmem = pl.BlockSpec(memory_space=pltpu.VMEM)
    anywhere = pl.BlockSpec(memory_space=pltpu.HBM)
    x_part, r_part, last = pl.pallas_call(
        functools.partial(kernel, sizes, (bx, by, bz)),
        out_shape=(shape,) * 3,
        in_specs=[anywhere, anywhere],
        out_specs=(vmem,) * 3,
        scratch_shapes=scratch,
        compiler_params=pltpu.CompilerParams(
            collective_id=0, has_side_effects=True, vmem_limit_bytes=66715648
        ),
    )(conductivity, source)
    return x_part + last, r_part + last


def plan(conductivity, source):
    sizes = tuple(lax.axis_size(axis) for axis in ("gx", "gy", "gz"))
    (bx, by, bz) = conductivity.shape
    fits = (bx, by, bz) == (8, 8, 256) and sizes[0] == 2 and sizes[1] == 4
    if fits:
        return gathered(sizes, conductivity, source)
    return body(conductivity, source)


def solution(mesh):
    in_specs = (P("gx", "gy", "gz"), P("gx", "gy", "gz"))
    out_specs = (P("gx", "gy", "gz"), P("gx", "gy", "gz"))
    return jax.shard_map(plan, mesh=mesh, in_specs=in_specs, out_specs=out_specs, check_vma=False)
```

```python
import functools

import jax
import jax.numpy as jnp
from jax import lax
from jax.experimental import pallas as pl
from jax.experimental.pallas import tpu as pltpu
from jax.sharding import PartitionSpec as P

LEVELS = 3
DEGREE = 4
COARSE_DEGREE = 8
MESH = pl.DeviceIdType.MESH


weight_table = {1: 14.0 / 30.0, 2: 3.0 / 30.0, 3: 1.0 / 30.0}
neighbour_offsets = [
    (along_one, along_two, along_three)
    for along_one in (-1, 0, 1)
    for along_two in (-1, 0, 1)
    for along_three in (-1, 0, 1)
    if (along_one, along_two, along_three) != (0, 0, 0)
]
smooth_low = 0.5
coarse_low = 0.03
upper_bound = 2.0


def padded_2(block, sides, width):
    for axis, dim in sides:
        count = lax.axis_size(axis)
        forward = [(i, i + 1) for i in range(count - 1)]
        backward = [(target, source) for source, target in forward]
        low = lax.ppermute(
            lax.slice_in_dim(block, block.shape[dim] - width, None, axis=dim), axis, forward
        )
        high = lax.ppermute(lax.slice_in_dim(block, 0, width, axis=dim), axis, backward)
        block = jnp.concatenate([low, block, high], axis=dim)
    return block


def shifted(padded, offset):
    return padded[
        1 + offset[0] : padded.shape[0] - 1 + offset[0],
        1 + offset[1] : padded.shape[1] - 1 + offset[1],
        1 + offset[2] : padded.shape[2] - 1 + offset[2],
    ]


def inner(values, margin):
    return values[
        margin : values.shape[0] - margin,
        margin : values.shape[1] - margin,
        margin : values.shape[2] - margin,
    ]


def stencil(field_pad, coeff_pad, spacing):
    centre_field = shifted(field_pad, (0, 0, 0))
    centre_coeff = shifted(coeff_pad, (0, 0, 0))
    total = jnp.zeros(centre_field.shape, jnp.float32)
    for offset in neighbour_offsets:
        weight = weight_table[abs(offset[0]) + abs(offset[1]) + abs(offset[2])]
        total = total + weight * (centre_coeff + shifted(coeff_pad, offset)) * (
            centre_field - shifted(field_pad, offset)
        )
    return total * (0.5 / spacing)


def diagonal_of(coeff_pad, spacing):
    centre_coeff = shifted(coeff_pad, (0, 0, 0))
    total = jnp.zeros(centre_coeff.shape, jnp.float32)
    for offset in neighbour_offsets:
        weight = weight_table[abs(offset[0]) + abs(offset[1]) + abs(offset[2])]
        total = total + weight * (centre_coeff + shifted(coeff_pad, offset))
    return total * (0.5 / spacing)


def coarsen(values):
    extent = values.shape
    return values.reshape(extent[0] // 2, 2, extent[1] // 2, 2, extent[2] // 2, 2).mean(
        axis=(1, 3, 5)
    )


def refine(values):
    return jnp.repeat(jnp.repeat(jnp.repeat(values, 2, axis=0), 2, axis=1), 2, axis=2)


def chebyshev_coefs(degree, lower):
    centre = (upper_bound + lower) / 2.0
    half_width = (upper_bound - lower) / 2.0
    ratio_term = centre / half_width
    rho_prev = 1.0 / ratio_term
    weights = []
    for number in range(1, degree):
        rho_next = 1.0 / (2.0 * ratio_term - rho_prev)
        weights.append((rho_next * rho_prev, 2.0 * rho_next / half_width))
        rho_prev = rho_next
    return (centre, weights)


def inside_mask(extent, margin):
    first_pos = (
        lax.axis_index("gx") * extent[0]
        + jnp.arange(extent[0] + 2 * margin, dtype=jnp.int32)
        - margin
    )
    second_pos = (
        lax.axis_index("gy") * extent[1]
        + jnp.arange(extent[1] + 2 * margin, dtype=jnp.int32)
        - margin
    )
    third_pos = (
        lax.axis_index("gz") * extent[2]
        + jnp.arange(extent[2] + 2 * margin, dtype=jnp.int32)
        - margin
    )
    first_ok = (first_pos >= 0) & (first_pos < extent[0] * lax.axis_size("gx"))
    second_ok = (second_pos >= 0) & (second_pos < extent[1] * lax.axis_size("gy"))
    third_ok = (third_pos >= 0) & (third_pos < extent[2] * lax.axis_size("gz"))
    return first_ok[:, None, None] & second_ok[None, :, None] & third_ok[None, None, :]


def operate_near(context, field):
    spacing, coeff_ext, diagonal_ext, inside = context
    padded = padded_2(field, (("gx", 0), ("gy", 1), ("gz", 2)), 1)
    return stencil(padded, inner(coeff_ext, 1), spacing)


def two_steps(context, solution, residual, update, first_pair, second_pair):
    spacing, coeff_ext, diagonal_ext, inside = context
    diagonal = inner(diagonal_ext, 1)
    stacked = jnp.stack([update, residual])
    padded = padded_2(stacked, (("gx", 1), ("gy", 2), ("gz", 3)), 2)
    update_wide = padded[0]
    residual_wide = padded[1]
    residual_near = inner(residual_wide, 1) - stencil(update_wide, coeff_ext, spacing)
    update_near = (
        first_pair[0] * inner(update_wide, 1) + first_pair[1] * residual_near / diagonal_ext
    )
    update_near = jnp.where(inside, update_near, 0.0)
    solution = solution + inner(update_near, 1)
    residual = inner(residual_near, 1) - stencil(update_near, inner(coeff_ext, 1), spacing)
    if second_pair is None:
        update = inner(update_near, 1)
    else:
        update = second_pair[0] * inner(update_near, 1) + second_pair[1] * residual / diagonal
        solution = solution + update
    return (solution, residual, update)


def relax(context, right_side, start, degree, lower, final):
    diagonal = inner(context[2], 1)
    centre, weights = chebyshev_coefs(degree, lower)
    if start is None:
        residual = right_side
    else:
        residual = right_side - operate_near(context, start)
    update = residual / (centre * diagonal)
    solution = update if start is None else start + update
    plan_list = list(weights) + ([None] if final else [])
    position = 0
    while position + 1 < len(plan_list):
        solution, residual, update = two_steps(
            context, solution, residual, update, plan_list[position], plan_list[position + 1]
        )
        position = position + 2
    leftover = plan_list[position:]
    for pair in leftover:
        residual = residual - operate_near(context, update)
        update = pair[0] * update + pair[1] * residual / diagonal
        solution = solution + update
    return (solution, residual)


def body(conductivity, source):
    coeff_now = conductivity
    contexts = []
    for grid_level in range(LEVELS):
        if grid_level > 0:
            coeff_now = coarsen(coeff_now)
        spacing = float(4**grid_level)
        coeff_ext = padded_2(coeff_now, (("gx", 0), ("gy", 1), ("gz", 2)), 2)
        inside = inside_mask(coeff_now.shape, 1)
        diagonal_ext = jnp.where(inside, diagonal_of(coeff_ext, spacing), 1.0)
        contexts.append((spacing, coeff_ext, diagonal_ext, inside))

    def cycle(grid_level, right_side):
        context = contexts[grid_level]
        if grid_level == LEVELS - 1:
            return relax(context, right_side, None, COARSE_DEGREE, coarse_low, False)
        solution, residual = relax(context, right_side, None, DEGREE, smooth_low, True)
        correction, ignored = cycle(grid_level + 1, coarsen(residual))
        solution = solution + refine(correction)
        return relax(context, right_side, solution, DEGREE, smooth_low, grid_level == 0)

    return cycle(0, source)


def cells(shape, dim):
    return lax.broadcasted_iota(jnp.int32, shape, dim)


def ones_where(condition):
    return jnp.where(condition, 1.0, 0.0).astype(jnp.bfloat16)


def pick(dense, chosen, parts=2):
    total = None
    for _ in range(parts):
        part = dense.astype(jnp.bfloat16)
        dense = dense - part.astype(jnp.float32)
        term = jnp.dot(part, chosen, preferred_element_type=jnp.float32)
        total = term if total is None else total + term
    return total


def turn(values, shift):
    dim = len(values.shape) - 1
    return pltpu.roll(values, shift % values.shape[dim], dim)


def beside(values):
    low, high = turn(values, 1), turn(values, -1)
    tiles = values.shape[0]
    if tiles > 1:
        lane = cells(values.shape, 2)
        low = jnp.where(lane == 0, jnp.concatenate([low[tiles - 1 :], low[: tiles - 1]]), low)
        high = jnp.where(lane == 127, jnp.concatenate([high[1:], high[:1]]), high)
    return low + high


FACE = 14.0 / 3.0


def around_of(before, here, after, tiles):
    faces = before[0] + after[0] + here[1]
    edges = before[1] + after[1]
    inward = FACE * here[0] + faces + (1.0 / 3.0) * edges
    return (FACE * faces + edges)[:tiles] + beside(inward)[:tiles]


class Level:
    def __init__(self, refs, scale):
        self.ks, self.r, self.dg, self.di = refs[:4]
        self.now, self.new = refs[4:6], refs[6:8]
        self.scale = scale

    def grab(self, ref, p, row):
        return (
            ref[p, :, row : row + 8, :],
            ref[p, :, row - 1 : row + 7, :] + ref[p, :, row + 1 : row + 9, :],
        )

    def diagonal(self, raw, span, rows):
        base, count = span
        for row in rows:
            at = slice(row, row + 8)
            before, here = self.grab(raw, base - 1, row), self.grab(raw, base, row)
            for p in (base + j for j in range(count)):
                after = self.grab(raw, p + 1, row)
                near = around_of(before, here, after, raw.shape[1])
                total = self.scale * (128.0 * here[0] + 3.0 * near)
                self.dg[p, :, at, :] = total
                self.di[p, :, at, :] = jnp.where(here[0] > 0.0, 1.0 / total, 0.0)
                self.ks[p, :, at, :] = (3.0 * self.scale) * here[0]
                before, here = here, after

    def first_update(self, span, rows, centre):
        base, count = span
        for row in rows:
            at = slice(row, row + 8)
            for p in (base + j for j in range(count)):
                scaled = self.r[p, :, at, :] * self.di[p, :, at, :]
                self.r[p, :, at, :] = scaled
                fresh = scaled * (1.0 / centre)
                self.now[0][p, :, at, :] = fresh
                self.now[1][p, :, at, :] = fresh * self.ks[p, :, at, :]

    def apply(self, span, rows, pair, tiles=None):
        base, count = span
        tiles = tiles or self.r.shape[1]
        some = slice(0, tiles)
        window = {}
        for row in rows:
            window[row] = [
                [self.grab(ref, q, row) for ref in self.now] for q in (base - 1, base)
            ]
        for p in (base + j for j in range(count)):
            for row in rows:
                at = slice(row, row + 8)
                before, here = window[row]
                after = [self.grab(ref, p + 1, row) for ref in self.now]
                plain, heavy = (around_of(*parts, tiles) for parts in zip(before, here, after))
                coeff = self.ks[p, some, at, :]
                field = here[0][0][:tiles]
                left = field - self.di[p, some, at, :] * (coeff * plain + heavy)
                left = self.r[p, some, at, :] - left
                self.r[p, some, at, :] = left
                if pair is not None:
                    fresh = pair[1] * left
                    if pair[0] != 0.0:
                        fresh = pair[0] * field + fresh
                    self.new[0][p, some, at, :] = fresh
                    self.new[1][p, some, at, :] = coeff * fresh
                window[row] = [here, after]
        self.now, self.new = self.new, self.now


def kernel(sizes, block, *refs):
    (nx, ny, nz) = sizes
    (bx, by, bz) = block
    deep = 5
    cx, cy = bx // 2, by // 2
    (k_in, b_in, x_out, r_out, d_out) = refs[:5]
    refs = refs[1:]
    (k_raw, k_mid, k_low) = refs[4:7]
    fine = Level(refs[7:15], 0.5 / 30.0)
    mid = Level(refs[15:23], 0.5 / 4.0 / 30.0)
    low = Level(refs[23:31], 0.5 / 16.0 / 30.0)
    (r_near, x_fine, x_mid, x_low, half_sum) = refs[31:36]
    (k_send, b_send, k_edge, b_edge, k_side, b_side) = refs[36:42]
    (z_send, z_passed, z_got, zr_send, zr_passed, zr_got) = refs[42:48]
    (load_sem, near_send, near_sem, z_sem, zr_sem, far_send, far_sem, chain) = refs[48:56]
    ix, iy, iz = lax.axis_index("gx"), lax.axis_index("gy"), lax.axis_index("gz")
    own = 1 + deep * ix
    other = (1 - ix, iy, iz)
    mine = (pl.ds(own, bx), pl.ds(0, 2), pl.ds(by, by), slice(None))

    def span(width):
        return (own - ix * width, bx + width)

    both, middle = (by // 2, by + by // 2), (by,)

    for ref, target, which in ((k_in, k_raw, 0), (b_in, r_near, 1), (b_in, fine.r, 2)):
        for t in range(2):
            pltpu.make_async_copy(
                ref.at[:, :, pl.ds(128 * t, 128)],
                target.at[pl.ds(own, bx), t, pl.ds(by, by), :],
                load_sem.at[which],
            ).start()

    barrier = pltpu.get_barrier_semaphore()
    z_there = {1: iz + 1 < nz, -1: iz > 0, 0: None}
    y_there = {1: iy + 1 < ny, -1: iy > 0, 0: None}

    def when(*conditions):
        kept = [c for c in conditions if c is not None]
        if not kept:
            return lambda f: f()
        total = kept[0]
        for c in kept[1:]:
            total = total & c
        return pl.when(total)

    def column(skip):
        for jx in range(nx):
            for jy in range(ny):
                if jx or jy or not skip:
                    yield ((ix + jx) % nx, (iy + jy) % ny)

    def counted(number, *conditions):
        for c in conditions:
            if c is not None:
                number = jnp.where(c, number, 0)
        return number

    def greet(target):
        pl.semaphore_signal(barrier, inc=1, device_id=target, device_id_type=MESH)

    peers = 0
    for dz, dys in ((0, (0, 1, -1)), (1, (0,)), (-1, (0,))):
        for dy in dys:
            there = (z_there[dz], y_there[dy])
            near = [ix] if dz else [jx for jx in (ix, 1 - ix) if dy or jx is not ix]

            @when(*there)
            def _():
                for jx in near:
                    greet((jx, iy + dy, iz + dz))

            peers = peers + counted(len(near), *there)

    def clear(ref, *at):
        for p in range(ref.shape[0]):
            ref[(p, *at)] = jnp.zeros(ref[(p, *at)].shape, jnp.float32)

    for p in (0, bx + deep + 1):
        k_raw[p] = jnp.zeros(k_raw.shape[1:], jnp.float32)
    for ref in (k_raw, fine.r, r_near):
        @pl.when(iy == 0)
        def _():
            clear(ref, slice(0, 2), slice(0, by))

        @pl.when(iy == ny - 1)
        def _():
            clear(ref, slice(0, 2), slice(2 * by, 3 * by))

    def blank(ref, dims):
        ref[dims] = jnp.zeros(ref[dims].shape, jnp.float32)

    for ref, passed in ((z_got, z_passed), (zr_got, zr_passed)):
        for side, gone in ((0, iz == 0), (1, iz == nz - 1)):
            @pl.when(gone)
            def _():
                blank(ref, (side,))
                blank(passed, (side,))

        for j, gone in ((2, iy == 0), (0, iy == ny - 1)):
            @pl.when(gone)
            def _():
                for side in (0, 1):
                    blank(ref, (side, j))
    for ref in (k_side, b_side):
        for side, gone in ((0, iz == 0), (1, iz == nz - 1)):
            @pl.when(gone)
            def _():
                blank(ref, (side,))
    for ref in (*fine.now, *fine.new, *mid.now, *mid.new, *low.now, *low.new, k_low, x_mid):
        clear(ref)
    top = nx * cx + 1
    for p in (0, top):
        k_mid[p] = jnp.zeros(k_mid.shape[1:], jnp.float32)
    for row in (0, ny * cy + 1):
        clear(k_mid, slice(None), slice(row, row + 1))
    half_sum[...] = jnp.zeros(half_sum.shape, jnp.float32)

    own_rows = slice(by, 2 * by)
    lane = cells((8, 128), 1)

    def residual_of(p):
        return fine.r[p, 0:2, own_rows, :] * fine.dg[p, 0:2, own_rows, :]
    shrink = ones_where(cells((256, 128), 0) >> 1 == cells((256, 128), 1))

    def wide(values):
        return jnp.concatenate([values[0], values[1]], axis=1)

    def coarse_block(read, send, exact):
        for q in range(cx):
            p = own + 2 * q
            half_sum[q, :, 0:by, :] = read(p) + read(p + 1)
        rows = [
            wide(
                half_sum[q, :, pl.ds(0, by, stride=2), :]
                + half_sum[q, :, pl.ds(1, by, stride=2), :]
            )
            for q in range(cx)
        ]
        parts = (pick(jnp.concatenate(rows, axis=0), shrink, exact) * 0.125).reshape(cx, by, 128)
        send[...] = parts
        return parts

    def coarse_edge(parts, edge):
        low_part = parts[0]
        top_part = turn(parts[0], 32)
        for q in range(1, cx):
            here = (lane >> 5) == q
            low_part = jnp.where(here, turn(parts[q], 32 * q), low_part)
            top_part = jnp.where(here, turn(parts[q], 32 * q - 96), top_part)
        edge[0, 0:by] = top_part
        edge[1, 0:by] = low_part

    def pack_z(ref, kind, into):
        slot = lane >> 4
        front = (lane & 15) < 8
        packs = [jnp.zeros((8, 128), jnp.float32)] * 2 if into is None else into
        top, bottom = packs
        for q in range(bx):
            here = slot == q
            low_tile = ref[own + q, 0, by : 2 * by, :]
            top_tile = ref[own + q, 1, by : 2 * by, :]
            if kind == 0:
                top = jnp.where(here & front, turn(top_tile, 16 * q - 120), top)
                bottom = jnp.where(
                    here & jnp.logical_not(front), turn(low_tile, 16 * q + 8), bottom
                )
            else:
                after = slot == (q + 1) % 8
                top = jnp.where(
                    here & jnp.logical_not(front), turn(top_tile, 16 * q + 8 - 120), top
                )
                bottom = jnp.where(after & front, turn(low_tile, 16 * q + 16), bottom)
        return (top, bottom)

    def save_z(packs, send):
        for side in (0, 1):
            send[side, 0] = packs[side]
            moved = turn(packs[side], -16 * (bx - deep))
            send[side, 1] = jnp.where(ix == 0, moved, packs[side])

    def remote(source, target, out_sem, in_sem, device):
        return pltpu.make_async_remote_copy(
            src_ref=source,
            dst_ref=target,
            send_sem=out_sem,
            recv_sem=in_sem,
            device_id=device,
            device_id_type=MESH,
        )

    def near_views(ref, depth, dy, start_x, source):
        if dy == 0:
            rows = pl.ds(by, by)
        elif source:
            rows = pl.ds(2 * by - depth, depth) if dy == 1 else pl.ds(by, depth)
        else:
            rows = pl.ds(by - depth, depth) if dy == 1 else pl.ds(2 * by, depth)
        return [
            ref.at[pl.ds(start, planes), pl.ds(0, 2), rows, :]
            for start, planes in ((start_x, depth), (own, bx))
        ]

    def near_start(source, target, depth, along_x, in_sem):
        start_from = jnp.where(ix == 0, bx + 1 - depth, deep + 1)
        start_to = jnp.where(ix == 0, deep + 1 - depth, bx + 1)
        for dy in (0, 1, -1) if along_x else (1, -1):
            @when(y_there[dy])
            def _():
                which = 0 if along_x else 1
                remote(
                    near_views(source, depth, dy, start_from, True)[which],
                    near_views(target, depth, dy, start_to, False)[which],
                    near_send.at[0],
                    in_sem,
                    (1 - ix if along_x else ix, iy + dy, iz),
                ).start()

    inner_y = (iy > 0) & (iy + 1 < ny)
    inner_z = (iz > 0) & (iz + 1 < nz)

    def part_of(ref, rows):
        (p, t, n) = ref.shape[:3]
        sizes = [
            (a, b, rows // (a * b))
            for a in range(1, p + 1)
            for b in range(1, t + 1)
            if rows % (a * b) == 0 and rows // (a * b) <= n
        ]
        (a, b, c) = sizes[0]
        return ref.at[pl.ds(0, a), pl.ds(0, b), pl.ds(0, c), :]

    def wait_rows(ref, out_sem, in_sem, sent, inner, base, each):
        for condition, number in ((inner, 2), (jnp.logical_not(inner), 1)):
            @pl.when(condition)
            def _():
                view = part_of(ref, base + number * each)
                move = remote(view, view, out_sem, in_sem, other)
                if sent:
                    move.wait_send()
                else:
                    move.wait_recv()

    def near_rows(depth, along_x):
        if along_x:
            return 2 * depth * by, 2 * depth * depth
        return 0, 2 * bx * depth

    def near_wait(depth, kinds, in_sem):
        base = sum(near_rows(depth, kind)[0] for kind in kinds)
        each = sum(near_rows(depth, kind)[1] for kind in kinds)
        wait_rows(k_raw, near_send.at[0], in_sem, False, inner_y, base, each)

    def near_sent(depths):
        for depth in depths:
            kinds = [near_rows(depth, kind) for kind in (True, False)]
            base, each = sum(k[0] for k in kinds), sum(k[1] for k in kinds)
            wait_rows(k_raw, near_send.at[0], near_sem.at[0], True, inner_y, base, each)

    def z_start(send, passed, sems):
        for side, dz in ((0, 1), (1, -1)):
            @pl.when(z_there[dz])
            def _():
                remote(
                    send.at[side],
                    passed.at[side],
                    near_send.at[1 + side],
                    sems.at[side],
                    (ix, iy, iz + dz),
                ).start()

    def z_pass_on(passed, got, sems):
        for side, dz in ((0, 1), (1, -1)):
            @pl.when(z_there[-dz])
            def _():
                view = passed.at[side]
                remote(view, view, near_send.at[1 + side], sems.at[side], other).wait_recv()
                for dy in (0, 1, -1):
                    @when(y_there[dy])
                    def _():
                        for xi in (0, 1) if dy else (1,):
                            remote(
                                passed.at[side, xi],
                                got.at[side, dy + 1, xi],
                                near_send.at[3 + side],
                                sems.at[2 + side],
                                (ix if xi == 0 else 1 - ix, iy + dy, iz),
                            ).start()

    def z_wait(passed, sems, sent):
        for side, dz in ((0, 1), (1, -1)):
            @pl.when(z_there[-dz])
            def _():
                args = (near_send.at[3 + side], sems.at[2 + side], sent, inner_y, by, 2 * by)
                wait_rows(k_raw, *args)

            if sent:
                @pl.when(z_there[dz])
                def _():
                    view = passed.at[side]
                    remote(view, view, near_send.at[1 + side], sems.at[side], other).wait_send()

    def unpack_z(passed, got, kind, target):
        front = (lane & 15) < 8
        kept = (lane < 8) | (lane >= 120)
        skip = 0 if kind == 0 else 8
        for group in range(3):
            for xi, planes in ((0, bx), (1, deep)):
                straight = group == 1 and xi == 0
                lower, upper = (
                    passed[side, 0] if straight else got[side, 2 - group, xi] for side in (0, 1)
                )
                pair = (lower, upper) if kind == 0 else (upper, lower)
                merged = jnp.where(front, *pair)
                first = own if xi == 0 else jnp.where(ix == 0, bx + 1, 1)
                for q in range(planes):
                    target[first + q, 2, by * group : by * group + by, :] = jnp.where(
                        kept, turn(merged, -(16 * q + 8 + skip)), 0.0
                    )

    def far_start(send, target, in_sem):
        for jx, jy in reversed(list(column(True))):
            remote(
                send.at[:, pl.ds(0, cy), :],
                target.at[pl.ds(1 + cx * ix, cx), 0, pl.ds(1 + cy * iy, cy), :],
                far_send.at[0],
                in_sem,
                (jx, jy, iz),
            ).start()

    def far_start_sides(edge, side_target, in_sem):
        for side, dz in ((0, 1), (1, -1)):
            @when(z_there[dz])
            def _():
                for jx, jy in reversed(list(column(False))):
                    remote(
                        edge.at[side, pl.ds(0, cy), :],
                        side_target.at[side, ix, pl.ds(cy * iy, cy), :],
                        far_send.at[0],
                        in_sem,
                        (jx, jy, iz + dz),
                    ).start()

    def far_wait(in_sem, sent=False):
        main, each = (nx * ny - 1) * cx * cy, nx * ny * cy
        wait_rows(k_raw, far_send.at[0], in_sem, sent, inner_z, main, each)

    def keep_own(send, target):
        for jy in range(ny):
            @pl.when(iy == jy)
            def _():
                for q in range(cx):
                    rows = slice(1 + cy * jy, 1 + cy * jy + cy)
                    target[1 + cx * ix + q, 0, rows, :] = send[q, 0:cy, :]

    def unpack_far(side_target, target):
        shape = side_target.shape[2:]
        column_of = cells(shape, 1)
        for jx in range(nx):
            below, above = side_target[0, jx], side_target[1, jx]
            for q in range(cx):
                upper = jnp.where(column_of < 32, turn(above, -32 * q), 0.0)
                target[1 + cx * jx + q, 1, 1 : 1 + shape[0], :] = jnp.where(
                    column_of >= 96, turn(below, 96 - 32 * q), upper
                )

    for which, ref in ((0, k_raw), (1, r_near), (2, fine.r)):
        view = ref.at[mine]
        pltpu.make_async_copy(view, view, load_sem.at[which]).wait()
    save_z(pack_z(fine.r, 1, pack_z(k_raw, 0, None)), z_send)
    pl.semaphore_wait(barrier, peers)

    def pass_on(step):
        for which, dy in ((0, 1), (1, -1)):
            behind = iy - dy * step

            @when(y_there[dy], behind >= 0, behind < ny)
            def _():
                pl.semaphore_signal(
                    chain.at[which], inc=1, device_id=(ix, iy + dy, iz), device_id_type=MESH
                )

    def pass_wait(step):
        for which, dy in ((0, 1), (1, -1)):
            behind = iy - dy * (step + 1)

            @when(behind >= 0, behind < ny)
            def _():
                pl.semaphore_wait(chain.at[which], 1)

    z_start(z_send, z_passed, z_sem)
    near_start(k_raw, k_raw, deep, True, near_sem.at[0])
    near_start(k_raw, k_raw, deep, False, near_sem.at[0])
    pass_on(1)
    coarse_edge(coarse_block(lambda p: k_raw[p, 0:2, own_rows, :], k_send, 3), k_edge)
    keep_own(k_send, k_mid)
    z_pass_on(z_passed, z_got, z_sem)
    near_start(r_near, fine.r, deep - 1, False, near_sem.at[1])
    near_start(r_near, fine.r, deep - 1, True, near_sem.at[2])
    for step in range(1, ny - 1):
        pass_wait(step)
        if step + 1 < ny - 1:
            pass_on(step + 1)
    for side, dz in ((0, 1), (1, -1)):
        @pl.when(z_there[dz])
        def _():
            pl.semaphore_signal(
                chain.at[2 + side], inc=1, device_id=(ix, iy, iz + dz), device_id_type=MESH
            )

    near_wait(deep, (True, False), near_sem.at[0])
    for side, dz in ((0, 1), (1, -1)):
        @pl.when(z_there[-dz])
        def _():
            pl.semaphore_wait(chain.at[2 + side], 1)

    far_start(k_send, k_mid, far_sem.at[0])
    far_start_sides(k_edge, k_side, far_sem.at[0])
    z_wait(z_passed, z_sem, False)
    unpack_z(z_passed, z_got, 0, k_raw)
    fine.diagonal(k_raw, span(4), both)
    unpack_z(z_passed, z_got, 1, fine.r)
    near_wait(deep - 1, (False,), near_sem.at[1])

    def strip(first, last):
        return (bx - last + ix * (deep + 1 + first - bx + last), last - first + 1)

    def add_fine(ref, first=0, last=bx - 1, fresh=False):
        for a in range(first, last + 1):
            q = bx - 1 - a + ix * (2 * a - bx + 1)
            value = ref[own + q, 0:2, own_rows, :]
            x_fine[q] = value if fresh else x_fine[q] + value

    def smooth_fine(first, last, grow, added):
        for number in range(DEGREE):
            pair = weights[number] if number < DEGREE - 1 else None
            rows, tiles = (both, None) if number < DEGREE - 1 else (middle, 2)
            fine.apply(strip(first, last), rows, pair, tiles)
            if pair is not None and number < added:
                add_fine(fine.now[0], max(first, 0), min(last, bx - 1))
            first, last = first + 1, last + grow

    centre, weights = chebyshev_coefs(DEGREE, smooth_low)
    near_wait(deep - 1, (True,), near_sem.at[2])
    fine.first_update(strip(-DEGREE, bx - 1), both, centre)
    add_fine(fine.now[0], fresh=True)
    smooth_fine(1 - DEGREE, bx - 1, 0, DEGREE)

    far_wait(far_sem.at[0], True)
    parts = coarse_block(residual_of, b_send, 2)
    far_start(b_send, mid.r, far_sem.at[1])
    coarse_edge(parts, b_edge)
    far_start_sides(b_edge, b_side, far_sem.at[1])
    near_sent((deep, deep - 1))
    z_wait(z_passed, z_sem, True)
    keep_own(b_send, mid.r)
    save_z(pack_z(fine.r, 0, None), zr_send)
    z_start(zr_send, zr_passed, zr_sem)
    near_start(fine.r, r_near, deep - 1, True, near_sem.at[3])
    near_start(fine.r, r_near, deep - 1, False, near_sem.at[3])
    own_fine = [(q, own + q) for q in range(bx)]
    for q, p in own_fine:
        r_near[p, 0:2, own_rows, :] = fine.r[p, 0:2, own_rows, :]

    mid_span, mid_rows = (1, nx * cx), tuple(range(1, ny * cy, 8))
    low_span, low_rows = (1, nx * cx // 2), tuple(range(1, ny * cy // 2, 8))
    lows = nx * cx // 2
    low_row = ny * cy // 2

    def to_low(read, target):
        rows = []
        for q in range(lows):
            total = None
            for p in (1 + 2 * q, 2 + 2 * q):
                for row in (1, 2):
                    part = read(p, pl.ds(row, low_row, stride=2))
                    total = part if total is None else total + part
            rows.append(wide(total))
        parts = pick(jnp.concatenate(rows, axis=0), shrink) * 0.125
        target[1 : 1 + lows, 0, 1 : 1 + low_row, :] = parts.reshape(lows, low_row, 128)

    far_wait(far_sem.at[0])
    unpack_far(k_side, k_mid)
    mid.diagonal(k_mid, mid_span, mid_rows)
    to_low(lambda p, rows: k_mid[p, :, rows, :], k_low)
    low.diagonal(k_low, low_span, low_rows)

    z_pass_on(zr_passed, zr_got, zr_sem)
    far_wait(far_sem.at[1])
    unpack_far(b_side, mid.r)
    start = 8
    inside = (slice(1, 1 + nx * cx), slice(None), slice(1, 1 + ny * cy))

    def add_mid(ref, fresh=False):
        for q in range(nx * cx):
            value = ref[1 + q, :, 1 : 1 + ny * cy, :]
            at = (q, slice(None), slice(start, start + ny * cy))
            x_mid[at] = value if fresh else x_mid[at] + value

    mid.first_update(mid_span, mid_rows, centre)
    add_mid(mid.now[0], True)
    for number in range(DEGREE):
        pair = weights[number] if number < DEGREE - 1 else None
        mid.apply(mid_span, mid_rows, pair)
        if pair is not None:
            add_mid(mid.now[0])

    to_low(lambda p, rows: mid.r[p, :, rows, :] * mid.dg[p, :, rows, :], low.r)
    low_centre, low_weights = chebyshev_coefs(COARSE_DEGREE, coarse_low)
    near_wait(deep - 1, (True, False), near_sem.at[3])
    z_wait(zr_passed, zr_sem, False)
    low.first_update(low_span, low_rows, low_centre)
    unpack_z(zr_passed, zr_got, 0, r_near)

    def low_now():
        return low.now[0][1 : 1 + lows, 0, 1 : 1 + low_row, :]

    x_low[...] = low_now()
    for pair in low_weights:
        low.apply(low_span, low_rows, pair)
        x_low[...] += low_now()

    spread = ones_where(cells((128, 256), 0) == cells((128, 256), 1) >> 1)
    fixed = pick(x_low[...].reshape(lows * low_row, 128), spread).reshape(lows, low_row, 256)
    for q in range(lows):
        for t in range(2):
            value = fixed[q, :, 128 * t : 128 * t + 128]
            for p in (1 + 2 * q, 2 + 2 * q):
                for row in (1, 2):
                    mid.now[0][p, t, pl.ds(row, low_row, stride=2), :] = value
    for p in range(1, 1 + nx * cx):
        at = (p, slice(None), slice(1, 1 + ny * cy))
        mid.now[1][at] = mid.ks[at] * mid.now[0][at]
    add_mid(mid.now[0])
    mid.apply(mid_span, mid_rows, (0.0, 1.0 / centre))
    add_mid(mid.now[0])
    for pair in weights:
        mid.apply(mid_span, mid_rows, pair)
        add_mid(mid.now[0])

    shape = (256, 384)
    from_lane, to_lane = cells(shape, 0), cells(shape, 1)
    to_lane = jnp.where(
        to_lane < 256, to_lane >> 1, (to_lane >> 1) + jnp.where(to_lane < 320, 0, 64)
    )
    widen = ones_where(from_lane == to_lane)
    planes = (bx + deep + 1) // 2
    rows = []
    x_rows = 16
    for j in range(planes):
        from_row = start - 3 + cy * iy
        rows.append(wide(x_mid[ix + j, :, pl.ds(from_row, x_rows), :]))
    fixed = pick(jnp.concatenate(rows, axis=0), widen).reshape(planes, x_rows, 384)
    for j in range(planes):
        for t in range(3):
            value = fixed[j, :, 128 * t : 128 * t + 128]
            for p in (0, 1):
                for row in (0, 1):
                    at = 1 - ix + 2 * j + p
                    fine.now[0][at, t, pl.ds(2 + row, 8, stride=2), :] = value[0:8]
                    fine.now[0][at, t, pl.ds(18 + row, 2, stride=2), :] = value[8:10]
    for p in range(1, 1 + bx + deep):
        fine.now[1][p] = (3.0 * fine.scale) * k_raw[p] * fine.now[0][p]
    add_fine(fine.now[0])
    fine.r = r_near
    fine.apply(span(4), both, (0.0, 1.0 / centre))
    add_fine(fine.now[0])
    smooth_fine(1 - DEGREE, bx - 1, 0, DEGREE - 2)
    for q, p in own_fine:
        last, left = fine.new[0][p, 0:2, own_rows, :], residual_of(p)
        for t in range(2):
            at = (q, slice(None), slice(128 * t, 128 * t + 128))
            x_out[at] = x_fine[q, t]
            d_out[at] = last[t]
            r_out[at] = left[t] - last[t]
    near_sent((deep - 1,))
    z_wait(zr_passed, zr_sem, True)
    far_wait(far_sem.at[1], True)


def gathered(sizes, conductivity, source):
    (nx, ny, nz) = sizes
    (bx, by, bz) = conductivity.shape
    kept = lambda *shape: pltpu.VMEM(shape, jnp.float32)
    fine = kept(bx + 7, 3, 3 * by, 128)
    mid = kept(nx * bx // 2 + 2, 2, ny * by // 2 + 8, 128)
    low = kept(nx * bx // 4 + 2, 1, ny * by // 4 + 8, 128)
    cx, cy = bx // 2, by // 2
    scratch = [fine, mid, low] + [fine] * 8 + [mid] * 8 + [low] * 8
    scratch += [fine, kept(bx, 2, by, 128), kept(nx * cx, 2, ny * cy + 24, 128)]
    scratch += [kept(nx * cx // 2, ny * cy // 2, 128), kept(cx, 2, 2 * by, 128)]
    scratch += [kept(cx, by, 128)] * 2 + [kept(2, 2 * by, 128)] * 2
    scratch += [kept(2, nx, ny * cy, 128)] * 2
    scratch += [kept(2, 2, by, 128), kept(2, 2, by, 128), kept(2, 3, 2, by, 128)] * 2
    dma = pltpu.SemaphoreType.DMA
    scratch += [dma((3,)), dma((5,)), dma((4,)), dma((4,)), dma((4,)), dma((1,)), dma((2,))]
    scratch += [pltpu.SemaphoreType.REGULAR((4,))]
    shape = pltpu.VMEM((bx, by, bz), jnp.float32)
    vmem = pl.BlockSpec(memory_space=pltpu.VMEM)
    anywhere = pl.BlockSpec(memory_space=pltpu.HBM)
    x_part, r_part, last = pl.pallas_call(
        functools.partial(kernel, sizes, (bx, by, bz)),
        out_shape=(shape,) * 3,
        in_specs=[anywhere, anywhere],
        out_specs=(vmem,) * 3,
        scratch_shapes=scratch,
        compiler_params=pltpu.CompilerParams(
            collective_id=0, has_side_effects=True, vmem_limit_bytes=66715648
        ),
    )(conductivity, source)
    return x_part + last, r_part + last


def plan(conductivity, source):
    sizes = tuple(lax.axis_size(axis) for axis in ("gx", "gy", "gz"))
    (bx, by, bz) = conductivity.shape
    fits = (bx, by, bz) == (8, 8, 256) and sizes[0] == 2 and sizes[1] == 4
    if fits:
        return gathered(sizes, conductivity, source)
    return body(conductivity, source)


def solution(mesh):
    in_specs = (P("gx", "gy", "gz"), P("gx", "gy", "gz"))
    out_specs = (P("gx", "gy", "gz"), P("gx", "gy", "gz"))
    return jax.shard_map(plan, mesh=mesh, in_specs=in_specs, out_specs=out_specs, check_vma=False)
```

```python
import functools

import jax
import jax.numpy as jnp
from jax import lax
from jax.experimental import pallas as pl
from jax.experimental.pallas import tpu as pltpu
from jax.sharding import PartitionSpec as P

LEVELS = 3
DEGREE = 4
COARSE_DEGREE = 8
MESH = pl.DeviceIdType.MESH


weight_table = {1: 14.0 / 30.0, 2: 3.0 / 30.0, 3: 1.0 / 30.0}
neighbour_offsets = [
    (along_one, along_two, along_three)
    for along_one in (-1, 0, 1)
    for along_two in (-1, 0, 1)
    for along_three in (-1, 0, 1)
    if (along_one, along_two, along_three) != (0, 0, 0)
]
smooth_low = 0.5
coarse_low = 0.03
upper_bound = 2.0


def padded_2(block, sides, width):
    for axis, dim in sides:
        count = lax.axis_size(axis)
        forward = [(i, i + 1) for i in range(count - 1)]
        backward = [(target, source) for source, target in forward]
        low = lax.ppermute(
            lax.slice_in_dim(block, block.shape[dim] - width, None, axis=dim), axis, forward
        )
        high = lax.ppermute(lax.slice_in_dim(block, 0, width, axis=dim), axis, backward)
        block = jnp.concatenate([low, block, high], axis=dim)
    return block


def shifted(padded, offset):
    return padded[
        1 + offset[0] : padded.shape[0] - 1 + offset[0],
        1 + offset[1] : padded.shape[1] - 1 + offset[1],
        1 + offset[2] : padded.shape[2] - 1 + offset[2],
    ]


def inner(values, margin):
    return values[
        margin : values.shape[0] - margin,
        margin : values.shape[1] - margin,
        margin : values.shape[2] - margin,
    ]


def stencil(field_pad, coeff_pad, spacing):
    centre_field = shifted(field_pad, (0, 0, 0))
    centre_coeff = shifted(coeff_pad, (0, 0, 0))
    total = jnp.zeros(centre_field.shape, jnp.float32)
    for offset in neighbour_offsets:
        weight = weight_table[abs(offset[0]) + abs(offset[1]) + abs(offset[2])]
        total = total + weight * (centre_coeff + shifted(coeff_pad, offset)) * (
            centre_field - shifted(field_pad, offset)
        )
    return total * (0.5 / spacing)


def diagonal_of(coeff_pad, spacing):
    centre_coeff = shifted(coeff_pad, (0, 0, 0))
    total = jnp.zeros(centre_coeff.shape, jnp.float32)
    for offset in neighbour_offsets:
        weight = weight_table[abs(offset[0]) + abs(offset[1]) + abs(offset[2])]
        total = total + weight * (centre_coeff + shifted(coeff_pad, offset))
    return total * (0.5 / spacing)


def coarsen(values):
    extent = values.shape
    return values.reshape(extent[0] // 2, 2, extent[1] // 2, 2, extent[2] // 2, 2).mean(
        axis=(1, 3, 5)
    )


def refine(values):
    return jnp.repeat(jnp.repeat(jnp.repeat(values, 2, axis=0), 2, axis=1), 2, axis=2)


def chebyshev_coefs(degree, lower):
    centre = (upper_bound + lower) / 2.0
    half_width = (upper_bound - lower) / 2.0
    ratio_term = centre / half_width
    rho_prev = 1.0 / ratio_term
    weights = []
    for number in range(1, degree):
        rho_next = 1.0 / (2.0 * ratio_term - rho_prev)
        weights.append((rho_next * rho_prev, 2.0 * rho_next / half_width))
        rho_prev = rho_next
    return (centre, weights)


def inside_mask(extent, margin):
    first_pos = (
        lax.axis_index("gx") * extent[0]
        + jnp.arange(extent[0] + 2 * margin, dtype=jnp.int32)
        - margin
    )
    second_pos = (
        lax.axis_index("gy") * extent[1]
        + jnp.arange(extent[1] + 2 * margin, dtype=jnp.int32)
        - margin
    )
    third_pos = (
        lax.axis_index("gz") * extent[2]
        + jnp.arange(extent[2] + 2 * margin, dtype=jnp.int32)
        - margin
    )
    first_ok = (first_pos >= 0) & (first_pos < extent[0] * lax.axis_size("gx"))
    second_ok = (second_pos >= 0) & (second_pos < extent[1] * lax.axis_size("gy"))
    third_ok = (third_pos >= 0) & (third_pos < extent[2] * lax.axis_size("gz"))
    return first_ok[:, None, None] & second_ok[None, :, None] & third_ok[None, None, :]


def operate_near(context, field):
    spacing, coeff_ext, diagonal_ext, inside = context
    padded = padded_2(field, (("gx", 0), ("gy", 1), ("gz", 2)), 1)
    return stencil(padded, inner(coeff_ext, 1), spacing)


def two_steps(context, solution, residual, update, first_pair, second_pair):
    spacing, coeff_ext, diagonal_ext, inside = context
    diagonal = inner(diagonal_ext, 1)
    stacked = jnp.stack([update, residual])
    padded = padded_2(stacked, (("gx", 1), ("gy", 2), ("gz", 3)), 2)
    update_wide = padded[0]
    residual_wide = padded[1]
    residual_near = inner(residual_wide, 1) - stencil(update_wide, coeff_ext, spacing)
    update_near = (
        first_pair[0] * inner(update_wide, 1) + first_pair[1] * residual_near / diagonal_ext
    )
    update_near = jnp.where(inside, update_near, 0.0)
    solution = solution + inner(update_near, 1)
    residual = inner(residual_near, 1) - stencil(update_near, inner(coeff_ext, 1), spacing)
    if second_pair is None:
        update = inner(update_near, 1)
    else:
        update = second_pair[0] * inner(update_near, 1) + second_pair[1] * residual / diagonal
        solution = solution + update
    return (solution, residual, update)


def relax(context, right_side, start, degree, lower, final):
    diagonal = inner(context[2], 1)
    centre, weights = chebyshev_coefs(degree, lower)
    if start is None:
        residual = right_side
    else:
        residual = right_side - operate_near(context, start)
    update = residual / (centre * diagonal)
    solution = update if start is None else start + update
    plan_list = list(weights) + ([None] if final else [])
    position = 0
    while position + 1 < len(plan_list):
        solution, residual, update = two_steps(
            context, solution, residual, update, plan_list[position], plan_list[position + 1]
        )
        position = position + 2
    leftover = plan_list[position:]
    for pair in leftover:
        residual = residual - operate_near(context, update)
        update = pair[0] * update + pair[1] * residual / diagonal
        solution = solution + update
    return (solution, residual)


def body(conductivity, source):
    coeff_now = conductivity
    contexts = []
    for grid_level in range(LEVELS):
        if grid_level > 0:
            coeff_now = coarsen(coeff_now)
        spacing = float(4**grid_level)
        coeff_ext = padded_2(coeff_now, (("gx", 0), ("gy", 1), ("gz", 2)), 2)
        inside = inside_mask(coeff_now.shape, 1)
        diagonal_ext = jnp.where(inside, diagonal_of(coeff_ext, spacing), 1.0)
        contexts.append((spacing, coeff_ext, diagonal_ext, inside))

    def cycle(grid_level, right_side):
        context = contexts[grid_level]
        if grid_level == LEVELS - 1:
            return relax(context, right_side, None, COARSE_DEGREE, coarse_low, False)
        solution, residual = relax(context, right_side, None, DEGREE, smooth_low, True)
        correction, ignored = cycle(grid_level + 1, coarsen(residual))
        solution = solution + refine(correction)
        return relax(context, right_side, solution, DEGREE, smooth_low, grid_level == 0)

    return cycle(0, source)


def cells(shape, dim):
    return lax.broadcasted_iota(jnp.int32, shape, dim)


def ones_where(condition):
    return jnp.where(condition, 1.0, 0.0).astype(jnp.bfloat16)


def pick(dense, chosen, parts=2):
    total = None
    for _ in range(parts):
        part = dense.astype(jnp.bfloat16)
        dense = dense - part.astype(jnp.float32)
        term = jnp.dot(part, chosen, preferred_element_type=jnp.float32)
        total = term if total is None else total + term
    return total


def turn(values, shift):
    dim = len(values.shape) - 1
    return pltpu.roll(values, shift % values.shape[dim], dim)


def beside(values):
    low, high = turn(values, 1), turn(values, -1)
    tiles = values.shape[0]
    if tiles > 1:
        lane = cells(values.shape, 2)
        low = jnp.where(lane == 0, jnp.concatenate([low[tiles - 1 :], low[: tiles - 1]]), low)
        high = jnp.where(lane == 127, jnp.concatenate([high[1:], high[:1]]), high)
    return low + high


FACE = 14.0 / 3.0


def around_of(before, here, after, tiles):
    faces = before[0] + after[0] + here[1]
    edges = before[1] + after[1]
    inward = FACE * here[0] + faces + (1.0 / 3.0) * edges
    return (FACE * faces + edges)[:tiles] + beside(inward)[:tiles]


class Level:
    def __init__(self, refs, scale):
        self.ks, self.r, self.dg, self.di = refs[:4]
        self.now, self.new = refs[4:6], refs[6:8]
        self.scale = scale

    def grab(self, ref, p, row):
        return (
            ref[p, :, row : row + 8, :],
            ref[p, :, row - 1 : row + 7, :] + ref[p, :, row + 1 : row + 9, :],
        )

    def diagonal(self, raw, span, rows):
        base, count = span
        for row in rows:
            at = slice(row, row + 8)
            before, here = self.grab(raw, base - 1, row), self.grab(raw, base, row)
            for p in (base + j for j in range(count)):
                after = self.grab(raw, p + 1, row)
                near = around_of(before, here, after, raw.shape[1])
                total = self.scale * (128.0 * here[0] + 3.0 * near)
                self.dg[p, :, at, :] = total
                self.di[p, :, at, :] = jnp.where(here[0] > 0.0, 1.0 / total, 0.0)
                self.ks[p, :, at, :] = (3.0 * self.scale) * here[0]
                before, here = here, after

    def first_update(self, span, rows, centre):
        base, count = span
        for row in rows:
            at = slice(row, row + 8)
            for p in (base + j for j in range(count)):
                scaled = self.r[p, :, at, :] * self.di[p, :, at, :]
                self.r[p, :, at, :] = scaled
                fresh = scaled * (1.0 / centre)
                self.now[0][p, :, at, :] = fresh
                self.now[1][p, :, at, :] = fresh * self.ks[p, :, at, :]

    def apply(self, span, rows, pair, tiles=None, total=None):
        base, count = span
        tiles = tiles or self.r.shape[1]
        some = slice(0, tiles)
        window = {}
        for row in rows:
            window[row] = [
                [self.grab(ref, q, row) for ref in self.now] for q in (base - 1, base)
            ]
        for p in (base + j for j in range(count)):
            for row in rows:
                at = slice(row, row + 8)
                before, here = window[row]
                after = [self.grab(ref, p + 1, row) for ref in self.now]
                plain, heavy = (around_of(*parts, tiles) for parts in zip(before, here, after))
                coeff = self.ks[p, some, at, :]
                field = here[0][0][:tiles]
                left = field - self.di[p, some, at, :] * (coeff * plain + heavy)
                left = self.r[p, some, at, :] - left
                self.r[p, some, at, :] = left
                if pair is not None:
                    fresh = pair[1] * left
                    if pair[0] != 0.0:
                        fresh = pair[0] * field + fresh
                    self.new[0][p, some, at, :] = fresh
                    self.new[1][p, some, at, :] = coeff * fresh
                    if total is not None:
                        place = (p - 1, some, slice(row + 7, row + 15), slice(None))
                        total[place] = total[place] + fresh
                window[row] = [here, after]
        self.now, self.new = self.new, self.now


def kernel(sizes, block, *refs):
    (nx, ny, nz) = sizes
    (bx, by, bz) = block
    deep = 5
    cx, cy = bx // 2, by // 2
    (k_in, b_in, x_out, r_out, d_out) = refs[:5]
    refs = refs[1:]
    (k_raw, k_mid, k_low) = refs[4:7]
    fine = Level(refs[7:15], 0.5 / 30.0)
    mid = Level(refs[15:23], 0.5 / 4.0 / 30.0)
    low = Level(refs[23:31], 0.5 / 16.0 / 30.0)
    (r_near, x_fine, x_mid, x_low, half_sum) = refs[31:36]
    (k_send, b_send, k_edge, b_edge, k_side, b_side) = refs[36:42]
    (z_send, z_passed, z_got, zr_send, zr_passed, zr_got) = refs[42:48]
    (load_sem, near_send, near_sem, z_sem, zr_sem, far_send, far_sem, chain) = refs[48:56]
    (shrink, spread, widen) = refs[56:59]
    ix, iy, iz = lax.axis_index("gx"), lax.axis_index("gy"), lax.axis_index("gz")
    own = 1 + deep * ix
    other = (1 - ix, iy, iz)
    mine = (pl.ds(own, bx), pl.ds(0, 2), pl.ds(by, by), slice(None))

    def span(width):
        return (own - ix * width, bx + width)

    both, middle = (by // 2, by + by // 2), (by,)

    for ref, target, which in ((k_in, k_raw, 0), (b_in, r_near, 1), (b_in, fine.r, 2)):
        for t in range(2):
            pltpu.make_async_copy(
                ref.at[:, :, pl.ds(128 * t, 128)],
                target.at[pl.ds(own, bx), t, pl.ds(by, by), :],
                load_sem.at[which],
            ).start()

    barrier = pltpu.get_barrier_semaphore()
    z_there = {1: iz + 1 < nz, -1: iz > 0, 0: None}
    y_there = {1: iy + 1 < ny, -1: iy > 0, 0: None}

    def when(*conditions):
        kept = [c for c in conditions if c is not None]
        if not kept:
            return lambda f: f()
        total = kept[0]
        for c in kept[1:]:
            total = total & c
        return pl.when(total)

    def column(skip):
        for jx in range(nx):
            for jy in range(ny):
                if jx or jy or not skip:
                    yield ((ix + jx) % nx, (iy + jy) % ny)

    def counted(number, *conditions):
        for c in conditions:
            if c is not None:
                number = jnp.where(c, number, 0)
        return number

    def greet(target):
        pl.semaphore_signal(barrier, inc=1, device_id=target, device_id_type=MESH)

    peers = 0
    for dz, dys in ((0, (0, 1, -1)), (1, (0,)), (-1, (0,))):
        for dy in dys:
            there = (z_there[dz], y_there[dy])
            near = [ix] if dz else [jx for jx in (ix, 1 - ix) if dy or jx is not ix]

            @when(*there)
            def _():
                for jx in near:
                    greet((jx, iy + dy, iz + dz))

            peers = peers + counted(len(near), *there)

    def clear(ref, *at):
        for p in range(ref.shape[0]):
            ref[(p, *at)] = jnp.zeros(ref[(p, *at)].shape, jnp.float32)

    for p in (0, bx + deep + 1):
        k_raw[p] = jnp.zeros(k_raw.shape[1:], jnp.float32)
    for ref in (k_raw, fine.r, r_near):
        @pl.when(iy == 0)
        def _():
            clear(ref, slice(0, 2), slice(0, by))

        @pl.when(iy == ny - 1)
        def _():
            clear(ref, slice(0, 2), slice(2 * by, 3 * by))

    def blank(ref, dims):
        ref[dims] = jnp.zeros(ref[dims].shape, jnp.float32)

    for ref, passed in ((z_got, z_passed), (zr_got, zr_passed)):
        for side, gone in ((0, iz == 0), (1, iz == nz - 1)):
            @pl.when(gone)
            def _():
                blank(ref, (side,))
                blank(passed, (side,))

        for j, gone in ((2, iy == 0), (0, iy == ny - 1)):
            @pl.when(gone)
            def _():
                for side in (0, 1):
                    blank(ref, (side, j))
    for ref in (k_side, b_side):
        for side, gone in ((0, iz == 0), (1, iz == nz - 1)):
            @pl.when(gone)
            def _():
                blank(ref, (side,))
    for ref in (*fine.now, *fine.new, *mid.now, *mid.new, *low.now, *low.new, k_low, x_mid):
        clear(ref)
    top = nx * cx + 1
    for p in (0, top):
        k_mid[p] = jnp.zeros(k_mid.shape[1:], jnp.float32)
    for row in (0, ny * cy + 1):
        clear(k_mid, slice(None), slice(row, row + 1))
    half_sum[...] = jnp.zeros(half_sum.shape, jnp.float32)

    own_rows = slice(by, 2 * by)
    lane = cells((8, 128), 1)

    def residual_of(p):
        return fine.r[p, 0:2, own_rows, :] * fine.dg[p, 0:2, own_rows, :]
    shrink[...] = ones_where(cells((256, 128), 0) >> 1 == cells((256, 128), 1))

    def wide(values):
        return jnp.concatenate([values[0], values[1]], axis=1)

    def coarse_block(read, send, exact):
        for q in range(cx):
            p = own + 2 * q
            half_sum[q, :, 0:by, :] = read(p) + read(p + 1)
        rows = [
            wide(
                half_sum[q, :, pl.ds(0, by, stride=2), :]
                + half_sum[q, :, pl.ds(1, by, stride=2), :]
            )
            for q in range(cx)
        ]
        parts = (pick(jnp.concatenate(rows, axis=0), shrink[...], exact) * 0.125).reshape(cx, by, 128)
        send[...] = parts
        return parts

    def coarse_edge(parts, edge):
        low_part = parts[0]
        top_part = turn(parts[0], 32)
        for q in range(1, cx):
            here = (lane >> 5) == q
            low_part = jnp.where(here, turn(parts[q], 32 * q), low_part)
            top_part = jnp.where(here, turn(parts[q], 32 * q - 96), top_part)
        edge[0, 0:by] = top_part
        edge[1, 0:by] = low_part

    def pack_z(ref, kind, into):
        slot = lane >> 4
        front = (lane & 15) < 8
        packs = [jnp.zeros((8, 128), jnp.float32)] * 2 if into is None else into
        top, bottom = packs
        for q in range(bx):
            here = slot == q
            low_tile = ref[own + q, 0, by : 2 * by, :]
            top_tile = ref[own + q, 1, by : 2 * by, :]
            if kind == 0:
                top = jnp.where(here & front, turn(top_tile, 16 * q - 120), top)
                bottom = jnp.where(
                    here & jnp.logical_not(front), turn(low_tile, 16 * q + 8), bottom
                )
            else:
                after = slot == (q + 1) % 8
                top = jnp.where(
                    here & jnp.logical_not(front), turn(top_tile, 16 * q + 8 - 120), top
                )
                bottom = jnp.where(after & front, turn(low_tile, 16 * q + 16), bottom)
        return (top, bottom)

    def save_z(packs, send):
        for side in (0, 1):
            send[side, 0] = packs[side]
            moved = turn(packs[side], -16 * (bx - deep))
            send[side, 1] = jnp.where(ix == 0, moved, packs[side])

    def remote(source, target, out_sem, in_sem, device):
        return pltpu.make_async_remote_copy(
            src_ref=source,
            dst_ref=target,
            send_sem=out_sem,
            recv_sem=in_sem,
            device_id=device,
            device_id_type=MESH,
        )

    def near_views(ref, depth, dy, start_x, source):
        if dy == 0:
            rows = pl.ds(by, by)
        elif source:
            rows = pl.ds(2 * by - depth, depth) if dy == 1 else pl.ds(by, depth)
        else:
            rows = pl.ds(by - depth, depth) if dy == 1 else pl.ds(2 * by, depth)
        return [
            ref.at[pl.ds(start, planes), pl.ds(0, 2), rows, :]
            for start, planes in ((start_x, depth), (own, bx))
        ]

    def near_start(source, target, depth, along_x, in_sem):
        start_from = jnp.where(ix == 0, bx + 1 - depth, deep + 1)
        start_to = jnp.where(ix == 0, deep + 1 - depth, bx + 1)
        for dy in (0, 1, -1) if along_x else (1, -1):
            @when(y_there[dy])
            def _():
                which = 0 if along_x else 1
                remote(
                    near_views(source, depth, dy, start_from, True)[which],
                    near_views(target, depth, dy, start_to, False)[which],
                    near_send.at[0],
                    in_sem,
                    (1 - ix if along_x else ix, iy + dy, iz),
                ).start()

    inner_y = (iy > 0) & (iy + 1 < ny)
    inner_z = (iz > 0) & (iz + 1 < nz)

    def part_of(ref, rows):
        (p, t, n) = ref.shape[:3]
        sizes = [
            (a, b, rows // (a * b))
            for a in range(1, p + 1)
            for b in range(1, t + 1)
            if rows % (a * b) == 0 and rows // (a * b) <= n
        ]
        (a, b, c) = sizes[0]
        return ref.at[pl.ds(0, a), pl.ds(0, b), pl.ds(0, c), :]

    def wait_rows(ref, out_sem, in_sem, sent, inner, base, each):
        for condition, number in ((inner, 2), (jnp.logical_not(inner), 1)):
            @pl.when(condition)
            def _():
                view = part_of(ref, base + number * each)
                move = remote(view, view, out_sem, in_sem, other)
                if sent:
                    move.wait_send()
                else:
                    move.wait_recv()

    def near_rows(depth, along_x):
        if along_x:
            return 2 * depth * by, 2 * depth * depth
        return 0, 2 * bx * depth

    def near_wait(depth, kinds, in_sem):
        base = sum(near_rows(depth, kind)[0] for kind in kinds)
        each = sum(near_rows(depth, kind)[1] for kind in kinds)
        wait_rows(k_raw, near_send.at[0], in_sem, False, inner_y, base, each)

    def near_sent(depths):
        for depth in depths:
            kinds = [near_rows(depth, kind) for kind in (True, False)]
            base, each = sum(k[0] for k in kinds), sum(k[1] for k in kinds)
            wait_rows(k_raw, near_send.at[0], near_sem.at[0], True, inner_y, base, each)

    def z_start(send, passed, sems):
        for side, dz in ((0, 1), (1, -1)):
            @pl.when(z_there[dz])
            def _():
                remote(
                    send.at[side],
                    passed.at[side],
                    near_send.at[1 + side],
                    sems.at[side],
                    (ix, iy, iz + dz),
                ).start()

    def z_pass_on(passed, got, sems):
        for side, dz in ((0, 1), (1, -1)):
            @pl.when(z_there[-dz])
            def _():
                view = passed.at[side]
                remote(view, view, near_send.at[1 + side], sems.at[side], other).wait_recv()
                for dy in (0, 1, -1):
                    @when(y_there[dy])
                    def _():
                        for xi in (0, 1) if dy else (1,):
                            remote(
                                passed.at[side, xi],
                                got.at[side, dy + 1, xi],
                                near_send.at[3 + side],
                                sems.at[2 + side],
                                (ix if xi == 0 else 1 - ix, iy + dy, iz),
                            ).start()

    def z_wait(passed, sems, sent):
        for side, dz in ((0, 1), (1, -1)):
            @pl.when(z_there[-dz])
            def _():
                args = (near_send.at[3 + side], sems.at[2 + side], sent, inner_y, by, 2 * by)
                wait_rows(k_raw, *args)

            if sent:
                @pl.when(z_there[dz])
                def _():
                    view = passed.at[side]
                    remote(view, view, near_send.at[1 + side], sems.at[side], other).wait_send()

    def unpack_z(passed, got, kind, target):
        front = (lane & 15) < 8
        kept = (lane < 8) | (lane >= 120)
        skip = 0 if kind == 0 else 8
        for group in range(3):
            for xi, planes in ((0, bx), (1, deep)):
                straight = group == 1 and xi == 0
                lower, upper = (
                    passed[side, 0] if straight else got[side, 2 - group, xi] for side in (0, 1)
                )
                pair = (lower, upper) if kind == 0 else (upper, lower)
                merged = jnp.where(front, *pair)
                first = own if xi == 0 else jnp.where(ix == 0, bx + 1, 1)
                for q in range(planes):
                    target[first + q, 2, by * group : by * group + by, :] = jnp.where(
                        kept, turn(merged, -(16 * q + 8 + skip)), 0.0
                    )

    def far_start(send, target, in_sem):
        for jx, jy in reversed(list(column(True))):
            remote(
                send.at[:, pl.ds(0, cy), :],
                target.at[pl.ds(1 + cx * ix, cx), 0, pl.ds(1 + cy * iy, cy), :],
                far_send.at[0],
                in_sem,
                (jx, jy, iz),
            ).start()

    def far_start_sides(edge, side_target, in_sem):
        for side, dz in ((0, 1), (1, -1)):
            @when(z_there[dz])
            def _():
                for jx, jy in reversed(list(column(False))):
                    remote(
                        edge.at[side, pl.ds(0, cy), :],
                        side_target.at[side, ix, pl.ds(cy * iy, cy), :],
                        far_send.at[0],
                        in_sem,
                        (jx, jy, iz + dz),
                    ).start()

    def far_wait(in_sem, sent=False):
        main, each = (nx * ny - 1) * cx * cy, nx * ny * cy
        wait_rows(k_raw, far_send.at[0], in_sem, sent, inner_z, main, each)

    def keep_own(send, target):
        for jy in range(ny):
            @pl.when(iy == jy)
            def _():
                for q in range(cx):
                    rows = slice(1 + cy * jy, 1 + cy * jy + cy)
                    target[1 + cx * ix + q, 0, rows, :] = send[q, 0:cy, :]

    def unpack_far(side_target, target):
        shape = side_target.shape[2:]
        column_of = cells(shape, 1)
        for jx in range(nx):
            below, above = side_target[0, jx], side_target[1, jx]
            for q in range(cx):
                upper = jnp.where(column_of < 32, turn(above, -32 * q), 0.0)
                target[1 + cx * jx + q, 1, 1 : 1 + shape[0], :] = jnp.where(
                    column_of >= 96, turn(below, 96 - 32 * q), upper
                )

    def loaded(which, ref):
        view = ref.at[mine]
        pltpu.make_async_copy(view, view, load_sem.at[which]).wait()

    loaded(0, k_raw)
    loaded(1, r_near)
    save_z(pack_z(r_near, 1, pack_z(k_raw, 0, None)), z_send)
    pl.semaphore_wait(barrier, peers)

    def pass_on(step):
        for which, dy in ((0, 1), (1, -1)):
            behind = iy - dy * step

            @when(y_there[dy], behind >= 0, behind < ny)
            def _():
                pl.semaphore_signal(
                    chain.at[which], inc=1, device_id=(ix, iy + dy, iz), device_id_type=MESH
                )

    def pass_wait(step):
        for which, dy in ((0, 1), (1, -1)):
            behind = iy - dy * (step + 1)

            @when(behind >= 0, behind < ny)
            def _():
                pl.semaphore_wait(chain.at[which], 1)

    z_start(z_send, z_passed, z_sem)
    near_start(k_raw, k_raw, deep, True, near_sem.at[0])
    near_start(k_raw, k_raw, deep, False, near_sem.at[0])
    pass_on(1)
    coarse_edge(coarse_block(lambda p: k_raw[p, 0:2, own_rows, :], k_send, 3), k_edge)
    keep_own(k_send, k_mid)
    z_pass_on(z_passed, z_got, z_sem)
    near_start(r_near, fine.r, deep - 1, False, near_sem.at[1])
    near_start(r_near, fine.r, deep - 1, True, near_sem.at[2])
    for step in range(1, ny - 1):
        pass_wait(step)
        if step + 1 < ny - 1:
            pass_on(step + 1)
    for side, dz in ((0, 1), (1, -1)):
        @pl.when(z_there[dz])
        def _():
            pl.semaphore_signal(
                chain.at[2 + side], inc=1, device_id=(ix, iy, iz + dz), device_id_type=MESH
            )

    shape = (256, 384)
    from_lane, to_lane = cells(shape, 0), cells(shape, 1)
    to_lane = jnp.where(
        to_lane < 256, to_lane >> 1, (to_lane >> 1) + jnp.where(to_lane < 320, 0, 64)
    )
    widen[...] = ones_where(from_lane == to_lane)
    spread[...] = ones_where(cells((128, 256), 0) == cells((128, 256), 1) >> 1)
    near_wait(deep, (True, False), near_sem.at[0])
    for side, dz in ((0, 1), (1, -1)):
        @pl.when(z_there[-dz])
        def _():
            pl.semaphore_wait(chain.at[2 + side], 1)

    far_start(k_send, k_mid, far_sem.at[0])
    far_start_sides(k_edge, k_side, far_sem.at[0])
    z_wait(z_passed, z_sem, False)
    unpack_z(z_passed, z_got, 0, k_raw)
    fine.diagonal(k_raw, span(4), both)
    loaded(2, fine.r)
    unpack_z(z_passed, z_got, 1, fine.r)
    near_wait(deep - 1, (False,), near_sem.at[1])

    def strip(first, last):
        return (bx - last + ix * (deep + 1 + first - bx + last), last - first + 1)

    def add_fine(ref, first=0, last=bx - 1, fresh=False):
        for a in range(first, last + 1):
            q = bx - 1 - a + ix * (2 * a - bx + 1)
            value = ref[own + q, 0:2, own_rows, :]
            x_fine[q] = value if fresh else x_fine[q] + value

    def smooth_fine(first, last, grow, added):
        for number in range(DEGREE):
            pair = weights[number] if number < DEGREE - 1 else None
            rows, tiles = (both, None) if number < DEGREE - 1 else (middle, 2)
            fine.apply(strip(first, last), rows, pair, tiles)
            if pair is not None and number < added:
                add_fine(fine.now[0], max(first, 0), min(last, bx - 1))
            first, last = first + 1, last + grow

    centre, weights = chebyshev_coefs(DEGREE, smooth_low)
    near_wait(deep - 1, (True,), near_sem.at[2])
    fine.first_update(strip(-DEGREE, bx - 1), both, centre)
    add_fine(fine.now[0], fresh=True)
    smooth_fine(1 - DEGREE, bx - 1, 0, DEGREE)

    far_wait(far_sem.at[0], True)
    parts = coarse_block(residual_of, b_send, 2)
    far_start(b_send, mid.r, far_sem.at[1])
    coarse_edge(parts, b_edge)
    far_start_sides(b_edge, b_side, far_sem.at[1])
    near_sent((deep, deep - 1))
    z_wait(z_passed, z_sem, True)
    keep_own(b_send, mid.r)
    save_z(pack_z(fine.r, 0, None), zr_send)
    z_start(zr_send, zr_passed, zr_sem)
    near_start(fine.r, r_near, deep - 1, True, near_sem.at[3])
    near_start(fine.r, r_near, deep - 1, False, near_sem.at[3])
    own_fine = [(q, own + q) for q in range(bx)]
    for q, p in own_fine:
        r_near[p, 0:2, own_rows, :] = fine.r[p, 0:2, own_rows, :]

    mid_span, mid_rows = (1, nx * cx), tuple(range(1, ny * cy, 8))
    low_span, low_rows = (1, nx * cx // 2), tuple(range(1, ny * cy // 2, 8))
    lows = nx * cx // 2
    low_row = ny * cy // 2

    def to_low(read, target):
        rows = []
        for q in range(lows):
            total = None
            for p in (1 + 2 * q, 2 + 2 * q):
                for row in (1, 2):
                    part = read(p, pl.ds(row, low_row, stride=2))
                    total = part if total is None else total + part
            rows.append(wide(total))
        parts = pick(jnp.concatenate(rows, axis=0), shrink[...]) * 0.125
        target[1 : 1 + lows, 0, 1 : 1 + low_row, :] = parts.reshape(lows, low_row, 128)

    far_wait(far_sem.at[0])
    unpack_far(k_side, k_mid)
    mid.diagonal(k_mid, mid_span, mid_rows)
    to_low(lambda p, rows: k_mid[p, :, rows, :], k_low)
    low.diagonal(k_low, low_span, low_rows)

    z_pass_on(zr_passed, zr_got, zr_sem)
    far_wait(far_sem.at[1])
    unpack_far(b_side, mid.r)
    start = 8
    inside = (slice(1, 1 + nx * cx), slice(None), slice(1, 1 + ny * cy))

    def add_mid(ref, fresh=False):
        for q in range(nx * cx):
            value = ref[1 + q, :, 1 : 1 + ny * cy, :]
            at = (q, slice(None), slice(start, start + ny * cy))
            x_mid[at] = value if fresh else x_mid[at] + value

    mid.first_update(mid_span, mid_rows, centre)
    add_mid(mid.now[0], True)
    for number in range(DEGREE):
        pair = weights[number] if number < DEGREE - 1 else None
        mid.apply(mid_span, mid_rows, pair, None, x_mid)

    to_low(lambda p, rows: mid.r[p, :, rows, :] * mid.dg[p, :, rows, :], low.r)
    low_centre, low_weights = chebyshev_coefs(COARSE_DEGREE, coarse_low)
    near_wait(deep - 1, (True, False), near_sem.at[3])
    z_wait(zr_passed, zr_sem, False)
    low.first_update(low_span, low_rows, low_centre)
    unpack_z(zr_passed, zr_got, 0, r_near)

    def low_now():
        return low.now[0][1 : 1 + lows, 0, 1 : 1 + low_row, :]

    x_low[...] = low_now()
    for pair in low_weights:
        low.apply(low_span, low_rows, pair)
        x_low[...] += low_now()

    fixed = pick(x_low[...].reshape(lows * low_row, 128), spread[...]).reshape(lows, low_row, 256)
    for q in range(lows):
        for t in range(2):
            value = fixed[q, :, 128 * t : 128 * t + 128]
            for p in (1 + 2 * q, 2 + 2 * q):
                for row in (1, 2):
                    mid.now[0][p, t, pl.ds(row, low_row, stride=2), :] = value
    for p in range(1, 1 + nx * cx):
        at = (p, slice(None), slice(1, 1 + ny * cy))
        mid.now[1][at] = mid.ks[at] * mid.now[0][at]
    add_mid(mid.now[0])
    mid.apply(mid_span, mid_rows, (0.0, 1.0 / centre), None, x_mid)
    for pair in weights:
        mid.apply(mid_span, mid_rows, pair, None, x_mid)

    planes = (bx + deep + 1) // 2
    rows = []
    x_rows = 16
    for j in range(planes):
        from_row = start - 3 + cy * iy
        rows.append(wide(x_mid[ix + j, :, pl.ds(from_row, x_rows), :]))
    fixed = pick(jnp.concatenate(rows, axis=0), widen[...]).reshape(planes, x_rows, 384)
    for j in range(planes):
        for t in range(3):
            value = fixed[j, :, 128 * t : 128 * t + 128]
            for p in (0, 1):
                for row in (0, 1):
                    at = 1 - ix + 2 * j + p
                    fine.now[0][at, t, pl.ds(2 + row, 8, stride=2), :] = value[0:8]
                    fine.now[0][at, t, pl.ds(18 + row, 2, stride=2), :] = value[8:10]
    for p in range(1, 1 + bx + deep):
        fine.now[1][p] = (3.0 * fine.scale) * k_raw[p] * fine.now[0][p]
    add_fine(fine.now[0])
    fine.r = r_near
    fine.apply(span(4), both, (0.0, 1.0 / centre))
    add_fine(fine.now[0])
    smooth_fine(1 - DEGREE, bx - 1, 0, DEGREE - 2)
    for q, p in own_fine:
        last, left = fine.new[0][p, 0:2, own_rows, :], residual_of(p)
        for t in range(2):
            at = (q, slice(None), slice(128 * t, 128 * t + 128))
            x_out[at] = x_fine[q, t]
            d_out[at] = last[t]
            r_out[at] = left[t] - last[t]
    near_sent((deep - 1,))
    z_wait(zr_passed, zr_sem, True)
    far_wait(far_sem.at[1], True)


def gathered(sizes, conductivity, source):
    (nx, ny, nz) = sizes
    (bx, by, bz) = conductivity.shape
    kept = lambda *shape: pltpu.VMEM(shape, jnp.float32)
    fine = kept(bx + 7, 3, 3 * by, 128)
    mid = kept(nx * bx // 2 + 2, 2, ny * by // 2 + 8, 128)
    low = kept(nx * bx // 4 + 2, 1, ny * by // 4 + 8, 128)
    cx, cy = bx // 2, by // 2
    scratch = [fine, mid, low] + [fine] * 8 + [mid] * 8 + [low] * 8
    scratch += [fine, kept(bx, 2, by, 128), kept(nx * cx, 2, ny * cy + 24, 128)]
    scratch += [kept(nx * cx // 2, ny * cy // 2, 128), kept(cx, 2, 2 * by, 128)]
    scratch += [kept(cx, by, 128)] * 2 + [kept(2, 2 * by, 128)] * 2
    scratch += [kept(2, nx, ny * cy, 128)] * 2
    scratch += [kept(2, 2, by, 128), kept(2, 2, by, 128), kept(2, 3, 2, by, 128)] * 2
    dma = pltpu.SemaphoreType.DMA
    scratch += [dma((3,)), dma((5,)), dma((4,)), dma((4,)), dma((4,)), dma((1,)), dma((2,))]
    scratch += [pltpu.SemaphoreType.REGULAR((4,))]
    chosen = lambda *shape: pltpu.VMEM(shape, jnp.bfloat16)
    scratch += [chosen(256, 128), chosen(128, 256), chosen(256, 384)]
    shape = pltpu.VMEM((bx, by, bz), jnp.float32)
    vmem = pl.BlockSpec(memory_space=pltpu.VMEM)
    anywhere = pl.BlockSpec(memory_space=pltpu.HBM)
    x_part, r_part, last = pl.pallas_call(
        functools.partial(kernel, sizes, (bx, by, bz)),
        out_shape=(shape,) * 3,
        in_specs=[anywhere, anywhere],
        out_specs=(vmem,) * 3,
        scratch_shapes=scratch,
        compiler_params=pltpu.CompilerParams(
            collective_id=0, has_side_effects=True, vmem_limit_bytes=66715648
        ),
    )(conductivity, source)
    return x_part + last, r_part + last


def plan(conductivity, source):
    sizes = tuple(lax.axis_size(axis) for axis in ("gx", "gy", "gz"))
    (bx, by, bz) = conductivity.shape
    fits = (bx, by, bz) == (8, 8, 256) and sizes[0] == 2 and sizes[1] == 4
    if fits:
        return gathered(sizes, conductivity, source)
    return body(conductivity, source)


def solution(mesh):
    in_specs = (P("gx", "gy", "gz"), P("gx", "gy", "gz"))
    out_specs = (P("gx", "gy", "gz"), P("gx", "gy", "gz"))
    return jax.shard_map(plan, mesh=mesh, in_specs=in_specs, out_specs=out_specs, check_vma=False)
```

```python
import functools

import jax
import jax.numpy as jnp
from jax import lax
from jax.experimental import pallas as pl
from jax.experimental.pallas import tpu as pltpu
from jax.sharding import PartitionSpec as P

LEVELS = 3
DEGREE = 4
COARSE_DEGREE = 8
MESH = pl.DeviceIdType.MESH


weight_table = {1: 14.0 / 30.0, 2: 3.0 / 30.0, 3: 1.0 / 30.0}
neighbour_offsets = [
    (along_one, along_two, along_three)
    for along_one in (-1, 0, 1)
    for along_two in (-1, 0, 1)
    for along_three in (-1, 0, 1)
    if (along_one, along_two, along_three) != (0, 0, 0)
]
smooth_low = 0.5
coarse_low = 0.03
upper_bound = 2.0


def padded_2(block, sides, width):
    for axis, dim in sides:
        count = lax.axis_size(axis)
        forward = [(i, i + 1) for i in range(count - 1)]
        backward = [(target, source) for source, target in forward]
        low = lax.ppermute(
            lax.slice_in_dim(block, block.shape[dim] - width, None, axis=dim), axis, forward
        )
        high = lax.ppermute(lax.slice_in_dim(block, 0, width, axis=dim), axis, backward)
        block = jnp.concatenate([low, block, high], axis=dim)
    return block


def shifted(padded, offset):
    return padded[
        1 + offset[0] : padded.shape[0] - 1 + offset[0],
        1 + offset[1] : padded.shape[1] - 1 + offset[1],
        1 + offset[2] : padded.shape[2] - 1 + offset[2],
    ]


def inner(values, margin):
    return values[
        margin : values.shape[0] - margin,
        margin : values.shape[1] - margin,
        margin : values.shape[2] - margin,
    ]


def stencil(field_pad, coeff_pad, spacing):
    centre_field = shifted(field_pad, (0, 0, 0))
    centre_coeff = shifted(coeff_pad, (0, 0, 0))
    total = jnp.zeros(centre_field.shape, jnp.float32)
    for offset in neighbour_offsets:
        weight = weight_table[abs(offset[0]) + abs(offset[1]) + abs(offset[2])]
        total = total + weight * (centre_coeff + shifted(coeff_pad, offset)) * (
            centre_field - shifted(field_pad, offset)
        )
    return total * (0.5 / spacing)


def diagonal_of(coeff_pad, spacing):
    centre_coeff = shifted(coeff_pad, (0, 0, 0))
    total = jnp.zeros(centre_coeff.shape, jnp.float32)
    for offset in neighbour_offsets:
        weight = weight_table[abs(offset[0]) + abs(offset[1]) + abs(offset[2])]
        total = total + weight * (centre_coeff + shifted(coeff_pad, offset))
    return total * (0.5 / spacing)


def coarsen(values):
    extent = values.shape
    return values.reshape(extent[0] // 2, 2, extent[1] // 2, 2, extent[2] // 2, 2).mean(
        axis=(1, 3, 5)
    )


def refine(values):
    return jnp.repeat(jnp.repeat(jnp.repeat(values, 2, axis=0), 2, axis=1), 2, axis=2)


def chebyshev_coefs(degree, lower):
    centre = (upper_bound + lower) / 2.0
    half_width = (upper_bound - lower) / 2.0
    ratio_term = centre / half_width
    rho_prev = 1.0 / ratio_term
    weights = []
    for number in range(1, degree):
        rho_next = 1.0 / (2.0 * ratio_term - rho_prev)
        weights.append((rho_next * rho_prev, 2.0 * rho_next / half_width))
        rho_prev = rho_next
    return (centre, weights)


def inside_mask(extent, margin):
    first_pos = (
        lax.axis_index("gx") * extent[0]
        + jnp.arange(extent[0] + 2 * margin, dtype=jnp.int32)
        - margin
    )
    second_pos = (
        lax.axis_index("gy") * extent[1]
        + jnp.arange(extent[1] + 2 * margin, dtype=jnp.int32)
        - margin
    )
    third_pos = (
        lax.axis_index("gz") * extent[2]
        + jnp.arange(extent[2] + 2 * margin, dtype=jnp.int32)
        - margin
    )
    first_ok = (first_pos >= 0) & (first_pos < extent[0] * lax.axis_size("gx"))
    second_ok = (second_pos >= 0) & (second_pos < extent[1] * lax.axis_size("gy"))
    third_ok = (third_pos >= 0) & (third_pos < extent[2] * lax.axis_size("gz"))
    return first_ok[:, None, None] & second_ok[None, :, None] & third_ok[None, None, :]


def operate_near(context, field):
    spacing, coeff_ext, diagonal_ext, inside = context
    padded = padded_2(field, (("gx", 0), ("gy", 1), ("gz", 2)), 1)
    return stencil(padded, inner(coeff_ext, 1), spacing)


def two_steps(context, solution, residual, update, first_pair, second_pair):
    spacing, coeff_ext, diagonal_ext, inside = context
    diagonal = inner(diagonal_ext, 1)
    stacked = jnp.stack([update, residual])
    padded = padded_2(stacked, (("gx", 1), ("gy", 2), ("gz", 3)), 2)
    update_wide = padded[0]
    residual_wide = padded[1]
    residual_near = inner(residual_wide, 1) - stencil(update_wide, coeff_ext, spacing)
    update_near = (
        first_pair[0] * inner(update_wide, 1) + first_pair[1] * residual_near / diagonal_ext
    )
    update_near = jnp.where(inside, update_near, 0.0)
    solution = solution + inner(update_near, 1)
    residual = inner(residual_near, 1) - stencil(update_near, inner(coeff_ext, 1), spacing)
    if second_pair is None:
        update = inner(update_near, 1)
    else:
        update = second_pair[0] * inner(update_near, 1) + second_pair[1] * residual / diagonal
        solution = solution + update
    return (solution, residual, update)


def relax(context, right_side, start, degree, lower, final):
    diagonal = inner(context[2], 1)
    centre, weights = chebyshev_coefs(degree, lower)
    if start is None:
        residual = right_side
    else:
        residual = right_side - operate_near(context, start)
    update = residual / (centre * diagonal)
    solution = update if start is None else start + update
    plan_list = list(weights) + ([None] if final else [])
    position = 0
    while position + 1 < len(plan_list):
        solution, residual, update = two_steps(
            context, solution, residual, update, plan_list[position], plan_list[position + 1]
        )
        position = position + 2
    leftover = plan_list[position:]
    for pair in leftover:
        residual = residual - operate_near(context, update)
        update = pair[0] * update + pair[1] * residual / diagonal
        solution = solution + update
    return (solution, residual)


def body(conductivity, source):
    coeff_now = conductivity
    contexts = []
    for grid_level in range(LEVELS):
        if grid_level > 0:
            coeff_now = coarsen(coeff_now)
        spacing = float(4**grid_level)
        coeff_ext = padded_2(coeff_now, (("gx", 0), ("gy", 1), ("gz", 2)), 2)
        inside = inside_mask(coeff_now.shape, 1)
        diagonal_ext = jnp.where(inside, diagonal_of(coeff_ext, spacing), 1.0)
        contexts.append((spacing, coeff_ext, diagonal_ext, inside))

    def cycle(grid_level, right_side):
        context = contexts[grid_level]
        if grid_level == LEVELS - 1:
            return relax(context, right_side, None, COARSE_DEGREE, coarse_low, False)
        solution, residual = relax(context, right_side, None, DEGREE, smooth_low, True)
        correction, ignored = cycle(grid_level + 1, coarsen(residual))
        solution = solution + refine(correction)
        return relax(context, right_side, solution, DEGREE, smooth_low, grid_level == 0)

    return cycle(0, source)


def cells(shape, dim):
    return lax.broadcasted_iota(jnp.int32, shape, dim)


def ones_where(condition):
    return jnp.where(condition, 1.0, 0.0).astype(jnp.bfloat16)


def pick(dense, chosen, parts=2):
    total = None
    for _ in range(parts):
        part = dense.astype(jnp.bfloat16)
        dense = dense - part.astype(jnp.float32)
        term = jnp.dot(part, chosen, preferred_element_type=jnp.float32)
        total = term if total is None else total + term
    return total


def turn(values, shift):
    dim = len(values.shape) - 1
    return pltpu.roll(values, shift % values.shape[dim], dim)


def beside(values):
    low, high = turn(values, 1), turn(values, -1)
    tiles = values.shape[0]
    if tiles > 1:
        lane = cells(values.shape, 2)
        low = jnp.where(lane == 0, jnp.concatenate([low[tiles - 1 :], low[: tiles - 1]]), low)
        high = jnp.where(lane == 127, jnp.concatenate([high[1:], high[:1]]), high)
    return low + high


FACE = 14.0 / 3.0


def around_of(before, here, after, tiles):
    faces = before[0] + after[0] + here[1]
    edges = before[1] + after[1]
    inward = FACE * here[0] + faces + (1.0 / 3.0) * edges
    return (FACE * faces + edges)[:tiles] + beside(inward)[:tiles]


class Level:
    def __init__(self, refs, scale):
        self.ks, self.r, self.dg, self.di = refs[:4]
        self.now, self.new = refs[4:6], refs[6:8]
        self.scale = scale

    def grab(self, ref, p, row):
        return (
            ref[p, :, row : row + 8, :],
            ref[p, :, row - 1 : row + 7, :] + ref[p, :, row + 1 : row + 9, :],
        )

    def diagonal(self, raw, span, rows):
        base, count = span
        for row in rows:
            at = slice(row, row + 8)
            before, here = self.grab(raw, base - 1, row), self.grab(raw, base, row)
            for p in (base + j for j in range(count)):
                after = self.grab(raw, p + 1, row)
                near = around_of(before, here, after, raw.shape[1])
                total = self.scale * (128.0 * here[0] + 3.0 * near)
                self.dg[p, :, at, :] = total
                self.di[p, :, at, :] = jnp.where(here[0] > 0.0, 1.0 / total, 0.0)
                self.ks[p, :, at, :] = (3.0 * self.scale) * here[0]
                before, here = here, after

    def first_update(self, span, rows, centre):
        base, count = span
        for row in rows:
            at = slice(row, row + 8)
            for p in (base + j for j in range(count)):
                scaled = self.r[p, :, at, :] * self.di[p, :, at, :]
                self.r[p, :, at, :] = scaled
                fresh = scaled * (1.0 / centre)
                self.now[0][p, :, at, :] = fresh
                self.now[1][p, :, at, :] = fresh * self.ks[p, :, at, :]

    def apply(self, span, rows, pair, tiles=None, total=None):
        base, count = span
        tiles = tiles or self.r.shape[1]
        some = slice(0, tiles)
        window = {}
        for row in rows:
            window[row] = [
                [self.grab(ref, q, row) for ref in self.now] for q in (base - 1, base)
            ]
        for p in (base + j for j in range(count)):
            for row in rows:
                at = slice(row, row + 8)
                before, here = window[row]
                after = [self.grab(ref, p + 1, row) for ref in self.now]
                plain, heavy = (around_of(*parts, tiles) for parts in zip(before, here, after))
                coeff = self.ks[p, some, at, :]
                field = here[0][0][:tiles]
                left = field - self.di[p, some, at, :] * (coeff * plain + heavy)
                left = self.r[p, some, at, :] - left
                self.r[p, some, at, :] = left
                if pair is not None:
                    fresh = pair[1] * left
                    if pair[0] != 0.0:
                        fresh = pair[0] * field + fresh
                    self.new[0][p, some, at, :] = fresh
                    self.new[1][p, some, at, :] = coeff * fresh
                    if total is not None:
                        place = (p - 1, some, slice(row + 7, row + 15), slice(None))
                        total[place] = total[place] + fresh
                window[row] = [here, after]
        self.now, self.new = self.new, self.now


def kernel(sizes, block, *refs):
    (nx, ny, nz) = sizes
    (bx, by, bz) = block
    deep = 5
    cx, cy = bx // 2, by // 2
    (k_in, b_in, x_out, r_out, d_out) = refs[:5]
    refs = refs[1:]
    (k_raw, k_mid, k_low) = refs[4:7]
    fine = Level(refs[7:15], 0.5 / 30.0)
    mid = Level(refs[15:23], 0.5 / 4.0 / 30.0)
    low = Level(refs[23:31], 0.5 / 16.0 / 30.0)
    (r_near, x_fine, x_mid, x_low, half_sum) = refs[31:36]
    (k_send, b_send, k_edge, b_edge, k_side, b_side) = refs[36:42]
    (z_send, z_passed, z_got, zr_send, zr_passed, zr_got) = refs[42:48]
    (load_sem, near_send, near_sem, z_sem, zr_sem, far_send, far_sem, chain) = refs[48:56]
    (shrink, spread, widen) = refs[56:59]
    ix, iy, iz = lax.axis_index("gx"), lax.axis_index("gy"), lax.axis_index("gz")
    own = 1 + deep * ix
    other = (1 - ix, iy, iz)
    mine = (pl.ds(own, bx), pl.ds(0, 2), pl.ds(by, by), slice(None))

    def span(width):
        return (own - ix * width, bx + width)

    both, middle = (by // 2, by + by // 2), (by,)

    for ref, target, which in ((k_in, k_raw, 0), (b_in, r_near, 1), (b_in, fine.r, 2)):
        for t in range(2):
            pltpu.make_async_copy(
                ref.at[:, :, pl.ds(128 * t, 128)],
                target.at[pl.ds(own, bx), t, pl.ds(by, by), :],
                load_sem.at[which],
            ).start()

    barrier = pltpu.get_barrier_semaphore()
    z_there = {1: iz + 1 < nz, -1: iz > 0, 0: None}
    y_there = {1: iy + 1 < ny, -1: iy > 0, 0: None}

    def when(*conditions):
        kept = [c for c in conditions if c is not None]
        if not kept:
            return lambda f: f()
        total = kept[0]
        for c in kept[1:]:
            total = total & c
        return pl.when(total)

    def column(skip):
        for jx in range(nx):
            for jy in range(ny):
                if jx or jy or not skip:
                    yield ((ix + jx) % nx, (iy + jy) % ny)

    def counted(number, *conditions):
        for c in conditions:
            if c is not None:
                number = jnp.where(c, number, 0)
        return number

    def greet(target):
        pl.semaphore_signal(barrier, inc=1, device_id=target, device_id_type=MESH)

    peers = 0
    for dz, dys in ((0, (0, 1, -1)), (1, (0,)), (-1, (0,))):
        for dy in dys:
            there = (z_there[dz], y_there[dy])
            near = [ix] if dz else [jx for jx in (ix, 1 - ix) if dy or jx is not ix]

            @when(*there)
            def _():
                for jx in near:
                    greet((jx, iy + dy, iz + dz))

            peers = peers + counted(len(near), *there)

    def clear(ref, *at):
        for p in range(ref.shape[0]):
            ref[(p, *at)] = jnp.zeros(ref[(p, *at)].shape, jnp.float32)

    for p in (0, bx + deep + 1):
        k_raw[p] = jnp.zeros(k_raw.shape[1:], jnp.float32)
    for ref in (k_raw, fine.r, r_near):
        @pl.when(iy == 0)
        def _():
            clear(ref, slice(0, 2), slice(0, by))

        @pl.when(iy == ny - 1)
        def _():
            clear(ref, slice(0, 2), slice(2 * by, 3 * by))

    def blank(ref, dims):
        ref[dims] = jnp.zeros(ref[dims].shape, jnp.float32)

    for ref, passed in ((z_got, z_passed), (zr_got, zr_passed)):
        for side, gone in ((0, iz == 0), (1, iz == nz - 1)):
            @pl.when(gone)
            def _():
                blank(ref, (side,))
                blank(passed, (side,))

        for j, gone in ((2, iy == 0), (0, iy == ny - 1)):
            @pl.when(gone)
            def _():
                for side in (0, 1):
                    blank(ref, (side, j))
    for ref in (k_side, b_side):
        for side, gone in ((0, iz == 0), (1, iz == nz - 1)):
            @pl.when(gone)
            def _():
                blank(ref, (side,))
    for ref in (*fine.now, *fine.new, *mid.now, *mid.new, *low.now, *low.new, k_low, x_mid):
        clear(ref)
    top = nx * cx + 1
    for p in (0, top):
        k_mid[p] = jnp.zeros(k_mid.shape[1:], jnp.float32)
    for row in (0, ny * cy + 1):
        clear(k_mid, slice(None), slice(row, row + 1))
    half_sum[...] = jnp.zeros(half_sum.shape, jnp.float32)

    own_rows = slice(by, 2 * by)
    lane = cells((8, 128), 1)

    def residual_of(p):
        return fine.r[p, 0:2, own_rows, :] * fine.dg[p, 0:2, own_rows, :]
    shrink[...] = ones_where(cells((256, 128), 0) >> 1 == cells((256, 128), 1))

    def wide(values):
        return jnp.concatenate([values[0], values[1]], axis=1)

    def coarse_block(read, send, exact):
        for q in range(cx):
            p = own + 2 * q
            half_sum[q, :, 0:by, :] = read(p) + read(p + 1)
        rows = [
            wide(
                half_sum[q, :, pl.ds(0, by, stride=2), :]
                + half_sum[q, :, pl.ds(1, by, stride=2), :]
            )
            for q in range(cx)
        ]
        parts = (pick(jnp.concatenate(rows, axis=0), shrink[...], exact) * 0.125).reshape(cx, by, 128)
        send[...] = parts
        return parts

    def coarse_edge(parts, edge):
        low_part = parts[0]
        top_part = turn(parts[0], 32)
        for q in range(1, cx):
            here = (lane >> 5) == q
            low_part = jnp.where(here, turn(parts[q], 32 * q), low_part)
            top_part = jnp.where(here, turn(parts[q], 32 * q - 96), top_part)
        edge[0, 0:by] = top_part
        edge[1, 0:by] = low_part

    def pack_z(ref, kind, into):
        slot = lane >> 4
        front = (lane & 15) < 8
        packs = [jnp.zeros((8, 128), jnp.float32)] * 2 if into is None else into
        top, bottom = packs
        for q in range(bx):
            here = slot == q
            low_tile = ref[own + q, 0, by : 2 * by, :]
            top_tile = ref[own + q, 1, by : 2 * by, :]
            if kind == 0:
                top = jnp.where(here & front, turn(top_tile, 16 * q - 120), top)
                bottom = jnp.where(
                    here & jnp.logical_not(front), turn(low_tile, 16 * q + 8), bottom
                )
            else:
                after = slot == (q + 1) % 8
                top = jnp.where(
                    here & jnp.logical_not(front), turn(top_tile, 16 * q + 8 - 120), top
                )
                bottom = jnp.where(after & front, turn(low_tile, 16 * q + 16), bottom)
        return (top, bottom)

    def save_z(packs, send):
        for side in (0, 1):
            send[side, 0] = packs[side]
            moved = turn(packs[side], -16 * (bx - deep))
            send[side, 1] = jnp.where(ix == 0, moved, packs[side])

    def remote(source, target, out_sem, in_sem, device):
        return pltpu.make_async_remote_copy(
            src_ref=source,
            dst_ref=target,
            send_sem=out_sem,
            recv_sem=in_sem,
            device_id=device,
            device_id_type=MESH,
        )

    def near_views(ref, depth, dy, start_x, source):
        if dy == 0:
            rows = pl.ds(by, by)
        elif source:
            rows = pl.ds(2 * by - depth, depth) if dy == 1 else pl.ds(by, depth)
        else:
            rows = pl.ds(by - depth, depth) if dy == 1 else pl.ds(2 * by, depth)
        return [
            ref.at[pl.ds(start, planes), pl.ds(0, 2), rows, :]
            for start, planes in ((start_x, depth), (own, bx))
        ]

    def near_start(source, target, depth, along_x, in_sem):
        start_from = jnp.where(ix == 0, bx + 1 - depth, deep + 1)
        start_to = jnp.where(ix == 0, deep + 1 - depth, bx + 1)
        for dy in (0, 1, -1) if along_x else (1, -1):
            @when(y_there[dy])
            def _():
                which = 0 if along_x else 1
                remote(
                    near_views(source, depth, dy, start_from, True)[which],
                    near_views(target, depth, dy, start_to, False)[which],
                    near_send.at[0],
                    in_sem,
                    (1 - ix if along_x else ix, iy + dy, iz),
                ).start()

    inner_y = (iy > 0) & (iy + 1 < ny)
    inner_z = (iz > 0) & (iz + 1 < nz)

    def part_of(ref, rows):
        (p, t, n) = ref.shape[:3]
        sizes = [
            (a, b, rows // (a * b))
            for a in range(1, p + 1)
            for b in range(1, t + 1)
            if rows % (a * b) == 0 and rows // (a * b) <= n
        ]
        (a, b, c) = sizes[0]
        return ref.at[pl.ds(0, a), pl.ds(0, b), pl.ds(0, c), :]

    def wait_rows(ref, out_sem, in_sem, sent, inner, base, each):
        for condition, number in ((inner, 2), (jnp.logical_not(inner), 1)):
            @pl.when(condition)
            def _():
                view = part_of(ref, base + number * each)
                move = remote(view, view, out_sem, in_sem, other)
                if sent:
                    move.wait_send()
                else:
                    move.wait_recv()

    def near_rows(depth, along_x):
        if along_x:
            return 2 * depth * by, 2 * depth * depth
        return 0, 2 * bx * depth

    def near_wait(depth, kinds, in_sem):
        base = sum(near_rows(depth, kind)[0] for kind in kinds)
        each = sum(near_rows(depth, kind)[1] for kind in kinds)
        wait_rows(k_raw, near_send.at[0], in_sem, False, inner_y, base, each)

    def near_sent(depths):
        for depth in depths:
            kinds = [near_rows(depth, kind) for kind in (True, False)]
            base, each = sum(k[0] for k in kinds), sum(k[1] for k in kinds)
            wait_rows(k_raw, near_send.at[0], near_sem.at[0], True, inner_y, base, each)

    def z_start(send, passed, sems):
        for side, dz in ((0, 1), (1, -1)):
            @pl.when(z_there[dz])
            def _():
                remote(
                    send.at[side],
                    passed.at[side],
                    near_send.at[1 + side],
                    sems.at[side],
                    (ix, iy, iz + dz),
                ).start()

    def z_pass_on(passed, got, sems):
        odd = iz % 2 == 1
        for side, dz, turn_of in ((0, 1, odd), (1, -1, None), (0, 1, jnp.logical_not(odd))):
            @when(z_there[-dz], turn_of)
            def _():
                view = passed.at[side]
                remote(view, view, near_send.at[1 + side], sems.at[side], other).wait_recv()
                for dy in (0, 1, -1):
                    @when(y_there[dy])
                    def _():
                        for xi in (0, 1) if dy else (1,):
                            remote(
                                passed.at[side, xi],
                                got.at[side, dy + 1, xi],
                                near_send.at[3 + side],
                                sems.at[2 + side],
                                (ix if xi == 0 else 1 - ix, iy + dy, iz),
                            ).start()

    def z_wait(passed, sems, sent):
        for side, dz in ((0, 1), (1, -1)):
            @pl.when(z_there[-dz])
            def _():
                args = (near_send.at[3 + side], sems.at[2 + side], sent, inner_y, by, 2 * by)
                wait_rows(k_raw, *args)

            if sent:
                @pl.when(z_there[dz])
                def _():
                    view = passed.at[side]
                    remote(view, view, near_send.at[1 + side], sems.at[side], other).wait_send()

    def unpack_z(passed, got, kind, target):
        front = (lane & 15) < 8
        kept = (lane < 8) | (lane >= 120)
        skip = 0 if kind == 0 else 8
        for group in range(3):
            for xi, planes in ((0, bx), (1, deep)):
                straight = group == 1 and xi == 0
                lower, upper = (
                    passed[side, 0] if straight else got[side, 2 - group, xi] for side in (0, 1)
                )
                pair = (lower, upper) if kind == 0 else (upper, lower)
                merged = jnp.where(front, *pair)
                first = own if xi == 0 else jnp.where(ix == 0, bx + 1, 1)
                for q in range(planes):
                    target[first + q, 2, by * group : by * group + by, :] = jnp.where(
                        kept, turn(merged, -(16 * q + 8 + skip)), 0.0
                    )

    def far_start(send, target, in_sem):
        for jx, jy in reversed(list(column(True))):
            remote(
                send.at[:, pl.ds(0, cy), :],
                target.at[pl.ds(1 + cx * ix, cx), 0, pl.ds(1 + cy * iy, cy), :],
                far_send.at[0],
                in_sem,
                (jx, jy, iz),
            ).start()

    def far_start_sides(edge, side_target, in_sem):
        for side, dz in ((0, 1), (1, -1)):
            @when(z_there[dz])
            def _():
                for jx, jy in reversed(list(column(False))):
                    remote(
                        edge.at[side, pl.ds(0, cy), :],
                        side_target.at[side, ix, pl.ds(cy * iy, cy), :],
                        far_send.at[0],
                        in_sem,
                        (jx, jy, iz + dz),
                    ).start()

    def far_wait(in_sem, sent=False):
        main, each = (nx * ny - 1) * cx * cy, nx * ny * cy
        wait_rows(k_raw, far_send.at[0], in_sem, sent, inner_z, main, each)

    def keep_own(send, target):
        for jy in range(ny):
            @pl.when(iy == jy)
            def _():
                for q in range(cx):
                    rows = slice(1 + cy * jy, 1 + cy * jy + cy)
                    target[1 + cx * ix + q, 0, rows, :] = send[q, 0:cy, :]

    def unpack_far(side_target, target):
        shape = side_target.shape[2:]
        column_of = cells(shape, 1)
        for jx in range(nx):
            below, above = side_target[0, jx], side_target[1, jx]
            for q in range(cx):
                upper = jnp.where(column_of < 32, turn(above, -32 * q), 0.0)
                target[1 + cx * jx + q, 1, 1 : 1 + shape[0], :] = jnp.where(
                    column_of >= 96, turn(below, 96 - 32 * q), upper
                )

    def loaded(which, ref):
        view = ref.at[mine]
        pltpu.make_async_copy(view, view, load_sem.at[which]).wait()

    loaded(0, k_raw)
    loaded(1, r_near)
    save_z(pack_z(r_near, 1, pack_z(k_raw, 0, None)), z_send)
    pl.semaphore_wait(barrier, peers)

    def pass_on(step):
        for which, dy in ((0, 1), (1, -1)):
            behind = iy - dy * step

            @when(y_there[dy], behind >= 0, behind < ny)
            def _():
                pl.semaphore_signal(
                    chain.at[which], inc=1, device_id=(ix, iy + dy, iz), device_id_type=MESH
                )

    def pass_wait(step):
        for which, dy in ((0, 1), (1, -1)):
            behind = iy - dy * (step + 1)

            @when(behind >= 0, behind < ny)
            def _():
                pl.semaphore_wait(chain.at[which], 1)

    z_start(z_send, z_passed, z_sem)
    near_start(k_raw, k_raw, deep, True, near_sem.at[0])
    near_start(k_raw, k_raw, deep, False, near_sem.at[0])
    pass_on(1)
    coarse_edge(coarse_block(lambda p: k_raw[p, 0:2, own_rows, :], k_send, 3), k_edge)
    keep_own(k_send, k_mid)
    z_pass_on(z_passed, z_got, z_sem)
    near_start(r_near, fine.r, deep - 1, False, near_sem.at[1])
    near_start(r_near, fine.r, deep - 1, True, near_sem.at[2])
    for step in range(1, ny - 1):
        pass_wait(step)
        if step + 1 < ny - 1:
            pass_on(step + 1)
    for side, dz in ((0, 1), (1, -1)):
        @pl.when(z_there[dz])
        def _():
            pl.semaphore_signal(
                chain.at[2 + side], inc=1, device_id=(ix, iy, iz + dz), device_id_type=MESH
            )

    shape = (256, 384)
    from_lane, to_lane = cells(shape, 0), cells(shape, 1)
    to_lane = jnp.where(
        to_lane < 256, to_lane >> 1, (to_lane >> 1) + jnp.where(to_lane < 320, 0, 64)
    )
    widen[...] = ones_where(from_lane == to_lane)
    spread[...] = ones_where(cells((128, 256), 0) == cells((128, 256), 1) >> 1)
    near_wait(deep, (True, False), near_sem.at[0])
    for side, dz in ((0, 1), (1, -1)):
        @pl.when(z_there[-dz])
        def _():
            pl.semaphore_wait(chain.at[2 + side], 1)

    far_start(k_send, k_mid, far_sem.at[0])
    far_start_sides(k_edge, k_side, far_sem.at[0])
    z_wait(z_passed, z_sem, False)
    unpack_z(z_passed, z_got, 0, k_raw)
    fine.diagonal(k_raw, span(4), both)
    loaded(2, fine.r)
    unpack_z(z_passed, z_got, 1, fine.r)
    near_wait(deep - 1, (False,), near_sem.at[1])

    def strip(first, last):
        return (bx - last + ix * (deep + 1 + first - bx + last), last - first + 1)

    def add_fine(ref, first=0, last=bx - 1, fresh=False):
        for a in range(first, last + 1):
            q = bx - 1 - a + ix * (2 * a - bx + 1)
            value = ref[own + q, 0:2, own_rows, :]
            x_fine[q] = value if fresh else x_fine[q] + value

    def smooth_fine(first, last, grow, added):
        for number in range(DEGREE):
            pair = weights[number] if number < DEGREE - 1 else None
            rows, tiles = (both, None) if number < DEGREE - 1 else (middle, 2)
            fine.apply(strip(first, last), rows, pair, tiles)
            if pair is not None and number < added:
                add_fine(fine.now[0], max(first, 0), min(last, bx - 1))
            first, last = first + 1, last + grow

    centre, weights = chebyshev_coefs(DEGREE, smooth_low)
    near_wait(deep - 1, (True,), near_sem.at[2])
    fine.first_update(strip(-DEGREE, bx - 1), both, centre)
    add_fine(fine.now[0], fresh=True)
    smooth_fine(1 - DEGREE, bx - 1, 0, DEGREE)

    far_wait(far_sem.at[0], True)
    parts = coarse_block(residual_of, b_send, 2)
    far_start(b_send, mid.r, far_sem.at[1])
    coarse_edge(parts, b_edge)
    far_start_sides(b_edge, b_side, far_sem.at[1])
    near_sent((deep, deep - 1))
    z_wait(z_passed, z_sem, True)
    keep_own(b_send, mid.r)
    save_z(pack_z(fine.r, 0, None), zr_send)
    z_start(zr_send, zr_passed, zr_sem)
    near_start(fine.r, r_near, deep - 1, True, near_sem.at[3])
    near_start(fine.r, r_near, deep - 1, False, near_sem.at[3])
    own_fine = [(q, own + q) for q in range(bx)]
    for q, p in own_fine:
        r_near[p, 0:2, own_rows, :] = fine.r[p, 0:2, own_rows, :]

    mid_span, mid_rows = (1, nx * cx), tuple(range(1, ny * cy, 8))
    low_span, low_rows = (1, nx * cx // 2), tuple(range(1, ny * cy // 2, 8))
    lows = nx * cx // 2
    low_row = ny * cy // 2

    def to_low(read, target):
        rows = []
        for q in range(lows):
            total = None
            for p in (1 + 2 * q, 2 + 2 * q):
                for row in (1, 2):
                    part = read(p, pl.ds(row, low_row, stride=2))
                    total = part if total is None else total + part
            rows.append(wide(total))
        parts = pick(jnp.concatenate(rows, axis=0), shrink[...]) * 0.125
        target[1 : 1 + lows, 0, 1 : 1 + low_row, :] = parts.reshape(lows, low_row, 128)

    far_wait(far_sem.at[0])
    unpack_far(k_side, k_mid)
    mid.diagonal(k_mid, mid_span, mid_rows)
    to_low(lambda p, rows: k_mid[p, :, rows, :], k_low)
    low.diagonal(k_low, low_span, low_rows)

    z_pass_on(zr_passed, zr_got, zr_sem)
    far_wait(far_sem.at[1])
    unpack_far(b_side, mid.r)
    start = 8
    inside = (slice(1, 1 + nx * cx), slice(None), slice(1, 1 + ny * cy))

    def add_mid(ref, fresh=False):
        for q in range(nx * cx):
            value = ref[1 + q, :, 1 : 1 + ny * cy, :]
            at = (q, slice(None), slice(start, start + ny * cy))
            x_mid[at] = value if fresh else x_mid[at] + value

    mid.first_update(mid_span, mid_rows, centre)
    add_mid(mid.now[0], True)
    for number in range(DEGREE):
        pair = weights[number] if number < DEGREE - 1 else None
        mid.apply(mid_span, mid_rows, pair, None, x_mid)

    to_low(lambda p, rows: mid.r[p, :, rows, :] * mid.dg[p, :, rows, :], low.r)
    low_centre, low_weights = chebyshev_coefs(COARSE_DEGREE, coarse_low)
    near_wait(deep - 1, (True, False), near_sem.at[3])
    z_wait(zr_passed, zr_sem, False)
    low.first_update(low_span, low_rows, low_centre)
    unpack_z(zr_passed, zr_got, 0, r_near)

    def low_now():
        return low.now[0][1 : 1 + lows, 0, 1 : 1 + low_row, :]

    x_low[...] = low_now()
    for pair in low_weights:
        low.apply(low_span, low_rows, pair)
        x_low[...] += low_now()

    fixed = pick(x_low[...].reshape(lows * low_row, 128), spread[...]).reshape(lows, low_row, 256)
    for q in range(lows):
        for t in range(2):
            value = fixed[q, :, 128 * t : 128 * t + 128]
            for p in (1 + 2 * q, 2 + 2 * q):
                for row in (1, 2):
                    mid.now[0][p, t, pl.ds(row, low_row, stride=2), :] = value
    for p in range(1, 1 + nx * cx):
        at = (p, slice(None), slice(1, 1 + ny * cy))
        mid.now[1][at] = mid.ks[at] * mid.now[0][at]
    add_mid(mid.now[0])
    mid.apply(mid_span, mid_rows, (0.0, 1.0 / centre), None, x_mid)
    for pair in weights:
        mid.apply(mid_span, mid_rows, pair, None, x_mid)

    planes = (bx + deep + 1) // 2
    rows = []
    x_rows = 16
    for j in range(planes):
        from_row = start - 3 + cy * iy
        rows.append(wide(x_mid[ix + j, :, pl.ds(from_row, x_rows), :]))
    fixed = pick(jnp.concatenate(rows, axis=0), widen[...]).reshape(planes, x_rows, 384)
    for j in range(planes):
        for t in range(3):
            value = fixed[j, :, 128 * t : 128 * t + 128]
            for p in (0, 1):
                for row in (0, 1):
                    at = 1 - ix + 2 * j + p
                    fine.now[0][at, t, pl.ds(2 + row, 8, stride=2), :] = value[0:8]
                    fine.now[0][at, t, pl.ds(18 + row, 2, stride=2), :] = value[8:10]
    for p in range(1, 1 + bx + deep):
        fine.now[1][p] = (3.0 * fine.scale) * k_raw[p] * fine.now[0][p]
    add_fine(fine.now[0])
    fine.r = r_near
    fine.apply(span(4), both, (0.0, 1.0 / centre))
    add_fine(fine.now[0])
    smooth_fine(1 - DEGREE, bx - 1, 0, DEGREE - 2)
    for q, p in own_fine:
        last, left = fine.new[0][p, 0:2, own_rows, :], residual_of(p)
        for t in range(2):
            at = (q, slice(None), slice(128 * t, 128 * t + 128))
            x_out[at] = x_fine[q, t]
            d_out[at] = last[t]
            r_out[at] = left[t] - last[t]
    near_sent((deep - 1,))
    z_wait(zr_passed, zr_sem, True)
    far_wait(far_sem.at[1], True)


def gathered(sizes, conductivity, source):
    (nx, ny, nz) = sizes
    (bx, by, bz) = conductivity.shape
    kept = lambda *shape: pltpu.VMEM(shape, jnp.float32)
    fine = kept(bx + 7, 3, 3 * by, 128)
    mid = kept(nx * bx // 2 + 2, 2, ny * by // 2 + 8, 128)
    low = kept(nx * bx // 4 + 2, 1, ny * by // 4 + 8, 128)
    cx, cy = bx // 2, by // 2
    scratch = [fine, mid, low] + [fine] * 8 + [mid] * 8 + [low] * 8
    scratch += [fine, kept(bx, 2, by, 128), kept(nx * cx, 2, ny * cy + 24, 128)]
    scratch += [kept(nx * cx // 2, ny * cy // 2, 128), kept(cx, 2, 2 * by, 128)]
    scratch += [kept(cx, by, 128)] * 2 + [kept(2, 2 * by, 128)] * 2
    scratch += [kept(2, nx, ny * cy, 128)] * 2
    scratch += [kept(2, 2, by, 128), kept(2, 2, by, 128), kept(2, 3, 2, by, 128)] * 2
    dma = pltpu.SemaphoreType.DMA
    scratch += [dma((3,)), dma((5,)), dma((4,)), dma((4,)), dma((4,)), dma((1,)), dma((2,))]
    scratch += [pltpu.SemaphoreType.REGULAR((4,))]
    chosen = lambda *shape: pltpu.VMEM(shape, jnp.bfloat16)
    scratch += [chosen(256, 128), chosen(128, 256), chosen(256, 384)]
    shape = pltpu.VMEM((bx, by, bz), jnp.float32)
    vmem = pl.BlockSpec(memory_space=pltpu.VMEM)
    anywhere = pl.BlockSpec(memory_space=pltpu.HBM)
    x_part, r_part, last = pl.pallas_call(
        functools.partial(kernel, sizes, (bx, by, bz)),
        out_shape=(shape,) * 3,
        in_specs=[anywhere, anywhere],
        out_specs=(vmem,) * 3,
        scratch_shapes=scratch,
        compiler_params=pltpu.CompilerParams(
            collective_id=0, has_side_effects=True, vmem_limit_bytes=66715648
        ),
    )(conductivity, source)
    return x_part + last, r_part + last


def plan(conductivity, source):
    sizes = tuple(lax.axis_size(axis) for axis in ("gx", "gy", "gz"))
    (bx, by, bz) = conductivity.shape
    fits = (bx, by, bz) == (8, 8, 256) and sizes[0] == 2 and sizes[1] == 4
    if fits:
        return gathered(sizes, conductivity, source)
    return body(conductivity, source)


def solution(mesh):
    in_specs = (P("gx", "gy", "gz"), P("gx", "gy", "gz"))
    out_specs = (P("gx", "gy", "gz"), P("gx", "gy", "gz"))
    return jax.shard_map(plan, mesh=mesh, in_specs=in_specs, out_specs=out_specs, check_vma=False)
```
